32 devices in a mesh: lat: 2 (over y), lon: 8 (over z, core), freq: 2 (over x).
Axes of the slice: x: 2, y: 2, z: 4, core: 2. Of those that a mesh axis runs over, the one named last changes fastest.
Arguments:
- spectrum: float32 [36, 36, 8, 1024], P('freq', None, 'lat', 'lon'), may hold values from 0.05 to 1
- group_speed: float32 [36], P('freq'), may hold values from 0.15 to 0.6
- sea_mask: int32 [8, 1024], P('lat', 'lon'), may hold values 0 or 1
- wind_growth: float32 [8, 1024], P('lat', 'lon'), may hold values from 0.2 to 2
- dissipation: float32 [8, 1024], P('lat', 'lon'), may hold values from 0.1 to 1
- wind_profile: float32 [1296], replicated, may hold values from 0.02 to 0.2
- nonlinear_coef: float32 [1296], replicated, may hold values from 0.05 to 0.5
- momentum: float32 [2, 1296], replicated, may hold values from -6 to 6
- quadruplet: int32 [2, 1296], replicated, may hold values from 0 to 1295, as said below
- ocean_cell: int32 [8, 1024], P('lat', 'lon'), may hold values from 0 to 8191, as said below
Outputs:
- spectrum_out: float32 [36, 36, 8, 1024], P('freq', None, 'lat', 'lon')
- ocean_stress: float32 [8192, 2], P(('lon', 'freq'))
The draws below stay inside these ranges and needn't reach their ends.
Inputs may be any that keep to these rules, and one draw needn't show every extreme that they name: quadruplet[0, b] names a bin 1 or 2 frequencies higher (at most the highest) and 1 to 6 directions further, cyclically; quadruplet[1, b] one 1 or 2 frequencies lower (at least the lowest) and 1 to 6 directions back. ocean_cell[i, j] = j * 8 + i2 with i2 within 1 of i.
All inputs are finite; a program needn't handle non-finite values. No bound on the sum of `sea_mask` on one device may be relied on, other than what follows from the above.
Results may differ from the reference program's by a relative error of at most 0.000094.
Values sent between devices are 32-bit elements; how exact they have to be, the bound alone decides.
A program may use at most 64 MiB of HBM per device.

```python
import math
import jax
import jax.numpy as jnp
from jax import lax

NF = 36
NDIR = 36
NB = 1296
NLAT = 8
NLON = 1024
OCELLS = 8192


def draw_quadruplet(key, part):
    keys = jax.random.split(jax.random.fold_in(key, 7), 4)
    bins = jnp.arange(NF * NDIR)
    freqs = bins // NDIR
    directions = bins % NDIR
    up_freq = jax.random.randint(keys[0], (NF * NDIR,), 1, 3)
    up_dir = jax.random.randint(keys[1], (NF * NDIR,), 1, 7)
    down_freq = jax.random.randint(keys[2], (NF * NDIR,), 1, 3)
    down_dir = jax.random.randint(keys[3], (NF * NDIR,), 1, 7)
    higher = jnp.minimum(freqs + up_freq, NF - 1) * NDIR + (directions + up_dir) % NDIR
    lower = jnp.maximum(freqs - down_freq, 0) * NDIR + (directions - down_dir + NDIR) % NDIR
    return jnp.stack([higher, lower]).astype(jnp.int32)


def draw_ocean_cell(key, part):
    jitter = jax.random.randint(jax.random.fold_in(key, 11), (NLAT, NLON), -1, 2)
    lat_rows = jnp.arange(NLAT)[:, None]
    lon_cols = jnp.arange(NLON)[None, :]
    shifted = jnp.clip(lat_rows + jitter, 0, NLAT - 1)
    return (lon_cols * NLAT + shifted).astype(jnp.int32)


def place_ends(values, key, low, top_value):
    spot = [jax.random.randint(jax.random.fold_in(key, axis), (), 0, length) for axis, length in enumerate(values.shape)]
    main_axis = values.shape.index(max(values.shape))
    next_to = spot[:main_axis] + [(spot[main_axis] + 1) % values.shape[main_axis]] + spot[main_axis + 1:]
    return values.at[tuple(spot)].set(low).at[tuple(next_to)].set(top_value)


def steps_of(rng, extent, pieces, least, top_value):
    level, own = 1.0, jax.random.fold_in(rng, 6)
    for axis_at, shards_of in pieces:
        heights = jnp.exp(jax.random.uniform(jax.random.fold_in(own, axis_at), (shards_of,), jnp.float32, least / len(pieces), top_value / len(pieces)))
        level = level * jnp.repeat(heights, extent[axis_at] // shards_of).reshape([-1 if axis == axis_at else 1 for axis in range(len(extent))])
    return level


def noise(key, shape, deviation, reach, dtype=jnp.bfloat16):
    values = deviation * jax.random.normal(key, shape, jnp.float32)
    return jnp.clip(values, min=-reach, max=reach).astype(dtype)


def setup_inputs(seed: int = 0) -> dict:
    splits = jax.random.split(jax.random.key(seed), 11)
    spectrum = jnp.clip(0.05 + 0.95 * jax.random.uniform(splits[0], (NF, NDIR, NLAT, NLON), jnp.float32) ** steps_of(splits[0], (NF, NDIR, NLAT, NLON), ((0, 2), (2, 2), (3, 8)), -0.2, 0.2), 0.05, 1.0)
    group_speed = jnp.clip(jnp.exp(math.log(0.6) - 1.3862944 * jax.random.uniform(splits[1], (NF,), jnp.float32) ** steps_of(splits[1], (NF,), ((0, 2),), -0.2, 0.2)), 0.15, 0.6)
    sea_mask = place_ends((jax.random.randint(splits[2], (NLAT, NLON), 0, 4) < 3).astype(jnp.int32), jax.random.fold_in(splits[2], 1), 0, 1)
    wind_growth = jnp.clip(jnp.exp(math.log(2.0) - 2.3025851 * jax.random.uniform(splits[3], (NLAT, NLON), jnp.float32) ** steps_of(splits[3], (NLAT, NLON), ((0, 2), (1, 8)), -0.2, 0.2)), 0.2, 2.0)
    dissipation = jnp.clip(jnp.exp(math.log(1.0) - 2.3025851 * jax.random.uniform(splits[4], (NLAT, NLON), jnp.float32) ** steps_of(splits[4], (NLAT, NLON), ((0, 2), (1, 8)), -0.2, 0.2)), 0.1, 1.0)
    wind_profile = jnp.clip(jnp.exp(jax.random.uniform(splits[5], (NB,), jnp.float32, math.log(0.02), math.log(0.2))), 0.02, 0.2)
    nonlinear_coef = jnp.clip(jnp.exp(jax.random.uniform(splits[6], (NB,), jnp.float32, math.log(0.05), math.log(0.5))), 0.05, 0.5)
    momentum = noise(splits[7], (2, NB), 1.0, 6.0, jnp.float32)
    quadruplet = draw_quadruplet(jax.random.fold_in(splits[10], 71), 0)
    ocean_cell = draw_ocean_cell(jax.random.fold_in(splits[10], 71), 0)
    return {"spectrum": spectrum, "group_speed": group_speed, "sea_mask": sea_mask, "wind_growth": wind_growth, "dissipation": dissipation, "wind_profile": wind_profile, "nonlinear_coef": nonlinear_coef, "momentum": momentum, "quadruplet": quadruplet, "ocean_cell": ocean_cell}


time_step = 0.5


def propagate_all(spectrum, group_speed, sea_mask):
    ndirs = spectrum.shape[1]
    angles = 2.0 * jnp.pi * jnp.arange(ndirs).astype(jnp.float32) / ndirs
    speed_x = (group_speed[:, None] * jnp.cos(angles)[None, :])[:, :, None, None]
    speed_y = (group_speed[:, None] * jnp.sin(angles)[None, :])[:, :, None, None]
    west = jnp.roll(spectrum, 1, axis=3)
    east = jnp.roll(spectrum, -1, axis=3)
    padded = jnp.pad(spectrum, ((0, 0), (0, 0), (1, 1), (0, 0)))
    south = padded[:, :, :-2, :]
    north = padded[:, :, 2:, :]
    moved = (spectrum - jnp.maximum(speed_x, 0.0) * (spectrum - west) - jnp.minimum(speed_x, 0.0) * (east - spectrum)
             - jnp.maximum(speed_y, 0.0) * (spectrum - south) - jnp.minimum(speed_y, 0.0) * (north - spectrum))
    return moved * sea_mask.astype(jnp.float32)[None, None]


def reference(spectrum, group_speed, sea_mask, wind_growth, dissipation, wind_profile, nonlinear_coef, momentum, quadruplet, ocean_cell):
    highest = lax.Precision.HIGHEST
    moved = propagate_all(spectrum, group_speed, sea_mask)
    nbins = NF * NDIR
    flat_moved = moved.reshape(nbins, -1)
    weights = momentum * wind_profile[None, :]
    stress = jnp.dot(weights, flat_moved, precision=highest) * wind_growth.reshape(-1)[None, :]
    ocean_stress = jax.ops.segment_sum(stress.T, ocean_cell.reshape(-1), OCELLS)

    def one_row(packed):
        energy_row, wind_row, dissip_row, mask_row = packed
        flat_bins = energy_row.reshape(nbins, -1)
        third = flat_bins[quadruplet[0]]
        fourth = flat_bins[quadruplet[1]]
        transfer = nonlinear_coef[:, None] * (flat_bins * flat_bins * (third + fourth) - 2.0 * flat_bins * third * fourth)
        scattered = jnp.zeros_like(transfer).at[quadruplet[0]].add(transfer).at[quadruplet[1]].add(transfer)
        energy = jnp.mean(flat_bins, axis=0)
        tendency = (wind_row[None, :] * wind_profile[:, None] * flat_bins + scattered - 2.0 * transfer
                    - dissip_row[None, :] * energy[None, :] * flat_bins)
        result = mask_row[None, :] * (flat_bins + time_step * tendency)
        return result.reshape(energy_row.shape)

    by_rows = jnp.moveaxis(moved, 2, 0)
    updated = lax.map(one_row, (by_rows, wind_growth, dissipation, sea_mask.astype(jnp.float32)))
    spectrum_out = jnp.moveaxis(updated, 0, 2)
    return spectrum_out, ocean_stress
```

```python
import functools

import jax
import jax.numpy as jnp
import numpy as np
from jax import lax
from jax.experimental import pallas as pl
from jax.experimental.pallas import tpu as pltpu
from jax.sharding import PartitionSpec as P

time_step = 0.5
MESH = pl.DeviceIdType.MESH
VMEM = pltpu.VMEM
LANES = 128
EDGE = 4
F32, BF16 = jnp.float32, jnp.bfloat16


def spread(nf):
    order = list(range(EDGE)) + list(range(nf - EDGE, nf)) + list(range(EDGE, nf - EDGE))
    return {f: i for i, f in enumerate(order)}


def round_up(n, m):
    return -(-n // m) * m


def split(v):
    high = v.astype(BF16)
    return high, (v - high.astype(F32)).astype(BF16)


def wave_kernel(sizes, angles, spectrum, *refs):
    sources, refs = refs[:10], refs[10:]
    result, stress, *refs = refs
    inputs, refs = refs[:10], refs[10:]
    speed, waves, profile, coef, momentum, quad, mask, wind, dissip, cells = inputs
    (
        x, mf, mh, ml, th, tl, pick, put, table, rates, cols, lines, coefs, shapes, weight0, weight1,
        gains, gains_far, speed_far, pack_up, pack_down, got_up, got_down, edge, edge_far,
        lon_pack, got_left, got_right, lon_far, far_left, far_right, cols_far, part, parts,
        load_sem, small_sem, raw_send, raw_recv, lat_send, lat_recv, lon_send, lon_recv,
        part_send, part_recv,
    ) = refs
    n_lat, n_lon, n_freq, nf, nd, rows, nbins = sizes
    half = nd // 2
    pair = 2 * nd
    band = nf * nd
    pitch = round_up(pair, 16)
    pad = pitch - pair
    own_chunks = nf // 2
    far_chunks = EDGE // 2
    chunks = own_chunks + far_chunks
    window = 3 * pitch
    reach = round_up(window, LANES)
    span = lines.shape[1]
    places = spread(nf)
    groups = pair // 8
    cosines, sines = angles
    li, lo, fi = lax.axis_index("lat"), lax.axis_index("lon"), lax.axis_index("freq")
    other = 1 - fi
    first = far_chunks * fi
    far_first = own_chunks * other

    own_rows = pl.multiple_of(first * (pair * rows), 8)
    load = pltpu.make_async_copy(spectrum, x.at[pl.ds(own_rows, band * rows)], load_sem)
    load.start()
    small = [
        pltpu.make_async_copy(a, b, small_sem.at[i])
        for i, (a, b) in enumerate(zip(sources, inputs))
    ]
    for copy in small:
        copy.start()

    east, west = lax.rem(lo + 1, n_lon), lax.rem(lo + n_lon - 1, n_lon)
    group = []
    for s in range(1, n_lat * n_freq):
        dl, df = divmod(s, n_freq)
        group.append(
            (dl, {"lat": lax.rem(li + dl, n_lat), "freq": lax.rem(fi + df, n_freq)})
        )
    barrier = pltpu.get_barrier_semaphore()
    peers = [{"lon": east}, {"lon": west}]
    peers += [{"lon": east, "freq": other}, {"lon": west, "freq": other}]
    peers += [g for _, g in group]
    for peer in peers:
        pl.semaphore_signal(barrier, inc=1, device_id=peer, device_id_type=MESH)

    packed = pack_up.shape[0]
    far_lat = EDGE * half
    up_ok, down_ok = li < n_lat - 1, li > 0

    def raw_copy():
        count = EDGE * nd * rows
        src = pl.multiple_of(other * ((nf - EDGE) * nd * rows), 8)
        dst = pl.multiple_of(fi * (band * rows), 8)
        return pltpu.make_async_remote_copy(
            spectrum.at[pl.ds(src, count)], x.at[pl.ds(dst, count)],
            raw_send.at[0], raw_recv.at[0], device_id={"freq": other}, device_id_type=MESH,
        )

    def speed_copy():
        return pltpu.make_async_remote_copy(
            sources[0], speed_far, raw_send.at[1], raw_recv.at[1],
            device_id={"freq": other}, device_id_type=MESH,
        )

    def lat_copy(up):
        src, dst = (pack_up, got_up) if up else (pack_down, got_down)
        i = int(up)
        return pltpu.make_async_remote_copy(
            src, dst.at[pl.ds(far_lat, packed)], lat_send.at[i], lat_recv.at[i],
            device_id={"lat": li + 1 if up else li - 1}, device_id_type=MESH,
        )

    def lat_far_copy(up):
        src, dst = (pack_up, got_up) if up else (pack_down, got_down)
        i = 2 + int(up)
        return pltpu.make_async_remote_copy(
            src.at[pl.ds(pl.multiple_of(other * far_lat, 8), far_lat)], dst.at[pl.ds(0, far_lat)],
            lat_send.at[i], lat_recv.at[i],
            device_id={"lat": li + 1 if up else li - 1, "freq": other}, device_id_type=MESH,
        )

    def lon_copy(to_east):
        i = int(to_east)
        return pltpu.make_async_remote_copy(
            lon_pack, got_left if to_east else got_right, lon_send.at[i], lon_recv.at[i],
            device_id={"lon": east if to_east else west}, device_id_type=MESH,
        )

    def lon_far_copy(to_east):
        i = 2 + int(to_east)
        return pltpu.make_async_remote_copy(
            lon_far, far_left if to_east else far_right, lon_send.at[i], lon_recv.at[i],
            device_id={"lon": east if to_east else west, "freq": other}, device_id_type=MESH,
        )

    def part_copy(s):
        return pltpu.make_async_remote_copy(
            part, parts.at[s], part_send.at[s], part_recv.at[s],
            device_id=group[s][1], device_id_type=MESH,
        )

    def signs(values, j):
        return [bool(values[(8 * j + i) % nd] > 0.0) for i in range(8)]

    eight = lax.broadcasted_iota(jnp.int32, (8, LANES), 0)
    lane = lax.broadcasted_iota(jnp.int32, (8, LANES), 1)

    def rows_of(flags):
        spot = None
        for i, flag in enumerate(flags):
            if flag:
                here = eight == i
                spot = here if spot is None else jnp.logical_or(spot, here)
        return spot

    def choose(flags, yes, no):
        if all(flags):
            return yes()
        if not any(flags):
            return no()
        return jnp.where(rows_of(flags), yes(), no())

    forward = [signs(cosines, j) for j in range(groups)]
    southern = [[(8 * j + i) % nd < half for i in range(8)] for j in range(groups)]

    pack_up[pl.ds(packed - 8, 8), :] = jnp.zeros((8, LANES), F32)
    pack_down[pl.ds(packed - 8, 8), :] = jnp.zeros((8, LANES), F32)
    load.wait()
    for f in range(nf):
        at = half * places[f]
        base = own_rows + nd * f * rows
        pack_up[pl.ds(at, half), :] = x[pl.ds(base + rows - 1, half, stride=rows), :]
        pack_down[pl.ds(at, half), :] = x[pl.ds(base + half * rows, half, stride=rows), :]

    step = 3 if own_chunks % 3 == 0 else 1

    def pack_step(t, acc):
        acc = list(acc)
        for u in range(step):
            c = t * step + u + first
            base = pl.multiple_of(c * (pair * rows), 8)
            for r in range(rows):
                k = c * rows + r
                for j in range(groups):
                    e = x[pl.ds(base + 8 * rows * j + r, 8, stride=rows), :]
                    z = choose(
                        forward[j],
                        lambda: jnp.where(lane == LANES - 1, e, 0.0),
                        lambda: jnp.where(lane == 0, e, 0.0),
                    )
                    acc[j] = acc[j] + pltpu.roll(z, k, 1)
        return tuple(acc)

    sums = lax.fori_loop(
        0, own_chunks // step, pack_step, tuple(jnp.zeros((8, LANES), F32) for _ in range(groups))
    )
    for j in range(groups):
        aligned = choose(forward[j], lambda: pltpu.roll(sums[j], 1, 1), lambda: sums[j])
        lon_pack[8 * j : 8 * j + 8, :] = aligned
    begin = (first + (own_chunks - far_chunks) * other) * rows
    whole = jnp.concatenate(
        [lon_pack[...], jnp.zeros((LANES - pair, LANES), F32)], axis=0
    )
    turned = pltpu.roll(whole, lax.rem(LANES - begin, LANES), 1).T
    lon_far[...] = turned[0:8, :]

    pl.semaphore_wait(barrier, len(peers))
    raw_copy().start()
    speed_copy().start()
    lon_copy(True).start()
    lon_copy(False).start()

    @pl.when(up_ok)
    def _():
        lat_copy(True).start()
        lat_far_copy(True).start()

    @pl.when(down_ok)
    def _():
        lat_copy(False).start()
        lat_far_copy(False).start()

    lon_far_copy(True).start()
    lon_far_copy(False).start()

    @pl.when(jnp.logical_not(down_ok))
    def _():
        got_up[...] = jnp.zeros_like(got_up)

    @pl.when(jnp.logical_not(up_ok))
    def _():
        got_down[...] = jnp.zeros_like(got_down)

    for ref in (mh, ml, th, tl):
        for at in (0, (chunks + 1) * pitch):
            ref[pl.ds(at, pitch), :] = jnp.zeros((pitch, ref.shape[1]), BF16)
    for copy in small:
        copy.wait()
    rates[...] = jnp.zeros_like(rates)
    rates[0:1, 0:nf] = speed[...].reshape(1, nf)
    gains[...] = jnp.broadcast_to(
        pltpu.roll(rates[...], EDGE * fi, 1).T[0 : gains.shape[0], 0:1], gains.shape
    )
    bin0 = fi * ((nf - EDGE) * nd)
    lines[...] = jnp.zeros_like(lines)
    target = (quad[...] - bin0).astype(F32)
    shift = jnp.zeros_like(target)
    for i in range(1, chunks):
        shift = shift + jnp.where(target >= float(pair * i), float(pad), 0.0)
    lines[0:2, 0:nbins] = target + shift
    lines[2:3, 0:nbins] = time_step * coef[...].reshape(1, nbins)
    weight = profile[...].reshape(1, nbins)
    lines[3:4, 0:nbins] = weight
    lines[4:6, 0:nbins] = momentum[...] * weight
    lines[...] = pltpu.roll(lines[...], lax.rem(span - bin0, span), 1)
    cols[...] = jnp.full_like(cols, -1.0)
    for k in range(-(-chunks * pair // LANES)):
        block = lines[:, LANES * k : LANES * k + LANES].T
        at = LANES * k
        while at < min(LANES * (k + 1), chunks * pair):
            c = at // pair
            stop = min(pair * (c + 1), LANES * (k + 1))
            cols[at + pad * c : stop + pad * c, :] = block[at - LANES * k : stop - LANES * k]
            at = stop
    for k in range(span // LANES):
        lines[:, LANES * k : LANES * k + LANES] = cols[LANES * k : LANES * k + LANES, :].T
    turned = waves[...].T
    table[pl.ds(0, pair), :] = jnp.broadcast_to(turned[0:pair, 0:1], (pair, LANES))
    table[pl.ds(pair, pair), :] = jnp.broadcast_to(turned[0:pair, 1:2], (pair, LANES))

    lanes = lax.broadcasted_iota(jnp.int32, (pitch, reach), 1)
    below = lax.broadcasted_iota(jnp.int32, (pitch, reach), 0)
    own_bin = lanes == below + pitch

    def build(c, carry):
        at = pl.multiple_of(pitch * c, 8)
        where = (lanes + (at - pitch)).astype(F32)
        for i in range(2):
            chosen = jnp.where(cols[pl.ds(at, pitch), i : i + 1] == where, 1.0, 0.0)
            pick[pl.ds(pl.multiple_of(2 * at + pitch * i, 16), pitch), :] = chosen.astype(BF16)
        row = (below + at).astype(F32)
        line = pltpu.roll(lines[...], lax.rem(span + pitch - at, span), 1)
        given = jnp.where(own_bin, -2.0, 0.0)
        for i in range(2):
            given = given + jnp.where(line[i : i + 1, :reach] == row, 1.0, 0.0)
        put[pl.ds(pl.multiple_of(at, 16), pitch), :] = given.astype(BF16)
        for i, ref in enumerate((coefs, shapes, weight0, weight1)):
            ref[pl.ds(at, pitch), :] = jnp.broadcast_to(
                cols[pl.ds(at, pitch), 2 + i : 3 + i], (pitch, LANES)
            )
        mf[pl.ds(at + pair, pad), :] = jnp.zeros((pad, mf.shape[1]), F32)
        return carry

    lax.fori_loop(0, chunks, build, 0)
    sea = mask[...].astype(F32)

    def propagate(c, outer, gain, halo, sums):
        base = pl.multiple_of(c * (pair * rows), 8)
        at = pl.multiple_of(c * pitch, 16)
        store = pl.multiple_of(c * pitch + pitch, 16)
        sums = list(sums)
        held = {}
        for j in range(groups):
            low, high = 8 * j < nd, 8 * j + 8 > nd
            if low and high:
                g = jnp.where(eight < nd - 8 * j, gain[0], gain[1])
            else:
                g = jnp.broadcast_to(gain[0] if low else gain[1], (8, LANES))
            ax = g * table[8 * j : 8 * j + 8, :]
            ay = g * table[pair + 8 * j : pair + 8 * j + 8, :]
            stay = 1.0 - ax - ay
            e = [x[pl.ds(base + 8 * rows * j + r, 8, stride=rows), :] for r in range(rows)]
            if sums:
                w0, w1 = weight0[pl.ds(at + 8 * j, 8), :], weight1[pl.ds(at + 8 * j, 8), :]
            for r in range(rows):
                rim = lane == choose(forward[j], lambda: 0, lambda: LANES - 1)
                nx = choose(
                    forward[j],
                    lambda: pltpu.roll(e[r], 1, 1),
                    lambda: pltpu.roll(e[r], LANES - 1, 1),
                )
                nx = jnp.where(rim, halo(r, j), nx)
                ny = choose(
                    southern[j],
                    lambda: e[r - 1] if r > 0 else outer(j),
                    lambda: e[r + 1] if r < rows - 1 else outer(j),
                )
                m = (stay * e[r] + ax * nx + ay * ny) * sea[r : r + 1, :]
                mf[pl.ds(at + 8 * j, 8), r * LANES : (r + 1) * LANES] = m
                held[j, r] = m
                if sums:
                    for i, v in enumerate((m, m * w0, m * w1)):
                        sums[3 * r + i] = sums[3 * r + i] + v
                if j % 2 == 1 or j == groups - 1:
                    start = j if j % 2 == 0 else j - 1
                    both = [held[start, r], held[j, r] if j > start else jnp.zeros_like(m)]
                    hi, lw = split(jnp.concatenate(both, axis=0))
                    mh[pl.ds(store + 8 * start, 16), r * LANES : (r + 1) * LANES] = hi
                    ml[pl.ds(store + 8 * start, 16), r * LANES : (r + 1) * LANES] = lw
        return tuple(sums)

    def interact(c, carry):
        at = pl.multiple_of(c * pitch, 16)
        lhs = pick[pl.ds(pl.multiple_of(2 * at, 16), 2 * pitch), :window]
        both = jnp.dot(lhs, mh[pl.ds(at, window), :], preferred_element_type=F32)
        both = both + jnp.dot(lhs, ml[pl.ds(at, window), :], preferred_element_type=F32)
        third, fourth = both[:pitch], both[pitch:]
        e = mf[pl.ds(at, pitch), :]
        scale = jnp.concatenate([coefs[pl.ds(at, pitch), :]] * rows, axis=1)
        product = third * fourth
        moved = (scale * e) * (e * (third + fourth) - (product + product))
        hi, lw = split(moved)
        to = pl.multiple_of(at + pitch, 16)
        th[pl.ds(to, pitch), :] = hi
        tl[pl.ds(to, pitch), :] = lw
        return carry

    def finish(c, carry):
        at = pl.multiple_of(c * pitch, 16)
        lhs = put[pl.ds(at, pitch), :window]
        back = jnp.dot(lhs, th[pl.ds(at, window), :], preferred_element_type=F32)
        back = back + jnp.dot(lhs, tl[pl.ds(at, window), :], preferred_element_type=F32)
        shape = shapes[pl.ds(at, pair), :]
        to = (c - first) * (pair * rows)
        for r in range(rows):
            here = slice(r * LANES, (r + 1) * LANES)
            e = mf[pl.ds(at, pair), here]
            growth = 1.0 + shape * (time_step * wind[r : r + 1, :])
            result[pl.ds(to + r, pair, stride=rows), :] = e * growth + back[:pair, here]
        return carry

    def receive(ref, first_row, where):
        for i in range(len(where)):
            at = first_row + half * where[i]
            ref[pl.ds(nd * i, half), :] = got_up[pl.ds(at, half), :]
            ref[pl.ds(nd * i + half, half), :] = got_down[pl.ds(at, half), :]

    @pl.when(down_ok)
    def _():
        lat_copy(True).wait_recv()

    @pl.when(up_ok)
    def _():
        lat_copy(False).wait_recv()

    receive(edge, far_lat, [places[f] for f in range(nf)])
    lon_copy(True).wait_recv()
    lon_copy(False).wait_recv()
    for j in range(groups):
        here = slice(8 * j, 8 * j + 8)
        got_left[here, :] = choose(
            forward[j],
            lambda: got_left[here, :],
            lambda: pltpu.roll(got_right[here, :], LANES - 1, 1),
        )

    def own(c, sums):
        def halo(r, j):
            return pltpu.roll(got_left[8 * j : 8 * j + 8, :], LANES - (c * rows + r), 1)

        def outer(j):
            return edge[pl.ds(pl.multiple_of((c - first) * pair, 8) + 8 * j, 8), :]

        gain = [gains[pl.ds(2 * c + i, 1), :] for i in range(2)]
        return propagate(c, outer, gain, halo, sums)

    sums = tuple(jnp.zeros((8, LANES), F32) for _ in range(3 * rows))
    sums = lax.fori_loop(first, first + own_chunks, own, sums)

    all_rows = n_lat * rows
    part[pl.ds(0, 8), :] = jnp.zeros((8, LANES), F32)
    ids = (lo * LANES + lax.broadcasted_iota(jnp.int32, (all_rows, LANES), 1)) * all_rows
    ids = ids + lax.broadcasted_iota(jnp.int32, (all_rows, LANES), 0)
    totals = [jnp.zeros((all_rows, LANES), F32) for _ in range(2)]
    for r in range(rows):
        part[r : r + 1, :] = jnp.sum(sums[3 * r], axis=0, keepdims=True)
        hit = cells[r : r + 1, :] == ids
        for i in range(2):
            tau = wind[r : r + 1, :] * jnp.sum(sums[3 * r + 1 + i], axis=0, keepdims=True)
            totals[i] = totals[i] + jnp.where(hit, tau, 0.0)
    for i in range(2):
        part[pl.ds(8 + i * all_rows, all_rows), :] = totals[i]
    for s in range(len(group)):
        part_copy(s).start()

    lax.fori_loop(
        2 * first - fi, chunks - far_chunks - 1 + fi * (far_chunks + 1), interact, 0
    )
    lax.fori_loop(2 * first, chunks - 2 * far_chunks + fi * 2 * far_chunks, finish, 0)

    for s in range(len(group)):
        part_copy(s).wait()
    en = part[pl.ds(0, 8), :]
    st = part[pl.ds(8, 2 * all_rows), :]
    for s, (dl, _) in enumerate(group):
        if dl == 0:
            en = en + parts[s, pl.ds(0, 8), :]
        st = st + parts[s, pl.ds(8, 2 * all_rows), :]
    loss = time_step * dissip[...] * (en[0:rows] / nbins)
    share = (LANES // n_freq) * all_rows
    cell = lax.broadcasted_iota(jnp.int32, (LANES, share), 1)
    first_cell = (lax.broadcasted_iota(jnp.int32, (LANES, share), 0) - fi * (LANES // n_freq)) * all_rows
    inside = jnp.logical_and(cell >= first_cell, cell < first_cell + all_rows)
    wide = jnp.dot(
        st, jnp.where(inside, 1.0, 0.0),
        precision=lax.Precision.HIGHEST, preferred_element_type=F32,
    )
    place = lax.broadcasted_iota(jnp.int32, (all_rows, share), 1) & (all_rows - 1)
    own_row = place == lax.broadcasted_iota(jnp.int32, (all_rows, share), 0)
    for i in range(2):
        picked = jnp.where(own_row, wide[i * all_rows : (i + 1) * all_rows], 0.0)
        stress[i : i + 1, :] = jnp.sum(picked, axis=0, keepdims=True)

    speed_copy().wait_recv()
    rates[0:1, 0:nf] = speed_far[...].reshape(1, nf)
    gains_far[...] = jnp.broadcast_to(
        pltpu.roll(rates[...], fi * (LANES - (nf - EDGE)), 1).T[0:8, 0:1], gains_far.shape
    )

    @pl.when(down_ok)
    def _():
        lat_far_copy(True).wait_recv()

    @pl.when(up_ok)
    def _():
        lat_far_copy(False).wait_recv()

    receive(edge_far, 0, list(range(EDGE)))
    lon_far_copy(True).wait_recv()
    lon_far_copy(False).wait_recv()
    left, right = far_left[...].T, far_right[...].T
    for j in range(groups):
        here = slice(8 * j, 8 * j + 8)
        ahead = eight[:, 0:8] < 0
        for i, flag in enumerate(forward[j]):
            if flag:
                ahead = jnp.logical_or(ahead, eight[:, 0:8] == i)
        cols_far[here, :] = jnp.where(ahead, left[here], right[here])
    raw_copy().wait_recv()

    for u in range(far_chunks):
        def halo(r, j):
            k = u * rows + r
            return jnp.broadcast_to(cols_far[8 * j : 8 * j + 8, k : k + 1], (8, LANES))

        def outer(j):
            return edge_far[pair * u + 8 * j : pair * u + 8 * j + 8, :]

        gain = [gains_far[2 * u + i : 2 * u + i + 1, :] for i in range(2)]
        propagate(far_first + u, outer, gain, halo, ())

    late = (chunks - far_chunks - 1) * other + fi
    lax.fori_loop(late, late + 2, interact, 0)
    late = (chunks - 2 * far_chunks) * other + fi * far_chunks
    lax.fori_loop(late, late + 2, finish, 0)

    def settle(t, carry):
        at = pl.multiple_of((t + first) * pitch, 8)
        for r in range(rows):
            spot = pl.ds(t * (pair * rows) + r, pair, stride=rows)
            e = mf[pl.ds(at, pair), r * LANES : (r + 1) * LANES]
            result[spot, :] = result[spot, :] - e * loss[r : r + 1, :]
        return carry

    lax.fori_loop(0, own_chunks, settle, 0)

    raw_copy().wait_send()
    speed_copy().wait_send()
    for flag in (True, False):
        lon_copy(flag).wait_send()
        lon_far_copy(flag).wait_send()

    @pl.when(up_ok)
    def _():
        lat_copy(True).wait_send()
        lat_far_copy(True).wait_send()

    @pl.when(down_ok)
    def _():
        lat_copy(False).wait_send()
        lat_far_copy(False).wait_send()


def write_kernel(result, stress, result_out, stress_out, sems):
    pieces = sems.shape[0] - 1
    size = result.shape[0] // pieces
    copies = [pltpu.make_async_copy(stress, stress_out, sems.at[pieces])]
    for i in range(pieces):
        here = pl.ds(size * i, size)
        copies.append(pltpu.make_async_copy(result.at[here], result_out.at[here], sems.at[i]))
    for copy in copies:
        copy.start()
    for copy in copies:
        copy.wait()


def local(
    axes,
    spectrum,
    group_speed,
    sea_mask,
    wind_growth,
    dissipation,
    wind_profile,
    nonlinear_coef,
    momentum,
    quadruplet,
    ocean_cell,
):
    n_lat, n_lon, n_freq = axes
    nf, nd, rows, width = spectrum.shape
    nbins = wind_profile.shape[0]
    assert n_freq == 2 and nf % 2 == 0 and width == LANES
    band, pair, half = nf * nd, 2 * nd, nd // 2
    pitch = round_up(pair, 16)
    chunks = nf // 2 + EDGE // 2
    all_rows = n_lat * rows
    angles = (np.float32(2.0 * np.pi) * np.arange(nd, dtype=np.float32) / np.float32(nd)).astype(
        np.float32
    )
    cosines, sines = np.cos(angles), np.sin(angles)
    waves = np.zeros((8, LANES), np.float32)
    waves[0, :pair], waves[1, :pair] = np.tile(np.abs(cosines), 2), np.tile(np.abs(sines), 2)

    packed = round_up(nf * half, 8)
    far_lat = EDGE * half
    peers = n_lat * n_freq - 1
    small = 8 + 2 * all_rows
    share = (width // n_freq) * all_rows
    span = round_up(max(nbins, (chunks + 2) * pitch), LANES)
    reach = round_up(3 * pitch, LANES)
    vmem = pl.BlockSpec(memory_space=VMEM)
    hbm = pl.BlockSpec(memory_space=pltpu.HBM)
    sizes = (n_lat, n_lon, n_freq, nf, nd, rows, nbins)
    dma = pltpu.SemaphoreType.DMA
    smalls = (
        group_speed,
        jnp.asarray(waves),
        wind_profile,
        nonlinear_coef,
        momentum,
        quadruplet,
        sea_mask,
        wind_growth,
        dissipation,
        ocean_cell,
    )
    out, ocean = pl.pallas_call(
        functools.partial(wave_kernel, sizes, (cosines, sines)),
        out_shape=(
            jax.ShapeDtypeStruct((band * rows, width), F32),
            jax.ShapeDtypeStruct((2, share), F32),
        ),
        in_specs=[hbm] * 11,
        out_specs=(vmem, vmem),
        scratch_shapes=[VMEM(a.shape, a.dtype) for a in smalls]
        + [
            VMEM((chunks * pair * rows, width), F32),
            VMEM((chunks * pitch, rows * width), F32),
            VMEM(((chunks + 2) * pitch, rows * width), BF16),
            VMEM(((chunks + 2) * pitch, rows * width), BF16),
            VMEM(((chunks + 2) * pitch, rows * width), BF16),
            VMEM(((chunks + 2) * pitch, rows * width), BF16),
            VMEM((2 * chunks * pitch, reach), BF16),
            VMEM((chunks * pitch, reach), BF16),
            VMEM((2 * pair, width), F32),
            VMEM((8, width), F32),
            VMEM((span, 8), F32),
            VMEM((8, span), F32),
            VMEM((chunks * pitch, width), F32),
            VMEM((chunks * pitch, width), F32),
            VMEM((chunks * pitch, width), F32),
            VMEM((chunks * pitch, width), F32),
            VMEM((round_up(nf + EDGE, 8), width), F32),
            VMEM((8, width), F32),
            VMEM(group_speed.shape, F32),
            VMEM((packed, width), F32),
            VMEM((packed, width), F32),
            VMEM((far_lat + packed, width), F32),
            VMEM((far_lat + packed, width), F32),
            VMEM((band, width), F32),
            VMEM((EDGE * nd, width), F32),
            VMEM((pair, width), F32),
            VMEM((pair, width), F32),
            VMEM((pair, width), F32),
            VMEM((8, width), F32),
            VMEM((8, width), F32),
            VMEM((8, width), F32),
            VMEM((pair, 8), F32),
            VMEM((small, width), F32),
            VMEM((peers, small, width), F32),
            dma, dma((len(smalls),)),
            dma((2,)), dma((2,)), dma((4,)), dma((4,)), dma((4,)), dma((4,)),
            dma((peers,)), dma((peers,)),
        ],
        compiler_params=pltpu.CompilerParams(
            collective_id=0, has_side_effects=True, vmem_limit_bytes=32 << 20
        ),
    )(
        *[
            pltpu.with_memory_space_constraint(a, pltpu.HBM)
            for a in (spectrum.reshape(band * rows, width), *smalls)
        ]
    )
    out, ocean = pl.pallas_call(
        write_kernel,
        out_shape=(
            jax.ShapeDtypeStruct((band * rows, width), F32),
            jax.ShapeDtypeStruct((2, share), F32),
        ),
        in_specs=[vmem, vmem],
        out_specs=(hbm, hbm),
        scratch_shapes=[dma((5,))],
        compiler_params=pltpu.CompilerParams(vmem_limit_bytes=1 << 20),
    )(out, ocean)
    return out.reshape(spectrum.shape), ocean.T


def solution(mesh):
    axes = tuple(mesh.shape[a] for a in ("lat", "lon", "freq"))
    return jax.shard_map(
        functools.partial(local, axes),
        mesh=mesh,
        in_specs=(
            P("freq", None, "lat", "lon"),
            P("freq"),
            P("lat", "lon"),
            P("lat", "lon"),
            P("lat", "lon"),
            P(),
            P(),
            P(),
            P(),
            P("lat", "lon"),
        ),
        out_specs=(P("freq", None, "lat", "lon"), P(("lon", "freq"), None)),
        check_vma=False,
    )
```

```python
import functools

import jax
import jax.numpy as jnp
import numpy as np
from jax import lax
from jax.experimental import pallas as pl
from jax.experimental.pallas import tpu as pltpu
from jax.sharding import PartitionSpec as P

time_step = 0.5
MESH = pl.DeviceIdType.MESH
VMEM = pltpu.VMEM
LANES = 128
EDGE = 4
F32, BF16 = jnp.float32, jnp.bfloat16


def spread(nf):
    order = list(range(EDGE)) + list(range(nf - EDGE, nf)) + list(range(EDGE, nf - EDGE))
    return {f: i for i, f in enumerate(order)}


def round_up(n, m):
    return -(-n // m) * m


def split(v):
    high = v.astype(BF16)
    return high, (v - high.astype(F32)).astype(BF16)


def thirds(v):
    high, low = split(v)
    rest = v - high.astype(F32) - low.astype(F32)
    return high, low, rest.astype(BF16)


def wave_kernel(sizes, angles, spectrum, *refs):
    sources, refs = refs[:10], refs[10:]
    result, stress, *refs = refs
    inputs, refs = refs[:10], refs[10:]
    speed, waves, profile, coef, momentum, quad, mask, wind, dissip, cells = inputs
    (
        x, mf, mh, ml, th, tl, pick, put, table, rates, cols, lines, coefs, shapes, weight0, weight1,
        gains, gains_far, speed_far, pack_up, pack_down, got_up, got_down, edge, edge_far,
        lon_pack, got_left, got_right, lon_far, far_left, far_right, cols_far, spread_out, energy, energy_got, tau_own, taus,
        load_sem, small_sem, ready_sem, raw_send, raw_recv, lat_send, lat_recv, lon_send, lon_recv,
        sum_send, sum_recv, tau_send, tau_recv,
    ) = refs
    n_lat, n_lon, n_freq, nf, nd, rows, nbins = sizes
    half = nd // 2
    pair = 2 * nd
    band = nf * nd
    all_rows = n_lat * rows
    pitch = round_up(pair, 16)
    pad = pitch - pair
    own_chunks = nf // 2
    far_chunks = EDGE // 2
    chunks = own_chunks + far_chunks
    window = 3 * pitch
    reach = round_up(window, LANES)
    span = lines.shape[1]
    places = spread(nf)
    groups = pair // 8
    cosines, sines = angles
    li, lo, fi = lax.axis_index("lat"), lax.axis_index("lon"), lax.axis_index("freq")
    other = 1 - fi
    first = far_chunks * fi
    far_first = own_chunks * other

    own_rows = pl.multiple_of(first * (pair * rows), 8)
    small = [
        pltpu.make_async_copy(a, b, small_sem.at[i])
        for i, (a, b) in enumerate(zip(sources, inputs))
    ]
    step = 3 if own_chunks % 3 == 0 else 1
    loads = []
    for i in range(own_chunks // step):
        count = step * pair * rows
        loads.append(
            pltpu.make_async_copy(
                spectrum.at[pl.ds(i * count, count)], x.at[pl.ds(own_rows + i * count, count)],
                load_sem.at[i],
            )
        )
    for copy in loads + small:
        copy.start()

    east, west = lax.rem(lo + 1, n_lon), lax.rem(lo + n_lon - 1, n_lon)
    group = []
    for s in range(1, n_lat * n_freq):
        dl, df = divmod(s, n_freq)
        group.append({"lat": lax.rem(li + dl, n_lat), "freq": lax.rem(fi + df, n_freq)})
    barrier = pltpu.get_barrier_semaphore()
    beside = [{"lon": east}, {"lon": west}]
    beside += [{"lon": east, "freq": other}, {"lon": west, "freq": other}]
    odd = lax.rem(lo, 2)
    for peer in group:
        pl.semaphore_signal(barrier, inc=1, device_id=peer, device_id_type=MESH)

    @pl.when(odd == 0)
    def _():
        for peer in beside:
            pl.semaphore_signal(barrier, inc=1, device_id=peer, device_id_type=MESH)

    packed = pack_up.shape[0]
    far_lat = EDGE * half
    up_ok, down_ok = li < n_lat - 1, li > 0

    def raw_copy(near):
        count = EDGE // 2 * nd * rows
        half_at = (other if near else fi) * count
        src = pl.multiple_of(other * ((nf - EDGE) * nd * rows) + half_at, 8)
        dst = pl.multiple_of(fi * (band * rows) + half_at, 8)
        i = 2 if near else 0
        return pltpu.make_async_remote_copy(
            spectrum.at[pl.ds(src, count)], x.at[pl.ds(dst, count)],
            raw_send.at[i], raw_recv.at[i], device_id={"freq": other}, device_id_type=MESH,
        )

    def speed_copy():
        return pltpu.make_async_remote_copy(
            sources[0], speed_far, raw_send.at[1], raw_recv.at[1],
            device_id={"freq": other}, device_id_type=MESH,
        )

    def lat_copy(up):
        src, dst = (pack_up, got_up) if up else (pack_down, got_down)
        i = int(up)
        return pltpu.make_async_remote_copy(
            src, dst.at[pl.ds(far_lat, packed)], lat_send.at[i], lat_recv.at[i],
            device_id={"lat": li + 1 if up else li - 1}, device_id_type=MESH,
        )

    def lat_far_copy(up):
        src, dst = (pack_up, got_up) if up else (pack_down, got_down)
        i = 2 + int(up)
        return pltpu.make_async_remote_copy(
            src.at[pl.ds(pl.multiple_of(other * far_lat, 8), far_lat)], dst.at[pl.ds(0, far_lat)],
            lat_send.at[i], lat_recv.at[i],
            device_id={"lat": li + 1 if up else li - 1, "freq": other}, device_id_type=MESH,
        )

    def lon_copy(to_east):
        i = int(to_east)
        return pltpu.make_async_remote_copy(
            lon_pack, got_left if to_east else got_right, lon_send.at[i], lon_recv.at[i],
            device_id={"lon": east if to_east else west}, device_id_type=MESH,
        )

    def lon_far_copy(to_east):
        i = 2 + int(to_east)
        return pltpu.make_async_remote_copy(
            lon_far, far_left if to_east else far_right, lon_send.at[i], lon_recv.at[i],
            device_id={"lon": east if to_east else west, "freq": other}, device_id_type=MESH,
        )

    def energy_copy():
        return pltpu.make_async_remote_copy(
            energy, energy_got, sum_send.at[0], sum_recv.at[0],
            device_id={"freq": other}, device_id_type=MESH,
        )

    def tau_copy(s):
        return pltpu.make_async_remote_copy(
            tau_own, taus.at[s], tau_send.at[s], tau_recv.at[s],
            device_id=group[s], device_id_type=MESH,
        )

    def signs(values, j):
        return [bool(values[(8 * j + i) % nd] > 0.0) for i in range(8)]

    eight = lax.broadcasted_iota(jnp.int32, (8, LANES), 0)
    lane = lax.broadcasted_iota(jnp.int32, (8, LANES), 1)

    def rows_of(flags):
        spot = None
        for i, flag in enumerate(flags):
            if flag:
                here = eight == i
                spot = here if spot is None else jnp.logical_or(spot, here)
        return spot

    def choose(flags, yes, no):
        if all(flags):
            return yes()
        if not any(flags):
            return no()
        return jnp.where(rows_of(flags), yes(), no())

    forward = [signs(cosines, j) for j in range(groups)]
    southern = [[(8 * j + i) % nd < half for i in range(8)] for j in range(groups)]

    pack_up[pl.ds(packed - 8, 8), :] = jnp.zeros((8, LANES), F32)
    pack_down[pl.ds(packed - 8, 8), :] = jnp.zeros((8, LANES), F32)
    sums = [jnp.zeros((8, LANES), F32) for _ in range(groups)]
    for i, copy in enumerate(loads):
        if i == len(loads) - 1:
            pl.semaphore_wait(barrier, len(group) + odd * len(beside))
            speed_copy().start()
            raw_copy(True).start()
        copy.wait()
        for f in range(2 * step * i, 2 * step * (i + 1)):
            at = half * places[f]
            base = own_rows + nd * f * rows
            pack_up[pl.ds(at, half), :] = x[pl.ds(base + rows - 1, half, stride=rows), :]
            pack_down[pl.ds(at, half), :] = x[pl.ds(base + half * rows, half, stride=rows), :]
        for u in range(step):
            c = i * step + u + first
            base = pl.multiple_of(c * (pair * rows), 8)
            for r in range(rows):
                k = c * rows + r
                for j in range(groups):
                    e = x[pl.ds(base + 8 * rows * j + r, 8, stride=rows), :]
                    z = choose(
                        forward[j],
                        lambda: jnp.where(lane == LANES - 1, e, 0.0),
                        lambda: jnp.where(lane == 0, e, 0.0),
                    )
                    sums[j] = sums[j] + pltpu.roll(z, k, 1)

    for j in range(groups):
        aligned = choose(forward[j], lambda: pltpu.roll(sums[j], 1, 1), lambda: sums[j])
        lon_pack[8 * j : 8 * j + 8, :] = aligned

    begin = (first + (own_chunks - far_chunks) * other) * rows
    whole = jnp.concatenate(
        [lon_pack[...], jnp.zeros((LANES - pair, LANES), F32)], axis=0
    )
    turned = pltpu.roll(whole, lax.rem(LANES - begin, LANES), 1).T
    lon_far[...] = turned[0:8, :]

    @pl.when(up_ok)
    def _():
        lat_copy(True).start()

    @pl.when(down_ok)
    def _():
        lat_copy(False).start()

    @pl.when(up_ok)
    def _():
        lat_far_copy(True).start()

    @pl.when(down_ok)
    def _():
        lat_far_copy(False).start()

    raw_copy(False).start()

    @pl.when(odd == 1)
    def _():
        for peer in beside:
            pl.semaphore_signal(ready_sem, inc=1, device_id=peer, device_id_type=MESH)
        for to_east in (True, False):
            lon_copy(to_east).start()
            lon_far_copy(to_east).start()

    for copy in small:
        copy.wait()
    rates[...] = jnp.zeros_like(rates)
    rates[0:1, 0:nf] = speed[...].reshape(1, nf)
    gains[...] = jnp.broadcast_to(
        pltpu.roll(rates[...], EDGE * fi, 1).T[0 : gains.shape[0], 0:1], gains.shape
    )
    bin0 = fi * ((nf - EDGE) * nd)
    lines[...] = jnp.zeros_like(lines)
    target = (quad[...] - bin0).astype(F32)
    shift = jnp.zeros_like(target)
    for i in range(1, chunks):
        shift = shift + jnp.where(target >= float(pair * i), float(pad), 0.0)
    lines[0:2, 0:nbins] = target + shift
    lines[2:3, 0:nbins] = time_step * coef[...].reshape(1, nbins)
    weight = profile[...].reshape(1, nbins)
    lines[3:4, 0:nbins] = weight
    lines[4:6, 0:nbins] = momentum[...] * weight
    lines[...] = pltpu.roll(lines[...], lax.rem(span - bin0, span), 1)
    cols[...] = jnp.full_like(cols, -1.0)
    for k in range(-(-chunks * pair // LANES)):
        block = lines[:, LANES * k : LANES * k + LANES].T
        at = LANES * k
        while at < min(LANES * (k + 1), chunks * pair):
            c = at // pair
            stop = min(pair * (c + 1), LANES * (k + 1))
            cols[at + pad * c : stop + pad * c, :] = block[at - LANES * k : stop - LANES * k]
            at = stop
    for k in range(span // LANES):
        lines[:, LANES * k : LANES * k + LANES] = cols[LANES * k : LANES * k + LANES, :].T
    turned = waves[...].T
    table[pl.ds(0, pair), :] = jnp.broadcast_to(turned[0:pair, 0:1], (pair, LANES))
    table[pl.ds(pair, pair), :] = jnp.broadcast_to(turned[0:pair, 1:2], (pair, LANES))

    def send_columns():
        pl.semaphore_wait(ready_sem, len(beside))
        for to_east in (True, False):
            lon_copy(to_east).start()
            lon_far_copy(to_east).start()

    @pl.when(jnp.logical_and(odd == 0, lo > 0))
    def _():
        send_columns()

    @pl.when(jnp.logical_not(down_ok))
    def _():
        got_up[...] = jnp.zeros_like(got_up)

    @pl.when(jnp.logical_not(up_ok))
    def _():
        got_down[...] = jnp.zeros_like(got_down)

    for ref in (mh, ml, th, tl):
        for at in (0, (chunks + 1) * pitch):
            ref[pl.ds(at, pitch), :] = jnp.zeros((pitch, ref.shape[1]), BF16)
    lanes = lax.broadcasted_iota(jnp.int32, (pitch, reach), 1)
    below = lax.broadcasted_iota(jnp.int32, (pitch, reach), 0)
    own_bin = lanes == below + pitch

    def build(c, carry):
        at = pl.multiple_of(pitch * c, 8)
        where = (lanes + (at - pitch)).astype(F32)
        for i in range(2):
            chosen = jnp.where(cols[pl.ds(at, pitch), i : i + 1] == where, 1.0, 0.0)
            pick[pl.ds(pl.multiple_of(2 * at + pitch * i, 16), pitch), :] = chosen.astype(BF16)
        row = (below + at).astype(F32)
        line = pltpu.roll(lines[...], lax.rem(span + pitch - at, span), 1)
        given = jnp.where(own_bin, -2.0, 0.0)
        for i in range(2):
            given = given + jnp.where(line[i : i + 1, :reach] == row, 1.0, 0.0)
        put[pl.ds(pl.multiple_of(at, 16), pitch), :] = given.astype(BF16)
        for i, ref in enumerate((coefs, shapes, weight0, weight1)):
            ref[pl.ds(at, pitch), :] = jnp.broadcast_to(
                cols[pl.ds(at, pitch), 2 + i : 3 + i], (pitch, LANES)
            )
        mf[pl.ds(at + pair, pad), :] = jnp.zeros((pad, mf.shape[1]), F32)
        return carry

    lax.fori_loop(0, chunks, build, 0)
    share = (LANES // n_freq) * all_rows
    cell = lax.broadcasted_iota(jnp.int32, (LANES, share), 1)
    first_cell = (lax.broadcasted_iota(jnp.int32, (LANES, share), 0) - fi * (LANES // n_freq)) * all_rows
    inside = jnp.logical_and(cell >= first_cell, cell < first_cell + all_rows)
    spread_out[...] = jnp.where(inside, 1.0, 0.0).astype(BF16)

    @pl.when(lo == 0)
    def _():
        send_columns()

    sea = mask[...].astype(F32)

    inner, rim_rows = list(range(1, rows - 1)), [0, rows - 1]
    slot = {r: i for i, r in enumerate(inner + rim_rows)}
    whole_cols = slice(0, rows * LANES)
    inner_cols, rim_cols = slice(0, len(inner) * LANES), slice(len(inner) * LANES, rows * LANES)

    def columns(r):
        return slice(slot[r] * LANES, slot[r] * LANES + LANES)

    def upwind(e, j):
        if all(forward[j]):
            return pltpu.roll(e, 1, 1)
        if not any(forward[j]):
            return pltpu.roll(e, LANES - 1, 1)
        at = lane + jnp.where(rows_of(forward[j]), LANES - 1, 1)
        return jnp.take_along_axis(e, at & (LANES - 1), axis=1)

    def propagate(c, outer, gain, halo, row_set, sums):
        base = pl.multiple_of(c * (pair * rows), 8)
        at = pl.multiple_of(c * pitch, 16)
        store = pl.multiple_of(c * pitch + pitch, 16)
        sums = dict(sums)
        held = {}
        for j in range(groups):
            low, high = 8 * j < nd, 8 * j + 8 > nd
            if low and high:
                g = jnp.where(eight < nd - 8 * j, gain[0], gain[1])
            else:
                g = jnp.broadcast_to(gain[0] if low else gain[1], (8, LANES))
            ax = g * table[8 * j : 8 * j + 8, :]
            ay = g * table[pair + 8 * j : pair + 8 * j + 8, :]
            stay = 1.0 - ax - ay
            e = [x[pl.ds(base + 8 * rows * j + r, 8, stride=rows), :] for r in range(rows)]
            if sums:
                w0, w1 = weight0[pl.ds(at + 8 * j, 8), :], weight1[pl.ds(at + 8 * j, 8), :]
            for r in row_set:
                rim = lane == choose(forward[j], lambda: 0, lambda: LANES - 1)
                nx = jnp.where(rim, halo(r, j), upwind(e[r], j))
                ny = choose(
                    southern[j],
                    lambda: e[r - 1] if r > 0 else outer(j),
                    lambda: e[r + 1] if r < rows - 1 else outer(j),
                )
                m = (stay * e[r] + ax * nx + ay * ny) * sea[r : r + 1, :]
                mf[pl.ds(at + 8 * j, 8), columns(r)] = m
                held[j, r] = m
                if sums:
                    for i, v in enumerate((m, m * w0, m * w1)):
                        sums[r, i] = sums[r, i] + v
                if j % 2 == 1 or j == groups - 1:
                    start = j if j % 2 == 0 else j - 1
                    both = [held[start, r], held[j, r] if j > start else jnp.zeros_like(m)]
                    hi, lw = split(jnp.concatenate(both, axis=0))
                    mh[pl.ds(store + 8 * start, 16), columns(r)] = hi
                    ml[pl.ds(store + 8 * start, 16), columns(r)] = lw
        return sums

    def interact(c, cs):
        width = (cs.stop - cs.start) // LANES
        at = pl.multiple_of(c * pitch, 16)
        lhs = pick[pl.ds(pl.multiple_of(2 * at, 16), 2 * pitch), :window]
        both = jnp.dot(lhs, mh[pl.ds(at, window), cs], preferred_element_type=F32)
        both = both + jnp.dot(lhs, ml[pl.ds(at, window), cs], preferred_element_type=F32)
        third, fourth = both[:pitch], both[pitch:]
        e = mf[pl.ds(at, pitch), cs]
        scale = jnp.concatenate([coefs[pl.ds(at, pitch), :]] * width, axis=1)
        product = third * fourth
        moved = (scale * e) * (e * (third + fourth) - (product + product))
        hi, lw = split(moved)
        to = pl.multiple_of(at + pitch, 16)
        th[pl.ds(to, pitch), cs] = hi
        tl[pl.ds(to, pitch), cs] = lw

    def finish(c, cs, loss=None):
        at = pl.multiple_of(c * pitch, 16)
        lhs = put[pl.ds(at, pitch), :window]
        back = jnp.dot(lhs, th[pl.ds(at, window), cs], preferred_element_type=F32)
        back = back + jnp.dot(lhs, tl[pl.ds(at, window), cs], preferred_element_type=F32)
        shape = shapes[pl.ds(at, pair), :]
        to = (c - first) * (pair * rows)
        for r in range(rows):
            here = columns(r)
            if here.start < cs.start or here.stop > cs.stop:
                continue
            e = mf[pl.ds(at, pair), here]
            stay = 1.0 if loss is None else 1.0 - loss[r : r + 1, :]
            growth = stay + shape * (time_step * wind[r : r + 1, :])
            gain = back[:pair, here.start - cs.start : here.stop - cs.start]
            result[pl.ds(to + r, pair, stride=rows), :] = e * growth + gain

    def run(what, begin, count, cs, at_once):
        def body(t, carry):
            for u in range(at_once):
                what(begin + t * at_once + u, cs)
            return carry

        lax.fori_loop(0, count // at_once, body, 0)
        for u in range(count - count % at_once, count):
            what(begin + u, cs)

    def receive(ref, first_row, where):
        for i in range(len(where)):
            at = first_row + half * where[i]
            ref[pl.ds(nd * i, half), :] = got_up[pl.ds(at, half), :]
            ref[pl.ds(nd * i + half, half), :] = got_down[pl.ds(at, half), :]

    lon_copy(True).wait_recv()
    lon_copy(False).wait_recv()
    for j in range(groups):
        here = slice(8 * j, 8 * j + 8)
        got_left[here, :] = choose(
            forward[j],
            lambda: got_left[here, :],
            lambda: pltpu.roll(got_right[here, :], LANES - 1, 1),
        )

    def own(row_set):
        names = [(r, i) for r in row_set for i in range(3)]

        def body(t, sums):
            sums = dict(zip(names, sums))
            for u in range(step):
                c = first + t * step + u

                def halo(r, j):
                    return pltpu.roll(got_left[8 * j : 8 * j + 8, :], LANES - (c * rows + r), 1)

                def outer(j):
                    return edge[pl.ds(pl.multiple_of((c - first) * pair, 8) + 8 * j, 8), :]

                gain = [gains[pl.ds(2 * c + i, 1), :] for i in range(2)]
                sums = propagate(c, outer, gain, halo, row_set, sums)
            return tuple(sums[n] for n in names)

        zeros = tuple(jnp.zeros((8, LANES), F32) for _ in names)
        return dict(zip(names, lax.fori_loop(0, own_chunks // step, body, zeros)))

    near_first = 2 * first - fi
    near_count = chunks - far_chunks - 1
    last_first = 2 * first
    last_count = chunks - 2 * far_chunks
    sums = own(inner)
    @pl.when(down_ok)
    def _():
        lat_copy(True).wait_recv()

    @pl.when(up_ok)
    def _():
        lat_copy(False).wait_recv()

    receive(edge, far_lat, [places[f] for f in range(nf)])
    sums.update(own(rim_rows))

    energy[...] = jnp.zeros((8, LANES), F32)
    ids = (lo * LANES + lax.broadcasted_iota(jnp.int32, (all_rows, LANES), 1)) * all_rows
    ids = ids + lax.broadcasted_iota(jnp.int32, (all_rows, LANES), 0)
    totals = [jnp.zeros((all_rows, LANES), F32) for _ in range(2)]
    for r in range(rows):
        energy[r : r + 1, :] = jnp.sum(sums[r, 0], axis=0, keepdims=True)
        hit = cells[r : r + 1, :] == ids
        for i in range(2):
            tau = wind[r : r + 1, :] * jnp.sum(sums[r, 1 + i], axis=0, keepdims=True)
            totals[i] = totals[i] + jnp.where(hit, tau, 0.0)
    for i in range(2):
        tau_own[pl.ds(i * all_rows, all_rows), :] = totals[i]
    energy_copy().start()
    for s in range(len(group)):
        tau_copy(s).start()

    run(interact, near_first, near_count, whole_cols, 4)
    run(finish, last_first, last_count, whole_cols, 4)

    speed_copy().wait_recv()
    rates[0:1, 0:nf] = speed_far[...].reshape(1, nf)
    gains_far[...] = jnp.broadcast_to(
        pltpu.roll(rates[...], fi * (LANES - (nf - EDGE)), 1).T[0:8, 0:1], gains_far.shape
    )

    @pl.when(down_ok)
    def _():
        lat_far_copy(True).wait_recv()

    @pl.when(up_ok)
    def _():
        lat_far_copy(False).wait_recv()

    receive(edge_far, 0, list(range(EDGE)))
    lon_far_copy(True).wait_recv()
    lon_far_copy(False).wait_recv()
    left, right = far_left[...].T, far_right[...].T
    for j in range(groups):
        here = slice(8 * j, 8 * j + 8)
        ahead = eight[:, 0:8] < 0
        for i, flag in enumerate(forward[j]):
            if flag:
                ahead = jnp.logical_or(ahead, eight[:, 0:8] == i)
        cols_far[here, :] = jnp.where(ahead, left[here], right[here])
    raw_copy(True).wait_recv()
    raw_copy(False).wait_recv()

    for u in range(far_chunks):
        def halo(r, j):
            k = u * rows + r
            return jnp.broadcast_to(cols_far[8 * j : 8 * j + 8, k : k + 1], (8, LANES))

        def outer(j):
            return edge_far[pair * u + 8 * j : pair * u + 8 * j + 8, :]

        gain = [gains_far[2 * u + i : 2 * u + i + 1, :] for i in range(2)]
        propagate(far_first + u, outer, gain, halo, range(rows), {})

    late = (chunks - far_chunks - 1) * other + fi
    run(interact, late, 2, whole_cols, 2)
    energy_copy().wait()
    loss = time_step * dissip[...] * ((energy[0:rows, :] + energy_got[0:rows, :]) / nbins)

    def settle(t, carry):
        at = pl.multiple_of((t + last_first) * pitch, 8)
        for r in range(rows):
            spot = pl.ds((t + last_first - first) * (pair * rows) + r, pair, stride=rows)
            e = mf[pl.ds(at, pair), columns(r)]
            result[spot, :] = result[spot, :] - e * loss[r : r + 1, :]
        return carry

    lax.fori_loop(0, last_count, settle, 0)

    late = (chunks - 2 * far_chunks) * other + fi * far_chunks
    run(functools.partial(finish, loss=loss), late, 2, whole_cols, 2)

    st = tau_own[...]
    for s in range(len(group)):
        tau_copy(s).wait()
        st = st + taus[s]
    wide = sum(
        jnp.dot(term, spread_out[...], preferred_element_type=F32) for term in thirds(st)
    )
    place = lax.broadcasted_iota(jnp.int32, (all_rows, share), 1) & (all_rows - 1)
    own_row = place == lax.broadcasted_iota(jnp.int32, (all_rows, share), 0)
    for i in range(2):
        picked = jnp.where(own_row, wide[i * all_rows : (i + 1) * all_rows], 0.0)
        stress[i : i + 1, :] = jnp.sum(picked, axis=0, keepdims=True)

    raw_copy(True).wait_send()
    raw_copy(False).wait_send()
    speed_copy().wait_send()
    for flag in (True, False):
        lon_copy(flag).wait_send()
        lon_far_copy(flag).wait_send()

    @pl.when(up_ok)
    def _():
        lat_copy(True).wait_send()
        lat_far_copy(True).wait_send()

    @pl.when(down_ok)
    def _():
        lat_copy(False).wait_send()
        lat_far_copy(False).wait_send()


def write_kernel(result, stress, result_out, stress_out, sems):
    pieces = sems.shape[0] - 1
    size = result.shape[0] // pieces
    copies = [pltpu.make_async_copy(stress, stress_out, sems.at[pieces])]
    for i in range(pieces):
        here = pl.ds(size * i, size)
        copies.append(pltpu.make_async_copy(result.at[here], result_out.at[here], sems.at[i]))
    for copy in copies:
        copy.start()
    for copy in copies:
        copy.wait()


def local(
    axes,
    spectrum,
    group_speed,
    sea_mask,
    wind_growth,
    dissipation,
    wind_profile,
    nonlinear_coef,
    momentum,
    quadruplet,
    ocean_cell,
):
    n_lat, n_lon, n_freq = axes
    nf, nd, rows, width = spectrum.shape
    nbins = wind_profile.shape[0]
    assert n_freq == 2 and nf % 2 == 0 and width == LANES
    band, pair, half = nf * nd, 2 * nd, nd // 2
    pitch = round_up(pair, 16)
    chunks = nf // 2 + EDGE // 2
    all_rows = n_lat * rows
    angles = (np.float32(2.0 * np.pi) * np.arange(nd, dtype=np.float32) / np.float32(nd)).astype(
        np.float32
    )
    cosines, sines = np.cos(angles), np.sin(angles)
    waves = np.zeros((8, LANES), np.float32)
    waves[0, :pair], waves[1, :pair] = np.tile(np.abs(cosines), 2), np.tile(np.abs(sines), 2)

    packed = round_up(nf * half, 8)
    far_lat = EDGE * half
    share = (width // n_freq) * all_rows
    span = round_up(max(nbins, (chunks + 2) * pitch), LANES)
    reach = round_up(3 * pitch, LANES)
    vmem = pl.BlockSpec(memory_space=VMEM)
    hbm = pl.BlockSpec(memory_space=pltpu.HBM)
    sizes = (n_lat, n_lon, n_freq, nf, nd, rows, nbins)
    dma = pltpu.SemaphoreType.DMA
    smalls = (
        group_speed,
        jnp.asarray(waves),
        wind_profile,
        nonlinear_coef,
        momentum,
        quadruplet,
        sea_mask,
        wind_growth,
        dissipation,
        ocean_cell,
    )
    out, ocean = pl.pallas_call(
        functools.partial(wave_kernel, sizes, (cosines, sines)),
        out_shape=(
            jax.ShapeDtypeStruct((band * rows, width), F32),
            jax.ShapeDtypeStruct((2, share), F32),
        ),
        in_specs=[hbm] * 11,
        out_specs=(vmem, vmem),
        scratch_shapes=[VMEM(a.shape, a.dtype) for a in smalls]
        + [
            VMEM((chunks * pair * rows, width), F32),
            VMEM((chunks * pitch, rows * width), F32),
            VMEM(((chunks + 2) * pitch, rows * width), BF16),
            VMEM(((chunks + 2) * pitch, rows * width), BF16),
            VMEM(((chunks + 2) * pitch, rows * width), BF16),
            VMEM(((chunks + 2) * pitch, rows * width), BF16),
            VMEM((2 * chunks * pitch, reach), BF16),
            VMEM((chunks * pitch, reach), BF16),
            VMEM((2 * pair, width), F32),
            VMEM((8, width), F32),
            VMEM((span, 8), F32),
            VMEM((8, span), F32),
            VMEM((chunks * pitch, width), F32),
            VMEM((chunks * pitch, width), F32),
            VMEM((chunks * pitch, width), F32),
            VMEM((chunks * pitch, width), F32),
            VMEM((round_up(nf + EDGE, 8), width), F32),
            VMEM((8, width), F32),
            VMEM(group_speed.shape, F32),
            VMEM((packed, width), F32),
            VMEM((packed, width), F32),
            VMEM((far_lat + packed, width), F32),
            VMEM((far_lat + packed, width), F32),
            VMEM((band, width), F32),
            VMEM((EDGE * nd, width), F32),
            VMEM((pair, width), F32),
            VMEM((pair, width), F32),
            VMEM((pair, width), F32),
            VMEM((8, width), F32),
            VMEM((8, width), F32),
            VMEM((8, width), F32),
            VMEM((pair, 8), F32),
            VMEM((width, share), BF16),
            VMEM((8, width), F32),
            VMEM((8, width), F32),
            VMEM((2 * all_rows, width), F32),
            VMEM((n_lat * n_freq - 1, 2 * all_rows, width), F32),
            dma((nf // 2,)), dma((len(smalls),)), pltpu.SemaphoreType.REGULAR,
            dma((3,)), dma((3,)), dma((4,)), dma((4,)), dma((4,)), dma((4,)),
            dma((1,)), dma((1,)), dma((n_lat * n_freq - 1,)), dma((n_lat * n_freq - 1,)),
        ],
        compiler_params=pltpu.CompilerParams(
            collective_id=0, has_side_effects=True, vmem_limit_bytes=32 << 20
        ),
    )(
        *[
            pltpu.with_memory_space_constraint(a, pltpu.HBM)
            for a in (spectrum.reshape(band * rows, width), *smalls)
        ]
    )
    out, ocean = pl.pallas_call(
        write_kernel,
        out_shape=(
            jax.ShapeDtypeStruct((band * rows, width), F32),
            jax.ShapeDtypeStruct((2, share), F32),
        ),
        in_specs=[vmem, vmem],
        out_specs=(hbm, hbm),
        scratch_shapes=[dma((5,))],
        compiler_params=pltpu.CompilerParams(vmem_limit_bytes=1 << 20),
    )(out, ocean)
    return out.reshape(spectrum.shape), ocean.T


def solution(mesh):
    axes = tuple(mesh.shape[a] for a in ("lat", "lon", "freq"))
    return jax.shard_map(
        functools.partial(local, axes),
        mesh=mesh,
        in_specs=(
            P("freq", None, "lat", "lon"),
            P("freq"),
            P("lat", "lon"),
            P("lat", "lon"),
            P("lat", "lon"),
            P(),
            P(),
            P(),
            P(),
            P("lat", "lon"),
        ),
        out_specs=(P("freq", None, "lat", "lon"), P(("lon", "freq"), None)),
        check_vma=False,
    )
```

```python
import functools

import jax
import jax.numpy as jnp
import numpy as np
from jax import lax
from jax.experimental import pallas as pl
from jax.experimental.pallas import tpu as pltpu
from jax.sharding import PartitionSpec as P

time_step = 0.5
MESH = pl.DeviceIdType.MESH
VMEM = pltpu.VMEM
LANES = 128
EDGE = 4
F32, BF16 = jnp.float32, jnp.bfloat16


def spread(nf):
    order = list(range(EDGE)) + list(range(nf - EDGE, nf)) + list(range(EDGE, nf - EDGE))
    return {f: i for i, f in enumerate(order)}


def round_up(n, m):
    return -(-n // m) * m


def split(v):
    high = v.astype(BF16)
    return high, (v - high.astype(F32)).astype(BF16)


def thirds(v):
    high, low = split(v)
    rest = v - high.astype(F32) - low.astype(F32)
    return high, low, rest.astype(BF16)


def layout(rows):
    inner, rim_rows = list(range(1, rows - 1)), [0, rows - 1]
    slot = {r: i for i, r in enumerate(inner + rim_rows)}

    def columns(r):
        return slice(slot[r] * LANES, slot[r] * LANES + LANES)

    whole = slice(0, rows * LANES)
    split_at = len(inner) * LANES
    return inner, rim_rows, columns, (whole, slice(0, split_at), slice(split_at, rows * LANES))


def finish_chunk(c, first, cs, shape, refs, result, growth, stay):
    nd, rows = shape
    put, th, tl, shapes, mf = refs
    pair = 2 * nd
    pitch = round_up(pair, 16)
    window = 3 * pitch
    columns = layout(rows)[2]
    at = pl.multiple_of(c * pitch, 16)
    lhs = put[pl.ds(at, pitch), :window]
    back = jnp.dot(lhs, th[pl.ds(at, window), cs], preferred_element_type=F32)
    back = back + jnp.dot(lhs, tl[pl.ds(at, window), cs], preferred_element_type=F32)
    profile = shapes[pl.ds(at, pair), :]
    to = (c - first) * (pair * rows)
    for r in range(rows):
        here = columns(r)
        if here.start < cs.start or here.stop > cs.stop:
            continue
        e = mf[pl.ds(at, pair), here]
        gain = back[:pair, here.start - cs.start : here.stop - cs.start]
        result[pl.ds(to + r, pair, stride=rows), :] = e * (stay(r) + profile * growth(r)) + gain


def wave_kernel(sizes, angles, spectrum, *refs):
    sources, refs = refs[:10], refs[10:]
    result, mf, th, tl, put, shapes, factors, stress, spread_out, *refs = refs
    inputs, refs = refs[:10], refs[10:]
    speed, waves, profile, coef, momentum, quad, mask, wind, dissip, cells = inputs
    (
        x, mh, ml, pick, table, rates, cols, lines, coefs, weight0, weight1,
        gains, gains_far, speed_far, pack_up, pack_down, got_up, got_down, edge, edge_far,
        lon_pack, got_left, got_right, lon_far, far_left, far_right, cols_far, energy, energy_got, tau_own, taus,
        load_sem, small_sem, lat_ready, diag_ready, lon_ready, raw_send, raw_recv, lat_send, lat_recv, lon_send, lon_recv,
        sum_send, sum_recv, tau_send, tau_recv,
    ) = refs
    n_lat, n_lon, n_freq, nf, nd, rows, nbins = sizes
    half = nd // 2
    pair = 2 * nd
    band = nf * nd
    all_rows = n_lat * rows
    pitch = round_up(pair, 16)
    pad = pitch - pair
    own_chunks = nf // 2
    far_chunks = EDGE // 2
    chunks = own_chunks + far_chunks
    window = 3 * pitch
    reach = round_up(window, LANES)
    span = lines.shape[1]
    places = spread(nf)
    groups = pair // 8
    cosines, sines = angles
    li, lo, fi = lax.axis_index("lat"), lax.axis_index("lon"), lax.axis_index("freq")
    other = 1 - fi
    first = far_chunks * fi
    far_first = own_chunks * other

    own_rows = pl.multiple_of(first * (pair * rows), 8)
    small = [
        pltpu.make_async_copy(a, b, small_sem.at[i])
        for i, (a, b) in enumerate(zip(sources, inputs))
    ]
    step = 3 if own_chunks % 3 == 0 else 1
    loads = []
    for i in range(own_chunks // step):
        count = step * pair * rows
        loads.append(
            pltpu.make_async_copy(
                spectrum.at[pl.ds(i * count, count)], x.at[pl.ds(own_rows + i * count, count)],
                load_sem.at[i],
            )
        )
    for copy in loads + small:
        copy.start()

    east, west = lax.rem(lo + 1, n_lon), lax.rem(lo + n_lon - 1, n_lon)
    group = []
    for s in range(1, n_lat * n_freq):
        dl, df = divmod(s, n_freq)
        group.append({"lat": lax.rem(li + dl, n_lat), "freq": lax.rem(fi + df, n_freq)})
    barrier = pltpu.get_barrier_semaphore()
    last = n_lon - 1
    higher = [li + dl < n_lat for dl in range(1, n_lat)]
    lat_peer = [
        [{"lat": lax.rem(li + dl, n_lat), "freq": f} for f in range(n_freq)] for dl in range(1, n_lat)
    ]
    beside = {
        side: [{"lon": side_at, "freq": f} for f in range(n_freq)]
        for side, side_at in (("east", east), ("west", west))
    }

    def signal(semaphore, peers):
        for peer in peers:
            pl.semaphore_signal(semaphore, inc=1, device_id=peer, device_id_type=MESH)

    def signal_if(condition, semaphore, peers):
        @pl.when(condition)
        def _():
            signal(semaphore, peers)

    signal(barrier, [{"freq": other}])
    for up, (in_first, in_second) in zip(higher, lat_peer):
        signal_if(jnp.logical_or(fi == 0, up), barrier, [in_first])
        signal_if(up, barrier, [in_second])
    signal_if(lo < last, barrier, beside["east"])
    signal_if(lo == 0, barrier, beside["west"])
    at_start, at_end = lax.div(last - lo, last), lax.div(lo, last)
    greeted = 1 + other * (n_lat - 1 + li) + fi * (2 * li) + 2 * (1 - at_start) + 2 * at_end
    answers_lat = n_lat - 1 - li
    answers_lon = 2 * (1 - at_end) + 2 * at_start

    def enter():
        pl.semaphore_wait(barrier, greeted)
        speed_copy().start()
        raw_copy(True).start()
        for up, (in_first, in_second) in zip(higher, lat_peer):
            signal_if(jnp.logical_and(fi == 1, jnp.logical_not(up)), lat_ready, [in_second])
            signal_if(jnp.logical_and(fi == 1, jnp.logical_not(up)), diag_ready, [in_first])
            signal_if(jnp.logical_and(fi == 0, jnp.logical_not(up)), diag_ready, [in_second])
        signal_if(lo > 0, lon_ready, beside["west"])
        signal_if(lo == last, lon_ready, beside["east"])

    packed = pack_up.shape[0]
    far_lat = EDGE * half
    up_ok, down_ok = li < n_lat - 1, li > 0

    def raw_copy(near):
        count = EDGE // 2 * nd * rows
        half_at = (other if near else fi) * count
        src = pl.multiple_of(other * ((nf - EDGE) * nd * rows) + half_at, 8)
        dst = pl.multiple_of(fi * (band * rows) + half_at, 8)
        i = 2 if near else 0
        return pltpu.make_async_remote_copy(
            spectrum.at[pl.ds(src, count)], x.at[pl.ds(dst, count)],
            raw_send.at[i], raw_recv.at[i], device_id={"freq": other}, device_id_type=MESH,
        )

    def speed_copy():
        return pltpu.make_async_remote_copy(
            sources[0], speed_far, raw_send.at[1], raw_recv.at[1],
            device_id={"freq": other}, device_id_type=MESH,
        )

    def lat_copy(up):
        src, dst = (pack_up, got_up) if up else (pack_down, got_down)
        i = int(up)
        return pltpu.make_async_remote_copy(
            src, dst.at[pl.ds(far_lat, packed)], lat_send.at[i], lat_recv.at[i],
            device_id={"lat": li + 1 if up else li - 1}, device_id_type=MESH,
        )

    def lat_far_copy(up):
        src, dst = (pack_up, got_up) if up else (pack_down, got_down)
        i = 2 + int(up)
        return pltpu.make_async_remote_copy(
            src.at[pl.ds(pl.multiple_of(other * far_lat, 8), far_lat)], dst.at[pl.ds(0, far_lat)],
            lat_send.at[i], lat_recv.at[i],
            device_id={"lat": li + 1 if up else li - 1, "freq": other}, device_id_type=MESH,
        )

    def lon_copy(to_east):
        i = int(to_east)
        return pltpu.make_async_remote_copy(
            lon_pack, got_left if to_east else got_right, lon_send.at[i], lon_recv.at[i],
            device_id={"lon": east if to_east else west}, device_id_type=MESH,
        )

    def lon_far_copy(to_east):
        i = 2 + int(to_east)
        return pltpu.make_async_remote_copy(
            lon_far, far_left if to_east else far_right, lon_send.at[i], lon_recv.at[i],
            device_id={"lon": east if to_east else west, "freq": other}, device_id_type=MESH,
        )

    def energy_copy():
        return pltpu.make_async_remote_copy(
            energy, energy_got, sum_send.at[0], sum_recv.at[0],
            device_id={"freq": other}, device_id_type=MESH,
        )

    def tau_copy(s):
        return pltpu.make_async_remote_copy(
            tau_own, taus.at[s], tau_send.at[s], tau_recv.at[s],
            device_id=group[s], device_id_type=MESH,
        )

    def signs(values, j):
        return [bool(values[(8 * j + i) % nd] > 0.0) for i in range(8)]

    eight = lax.broadcasted_iota(jnp.int32, (8, LANES), 0)
    lane = lax.broadcasted_iota(jnp.int32, (8, LANES), 1)

    def rows_of(flags):
        spot = None
        for i, flag in enumerate(flags):
            if flag:
                here = eight == i
                spot = here if spot is None else jnp.logical_or(spot, here)
        return spot

    def choose(flags, yes, no):
        if all(flags):
            return yes()
        if not any(flags):
            return no()
        return jnp.where(rows_of(flags), yes(), no())

    forward = [signs(cosines, j) for j in range(groups)]
    southern = [[(8 * j + i) % nd < half for i in range(8)] for j in range(groups)]

    @pl.when(fi == 1)
    def _():
        enter()

    pack_up[pl.ds(packed - 8, 8), :] = jnp.zeros((8, LANES), F32)
    pack_down[pl.ds(packed - 8, 8), :] = jnp.zeros((8, LANES), F32)
    sums = [jnp.zeros((8, LANES), F32) for _ in range(groups)]
    for i, copy in enumerate(loads):
        if i == len(loads) - 1:

            @pl.when(fi == 0)
            def _():
                enter()

        copy.wait()
        for f in range(2 * step * i, 2 * step * (i + 1)):
            at = half * places[f]
            base = own_rows + nd * f * rows
            pack_up[pl.ds(at, half), :] = x[pl.ds(base + rows - 1, half, stride=rows), :]
            pack_down[pl.ds(at, half), :] = x[pl.ds(base + half * rows, half, stride=rows), :]
        for u in range(step):
            c = i * step + u + first
            base = pl.multiple_of(c * (pair * rows), 8)
            for r in range(rows):
                k = c * rows + r
                for j in range(groups):
                    e = x[pl.ds(base + 8 * rows * j + r, 8, stride=rows), :]
                    z = choose(
                        forward[j],
                        lambda: jnp.where(lane == LANES - 1, e, 0.0),
                        lambda: jnp.where(lane == 0, e, 0.0),
                    )
                    sums[j] = sums[j] + pltpu.roll(z, k, 1)

    for j in range(groups):
        aligned = choose(forward[j], lambda: pltpu.roll(sums[j], 1, 1), lambda: sums[j])
        lon_pack[8 * j : 8 * j + 8, :] = aligned

    begin = (first + (own_chunks - far_chunks) * other) * rows
    whole = jnp.concatenate(
        [lon_pack[...], jnp.zeros((LANES - pair, LANES), F32)], axis=0
    )
    turned = pltpu.roll(whole, lax.rem(LANES - begin, LANES), 1).T
    lon_far[...] = turned[0:8, :]

    def send_columns(answered):
        if answered:
            pl.semaphore_wait(lon_ready, answers_lon)
        for to_east in (True, False):
            lon_copy(to_east).start()
            lon_far_copy(to_east).start()

    @pl.when(lo == last)
    def _():
        send_columns(False)

    @pl.when(jnp.logical_and(fi == 1, up_ok))
    def _():
        pl.semaphore_wait(lat_ready, answers_lat)

    @pl.when(up_ok)
    def _():
        lat_copy(True).start()

    @pl.when(down_ok)
    def _():
        lat_copy(False).start()

    @pl.when(up_ok)
    def _():
        pl.semaphore_wait(diag_ready, answers_lat)
        lat_far_copy(True).start()

    @pl.when(down_ok)
    def _():
        lat_far_copy(False).start()

    raw_copy(False).start()

    for copy in small:
        copy.wait()
    rates[...] = jnp.zeros_like(rates)
    rates[0:1, 0:nf] = speed[...].reshape(1, nf)
    gains[...] = jnp.broadcast_to(
        pltpu.roll(rates[...], EDGE * fi, 1).T[0 : gains.shape[0], 0:1], gains.shape
    )
    bin0 = fi * ((nf - EDGE) * nd)
    lines[...] = jnp.zeros_like(lines)
    target = (quad[...] - bin0).astype(F32)
    shift = jnp.zeros_like(target)
    for i in range(1, chunks):
        shift = shift + jnp.where(target >= float(pair * i), float(pad), 0.0)
    lines[0:2, 0:nbins] = target + shift
    lines[2:3, 0:nbins] = time_step * coef[...].reshape(1, nbins)
    weight = profile[...].reshape(1, nbins)
    lines[3:4, 0:nbins] = weight
    lines[4:6, 0:nbins] = momentum[...] * weight
    lines[...] = pltpu.roll(lines[...], lax.rem(span - bin0, span), 1)
    cols[...] = jnp.full_like(cols, -1.0)
    for k in range(-(-chunks * pair // LANES)):
        block = lines[:, LANES * k : LANES * k + LANES].T
        at = LANES * k
        while at < min(LANES * (k + 1), chunks * pair):
            c = at // pair
            stop = min(pair * (c + 1), LANES * (k + 1))
            cols[at + pad * c : stop + pad * c, :] = block[at - LANES * k : stop - LANES * k]
            at = stop
    for k in range(span // LANES):
        lines[:, LANES * k : LANES * k + LANES] = cols[LANES * k : LANES * k + LANES, :].T
    turned = waves[...].T
    table[pl.ds(0, pair), :] = jnp.broadcast_to(turned[0:pair, 0:1], (pair, LANES))
    table[pl.ds(pair, pair), :] = jnp.broadcast_to(turned[0:pair, 1:2], (pair, LANES))

    @pl.when(jnp.logical_and(lo > 0, lo < last))
    def _():
        send_columns(True)

    @pl.when(jnp.logical_not(down_ok))
    def _():
        got_up[...] = jnp.zeros_like(got_up)

    @pl.when(jnp.logical_not(up_ok))
    def _():
        got_down[...] = jnp.zeros_like(got_down)

    for ref in (mh, ml, th, tl):
        for at in (0, (chunks + 1) * pitch):
            ref[pl.ds(at, pitch), :] = jnp.zeros((pitch, ref.shape[1]), BF16)
    lanes = lax.broadcasted_iota(jnp.int32, (pitch, reach), 1)
    below = lax.broadcasted_iota(jnp.int32, (pitch, reach), 0)
    own_bin = lanes == below + pitch

    def build(c, carry):
        at = pl.multiple_of(pitch * c, 8)
        where = (lanes + (at - pitch)).astype(F32)
        for i in range(2):
            chosen = jnp.where(cols[pl.ds(at, pitch), i : i + 1] == where, 1.0, 0.0)
            pick[pl.ds(pl.multiple_of(2 * at + pitch * i, 16), pitch), :] = chosen.astype(BF16)
        row = (below + at).astype(F32)
        line = pltpu.roll(lines[...], lax.rem(span + pitch - at, span), 1)
        given = jnp.where(own_bin, -2.0, 0.0)
        for i in range(2):
            given = given + jnp.where(line[i : i + 1, :reach] == row, 1.0, 0.0)
        put[pl.ds(pl.multiple_of(at, 16), pitch), :] = given.astype(BF16)
        for i, ref in enumerate((coefs, shapes, weight0, weight1)):
            ref[pl.ds(at, pitch), :] = jnp.broadcast_to(
                cols[pl.ds(at, pitch), 2 + i : 3 + i], (pitch, LANES)
            )
        mf[pl.ds(at + pair, pad), :] = jnp.zeros((pad, mf.shape[1]), F32)
        return carry

    lax.fori_loop(0, chunks, build, 0)
    share = (LANES // n_freq) * all_rows
    cell = lax.broadcasted_iota(jnp.int32, (LANES, share), 1)
    first_cell = (lax.broadcasted_iota(jnp.int32, (LANES, share), 0) - fi * (LANES // n_freq)) * all_rows
    inside = jnp.logical_and(cell >= first_cell, cell < first_cell + all_rows)
    spread_out[...] = jnp.where(inside, 1.0, 0.0).astype(BF16)

    @pl.when(lo == 0)
    def _():
        send_columns(True)

    sea = mask[...].astype(F32)

    inner, rim_rows, columns, (whole_cols, inner_cols, rim_cols) = layout(rows)

    def upwind(e, j):
        if all(forward[j]):
            return pltpu.roll(e, 1, 1)
        if not any(forward[j]):
            return pltpu.roll(e, LANES - 1, 1)
        at = lane + jnp.where(rows_of(forward[j]), LANES - 1, 1)
        return jnp.take_along_axis(e, at & (LANES - 1), axis=1)

    def propagate(c, outer, gain, halo, row_set, sums):
        base = pl.multiple_of(c * (pair * rows), 8)
        at = pl.multiple_of(c * pitch, 16)
        store = pl.multiple_of(c * pitch + pitch, 16)
        sums = dict(sums)
        held = {}
        for j in range(groups):
            low, high = 8 * j < nd, 8 * j + 8 > nd
            if low and high:
                g = jnp.where(eight < nd - 8 * j, gain[0], gain[1])
            else:
                g = jnp.broadcast_to(gain[0] if low else gain[1], (8, LANES))
            ax = g * table[8 * j : 8 * j + 8, :]
            ay = g * table[pair + 8 * j : pair + 8 * j + 8, :]
            stay = 1.0 - ax - ay
            e = [x[pl.ds(base + 8 * rows * j + r, 8, stride=rows), :] for r in range(rows)]
            if sums:
                w0, w1 = weight0[pl.ds(at + 8 * j, 8), :], weight1[pl.ds(at + 8 * j, 8), :]
            for r in row_set:
                rim = lane == choose(forward[j], lambda: 0, lambda: LANES - 1)
                nx = jnp.where(rim, halo(r, j), upwind(e[r], j))
                ny = choose(
                    southern[j],
                    lambda: e[r - 1] if r > 0 else outer(j),
                    lambda: e[r + 1] if r < rows - 1 else outer(j),
                )
                m = (stay * e[r] + ax * nx + ay * ny) * sea[r : r + 1, :]
                mf[pl.ds(at + 8 * j, 8), columns(r)] = m
                held[j, r] = m
                if sums:
                    for i, v in enumerate((m, m * w0, m * w1)):
                        sums[r, i] = sums[r, i] + v
                if j % 2 == 1 or j == groups - 1:
                    start = j if j % 2 == 0 else j - 1
                    both = [held[start, r], held[j, r] if j > start else jnp.zeros_like(m)]
                    hi, lw = split(jnp.concatenate(both, axis=0))
                    mh[pl.ds(store + 8 * start, 16), columns(r)] = hi
                    ml[pl.ds(store + 8 * start, 16), columns(r)] = lw
        return sums

    def interact(c, cs):
        width = (cs.stop - cs.start) // LANES
        at = pl.multiple_of(c * pitch, 16)
        lhs = pick[pl.ds(pl.multiple_of(2 * at, 16), 2 * pitch), :window]
        both = jnp.dot(lhs, mh[pl.ds(at, window), cs], preferred_element_type=F32)
        both = both + jnp.dot(lhs, ml[pl.ds(at, window), cs], preferred_element_type=F32)
        third, fourth = both[:pitch], both[pitch:]
        e = mf[pl.ds(at, pitch), cs]
        scale = jnp.concatenate([coefs[pl.ds(at, pitch), :]] * width, axis=1)
        product = third * fourth
        moved = (scale * e) * (e * (third + fourth) - (product + product))
        hi, lw = split(moved)
        to = pl.multiple_of(at + pitch, 16)
        th[pl.ds(to, pitch), cs] = hi
        tl[pl.ds(to, pitch), cs] = lw

    def finish(c, cs):
        finish_chunk(
            c, first, cs, (nd, rows), (put, th, tl, shapes, mf), result,
            lambda r: time_step * wind[r : r + 1, :], lambda r: 1.0,
        )

    def run(what, begin, count, cs, at_once):
        def body(t, carry):
            for u in range(at_once):
                what(begin + t * at_once + u, cs)
            return carry

        lax.fori_loop(0, count // at_once, body, 0)
        for u in range(count - count % at_once, count):
            what(begin + u, cs)

    def receive(ref, first_row, where):
        for i in range(len(where)):
            at = first_row + half * where[i]
            ref[pl.ds(nd * i, half), :] = got_up[pl.ds(at, half), :]
            ref[pl.ds(nd * i + half, half), :] = got_down[pl.ds(at, half), :]

    lon_copy(True).wait_recv()
    lon_copy(False).wait_recv()
    for j in range(groups):
        here = slice(8 * j, 8 * j + 8)
        got_left[here, :] = choose(
            forward[j],
            lambda: got_left[here, :],
            lambda: pltpu.roll(got_right[here, :], LANES - 1, 1),
        )

    def own(row_set):
        names = [(r, i) for r in row_set for i in range(3)]

        def body(t, sums):
            sums = dict(zip(names, sums))
            for u in range(step):
                c = first + t * step + u

                def halo(r, j):
                    return pltpu.roll(got_left[8 * j : 8 * j + 8, :], LANES - (c * rows + r), 1)

                def outer(j):
                    return edge[pl.ds(pl.multiple_of((c - first) * pair, 8) + 8 * j, 8), :]

                gain = [gains[pl.ds(2 * c + i, 1), :] for i in range(2)]
                sums = propagate(c, outer, gain, halo, row_set, sums)
            return tuple(sums[n] for n in names)

        zeros = tuple(jnp.zeros((8, LANES), F32) for _ in names)
        return dict(zip(names, lax.fori_loop(0, own_chunks // step, body, zeros)))

    near_first = 2 * first - fi
    near_count = chunks - far_chunks - 1
    last_first = 2 * first
    last_count = chunks - 2 * far_chunks
    sums = own(inner)
    @pl.when(down_ok)
    def _():
        lat_copy(True).wait_recv()

    @pl.when(up_ok)
    def _():
        lat_copy(False).wait_recv()

    receive(edge, far_lat, [places[f] for f in range(nf)])
    sums.update(own(rim_rows))

    energy[...] = jnp.zeros((8, LANES), F32)
    ids = (lo * LANES + lax.broadcasted_iota(jnp.int32, (all_rows, LANES), 1)) * all_rows
    ids = ids + lax.broadcasted_iota(jnp.int32, (all_rows, LANES), 0)
    totals = [jnp.zeros((all_rows, LANES), F32) for _ in range(2)]
    for r in range(rows):
        energy[r : r + 1, :] = jnp.sum(sums[r, 0], axis=0, keepdims=True)
        hit = cells[r : r + 1, :] == ids
        for i in range(2):
            tau = wind[r : r + 1, :] * jnp.sum(sums[r, 1 + i], axis=0, keepdims=True)
            totals[i] = totals[i] + jnp.where(hit, tau, 0.0)
    for i in range(2):
        tau_own[pl.ds(i * all_rows, all_rows), :] = totals[i]
    energy_copy().start()
    for s in range(len(group)):
        tau_copy(s).start()

    run(interact, near_first, near_count, whole_cols, 4)
    run(finish, last_first, last_count, whole_cols, 4)

    speed_copy().wait_recv()
    rates[0:1, 0:nf] = speed_far[...].reshape(1, nf)
    gains_far[...] = jnp.broadcast_to(
        pltpu.roll(rates[...], fi * (LANES - (nf - EDGE)), 1).T[0:8, 0:1], gains_far.shape
    )

    @pl.when(down_ok)
    def _():
        lat_far_copy(True).wait_recv()

    @pl.when(up_ok)
    def _():
        lat_far_copy(False).wait_recv()

    receive(edge_far, 0, list(range(EDGE)))
    lon_far_copy(True).wait_recv()
    lon_far_copy(False).wait_recv()
    left, right = far_left[...].T, far_right[...].T
    for j in range(groups):
        here = slice(8 * j, 8 * j + 8)
        ahead = eight[:, 0:8] < 0
        for i, flag in enumerate(forward[j]):
            if flag:
                ahead = jnp.logical_or(ahead, eight[:, 0:8] == i)
        cols_far[here, :] = jnp.where(ahead, left[here], right[here])
    raw_copy(True).wait_recv()
    raw_copy(False).wait_recv()

    for u in range(far_chunks):
        def halo(r, j):
            k = u * rows + r
            return jnp.broadcast_to(cols_far[8 * j : 8 * j + 8, k : k + 1], (8, LANES))

        def outer(j):
            return edge_far[pair * u + 8 * j : pair * u + 8 * j + 8, :]

        gain = [gains_far[2 * u + i : 2 * u + i + 1, :] for i in range(2)]
        propagate(far_first + u, outer, gain, halo, range(rows), {})

    late = (chunks - far_chunks - 1) * other + fi
    run(interact, late, 2, whole_cols, 2)
    energy_copy().wait()
    factors[0:rows, :] = time_step * dissip[...] * ((energy[0:rows, :] + energy_got[0:rows, :]) / nbins)
    factors[rows : 2 * rows, :] = time_step * wind[...]

    st = tau_own[...]
    for s in range(len(group)):
        tau_copy(s).wait()
        st = st + taus[s]
    stress[...] = st

    raw_copy(True).wait_send()
    raw_copy(False).wait_send()
    speed_copy().wait_send()
    for flag in (True, False):
        lon_copy(flag).wait_send()
        lon_far_copy(flag).wait_send()

    @pl.when(up_ok)
    def _():
        lat_copy(True).wait_send()
        lat_far_copy(True).wait_send()

    @pl.when(down_ok)
    def _():
        lat_copy(False).wait_send()
        lat_far_copy(False).wait_send()


def write_kernel(
    sizes, before, mf, th, tl, put, shapes, factors, taus, spread_out, result_out, stress_out,
    result, stress, sems,
):
    n_lat, n_lon, n_freq, nf, nd, rows, nbins = sizes
    pair = 2 * nd
    pitch = round_up(pair, 16)
    own_chunks, far_chunks = nf // 2, EDGE // 2
    columns, (whole_cols, _, _) = layout(rows)[2:]
    fi = lax.axis_index("freq")
    first = far_chunks * fi
    size = pair * rows

    def out(i):
        here = pl.ds(pl.multiple_of(lax.rem(i + first, own_chunks) * size, 8), size)
        return pltpu.make_async_copy(result.at[here], result_out.at[here], sems.at[i])

    def settle(i, carry):
        t = lax.rem(i + first, own_chunks)
        at = pl.multiple_of((t + first) * pitch, 8)
        for r in range(rows):
            spot = pl.ds(t * size + r, pair, stride=rows)
            e = mf[pl.ds(at, pair), columns(r)]
            result[spot, :] = before[spot, :] - e * factors[r : r + 1, :]
        out(i).start()
        return carry

    settled = own_chunks - far_chunks
    lax.fori_loop(0, settled, settle, 0)
    for i in range(settled, own_chunks):
        finish_chunk(
            lax.rem(i + first, own_chunks) + first, first, whole_cols, (nd, rows),
            (put, th, tl, shapes, mf), result,
            lambda r: factors[rows + r : rows + r + 1, :], lambda r: 1.0 - factors[r : r + 1, :],
        )
    for i in range(settled, own_chunks):
        out(i).start()

    all_rows = n_lat * rows
    share = (LANES // n_freq) * all_rows
    st = taus[...]
    wide = sum(
        jnp.dot(term, spread_out[...], preferred_element_type=F32) for term in thirds(st)
    )
    place = lax.broadcasted_iota(jnp.int32, (all_rows, share), 1) & (all_rows - 1)
    own_row = place == lax.broadcasted_iota(jnp.int32, (all_rows, share), 0)
    for i in range(2):
        picked = jnp.where(own_row, wide[i * all_rows : (i + 1) * all_rows], 0.0)
        stress[i : i + 1, :] = jnp.sum(picked, axis=0, keepdims=True)
    last = pltpu.make_async_copy(stress, stress_out, sems.at[own_chunks])
    last.start()

    def wait(i, carry):
        out(i).wait()
        return carry

    lax.fori_loop(0, own_chunks, wait, 0)
    last.wait()


def local(
    axes,
    spectrum,
    group_speed,
    sea_mask,
    wind_growth,
    dissipation,
    wind_profile,
    nonlinear_coef,
    momentum,
    quadruplet,
    ocean_cell,
):
    n_lat, n_lon, n_freq = axes
    nf, nd, rows, width = spectrum.shape
    nbins = wind_profile.shape[0]
    assert n_freq == 2 and nf % 2 == 0 and width == LANES
    band, pair, half = nf * nd, 2 * nd, nd // 2
    pitch = round_up(pair, 16)
    chunks = nf // 2 + EDGE // 2
    all_rows = n_lat * rows
    angles = (np.float32(2.0 * np.pi) * np.arange(nd, dtype=np.float32) / np.float32(nd)).astype(
        np.float32
    )
    cosines, sines = np.cos(angles), np.sin(angles)
    waves = np.zeros((8, LANES), np.float32)
    waves[0, :pair], waves[1, :pair] = np.tile(np.abs(cosines), 2), np.tile(np.abs(sines), 2)

    packed = round_up(nf * half, 8)
    far_lat = EDGE * half
    share = (width // n_freq) * all_rows
    span = round_up(max(nbins, (chunks + 2) * pitch), LANES)
    reach = round_up(3 * pitch, LANES)
    vmem = pl.BlockSpec(memory_space=VMEM)
    hbm = pl.BlockSpec(memory_space=pltpu.HBM)
    sizes = (n_lat, n_lon, n_freq, nf, nd, rows, nbins)
    dma = pltpu.SemaphoreType.DMA
    smalls = (
        group_speed,
        jnp.asarray(waves),
        wind_profile,
        nonlinear_coef,
        momentum,
        quadruplet,
        sea_mask,
        wind_growth,
        dissipation,
        ocean_cell,
    )
    between = [
        jax.ShapeDtypeStruct(shape, dtype)
        for shape, dtype in (
            ((band * rows, width), F32),
            ((chunks * pitch, rows * width), F32),
            (((chunks + 2) * pitch, rows * width), BF16),
            (((chunks + 2) * pitch, rows * width), BF16),
            ((chunks * pitch, reach), BF16),
            ((chunks * pitch, width), F32),
            ((2 * rows, width), F32),
            ((2 * all_rows, width), F32),
            ((width, share), BF16),
        )
    ]
    made = pl.pallas_call(
        functools.partial(wave_kernel, sizes, (cosines, sines)),
        out_shape=between,
        in_specs=[hbm] * 11,
        out_specs=[vmem] * len(between),
        scratch_shapes=[VMEM(a.shape, a.dtype) for a in smalls]
        + [
            VMEM((chunks * pair * rows, width), F32),
            VMEM(((chunks + 2) * pitch, rows * width), BF16),
            VMEM(((chunks + 2) * pitch, rows * width), BF16),
            VMEM((2 * chunks * pitch, reach), BF16),
            VMEM((2 * pair, width), F32),
            VMEM((8, width), F32),
            VMEM((span, 8), F32),
            VMEM((8, span), F32),
            VMEM((chunks * pitch, width), F32),
            VMEM((chunks * pitch, width), F32),
            VMEM((chunks * pitch, width), F32),
            VMEM((round_up(nf + EDGE, 8), width), F32),
            VMEM((8, width), F32),
            VMEM(group_speed.shape, F32),
            VMEM((packed, width), F32),
            VMEM((packed, width), F32),
            VMEM((far_lat + packed, width), F32),
            VMEM((far_lat + packed, width), F32),
            VMEM((band, width), F32),
            VMEM((EDGE * nd, width), F32),
            VMEM((pair, width), F32),
            VMEM((pair, width), F32),
            VMEM((pair, width), F32),
            VMEM((8, width), F32),
            VMEM((8, width), F32),
            VMEM((8, width), F32),
            VMEM((pair, 8), F32),
            VMEM((8, width), F32),
            VMEM((8, width), F32),
            VMEM((2 * all_rows, width), F32),
            VMEM((n_lat * n_freq - 1, 2 * all_rows, width), F32),
            dma((nf // 2,)), dma((len(smalls),)),
            *[pltpu.SemaphoreType.REGULAR] * 3,
            dma((3,)), dma((3,)), dma((4,)), dma((4,)), dma((4,)), dma((4,)),
            dma((1,)), dma((1,)), dma((n_lat * n_freq - 1,)), dma((n_lat * n_freq - 1,)),
        ],
        compiler_params=pltpu.CompilerParams(
            collective_id=0, has_side_effects=True, vmem_limit_bytes=32 << 20
        ),
    )(
        *[
            pltpu.with_memory_space_constraint(a, pltpu.HBM)
            for a in (spectrum.reshape(band * rows, width), *smalls)
        ]
    )
    out, ocean = pl.pallas_call(
        functools.partial(write_kernel, sizes),
        out_shape=(
            jax.ShapeDtypeStruct((band * rows, width), F32),
            jax.ShapeDtypeStruct((2, share), F32),
        ),
        in_specs=[vmem] * len(between),
        out_specs=(hbm, hbm),
        scratch_shapes=[
            VMEM((band * rows, width), F32), VMEM((2, share), F32), dma((nf // 2 + 1,)),
        ],
        compiler_params=pltpu.CompilerParams(vmem_limit_bytes=16 << 20),
    )(*made)
    return out.reshape(spectrum.shape), ocean.T


def solution(mesh):
    axes = tuple(mesh.shape[a] for a in ("lat", "lon", "freq"))
    return jax.shard_map(
        functools.partial(local, axes),
        mesh=mesh,
        in_specs=(
            P("freq", None, "lat", "lon"),
            P("freq"),
            P("lat", "lon"),
            P("lat", "lon"),
            P("lat", "lon"),
            P(),
            P(),
            P(),
            P(),
            P("lat", "lon"),
        ),
        out_specs=(P("freq", None, "lat", "lon"), P(("lon", "freq"), None)),
        check_vma=False,
    )
```

```python
import functools

import jax
import jax.numpy as jnp
import numpy as np
from jax import lax
from jax.experimental import pallas as pl
from jax.experimental.pallas import tpu as pltpu
from jax.sharding import PartitionSpec as P

time_step = 0.5
MESH = pl.DeviceIdType.MESH
VMEM = pltpu.VMEM
LANES = 128
EDGE = 4
F32, BF16 = jnp.float32, jnp.bfloat16


def spread(nf):
    order = list(range(EDGE)) + list(range(nf - EDGE, nf)) + list(range(EDGE, nf - EDGE))
    return {f: i for i, f in enumerate(order)}


def round_up(n, m):
    return -(-n // m) * m


def split(v):
    high = v.astype(BF16)
    return high, (v - high.astype(F32)).astype(BF16)


def thirds(v):
    high, low = split(v)
    rest = v - high.astype(F32) - low.astype(F32)
    return high, low, rest.astype(BF16)


def layout(rows):
    inner, rim_rows = list(range(1, rows - 1)), [0, rows - 1]
    slot = {r: i for i, r in enumerate(inner + rim_rows)}

    def columns(r):
        return slice(slot[r] * LANES, slot[r] * LANES + LANES)

    whole = slice(0, rows * LANES)
    split_at = len(inner) * LANES
    return inner, rim_rows, columns, (whole, slice(0, split_at), slice(split_at, rows * LANES))


def finish_chunk(c, first, cs, shape, refs, result, growth, stay):
    nd, rows = shape
    put, th, tl, shapes, mf = refs
    pair = 2 * nd
    pitch = round_up(pair, 16)
    window = 3 * pitch
    columns = layout(rows)[2]
    at = pl.multiple_of(c * pitch, 16)
    lhs = put[pl.ds(at, pitch), :window]
    back = jnp.dot(lhs, th[pl.ds(at, window), cs], preferred_element_type=F32)
    back = back + jnp.dot(lhs, tl[pl.ds(at, window), cs], preferred_element_type=F32)
    profile = shapes[pl.ds(at, pair), :]
    to = (c - first) * (pair * rows)
    for r in range(rows):
        here = columns(r)
        if here.start < cs.start or here.stop > cs.stop:
            continue
        e = mf[pl.ds(at, pair), here]
        gain = back[:pair, here.start - cs.start : here.stop - cs.start]
        result[pl.ds(to + r, pair, stride=rows), :] = e * (stay(r) + profile * growth(r)) + gain


def wave_kernel(sizes, angles, spectrum, *refs):
    sources, refs = refs[:10], refs[10:]
    result, mf, th, tl, put, shapes, factors, stress, spread_out, *refs = refs
    inputs, refs = refs[:10], refs[10:]
    speed, waves, profile, coef, momentum, quad, mask, wind, dissip, cells = inputs
    (
        x, mh, ml, pick, table, rates, cols, lines, coefs, weight0, weight1, rim_weights,
        gains, gains_far, speed_far, pack_up, pack_down, got_up, got_down, edge, edge_far,
        lon_pack, got_left, got_right, lon_far, far_left, far_right, cols_far, energy, energy_got, tau_own, taus,
        load_sem, small_sem, lat_ready, diag_ready, lon_ready, raw_send, raw_recv, lat_send, lat_recv, lon_send, lon_recv,
        sum_send, sum_recv, tau_send, tau_recv,
    ) = refs
    n_lat, n_lon, n_freq, nf, nd, rows, nbins = sizes
    half = nd // 2
    pair = 2 * nd
    band = nf * nd
    all_rows = n_lat * rows
    pitch = round_up(pair, 16)
    pad = pitch - pair
    own_chunks = nf // 2
    far_chunks = EDGE // 2
    chunks = own_chunks + far_chunks
    window = 3 * pitch
    reach = round_up(window, LANES)
    span = lines.shape[1]
    places = spread(nf)
    groups = pair // 8
    cosines, sines = angles
    li, lo, fi = lax.axis_index("lat"), lax.axis_index("lon"), lax.axis_index("freq")
    other = 1 - fi
    first = far_chunks * fi
    far_first = own_chunks * other

    own_rows = pl.multiple_of(first * (pair * rows), 8)
    small = [
        pltpu.make_async_copy(a, b, small_sem.at[i])
        for i, (a, b) in enumerate(zip(sources, inputs))
    ]
    step = 3 if own_chunks % 3 == 0 else 1
    loads = []
    for i in range(own_chunks // step):
        count = step * pair * rows
        loads.append(
            pltpu.make_async_copy(
                spectrum.at[pl.ds(i * count, count)], x.at[pl.ds(own_rows + i * count, count)],
                load_sem.at[i],
            )
        )
    for copy in loads + small:
        copy.start()

    east, west = lax.rem(lo + 1, n_lon), lax.rem(lo + n_lon - 1, n_lon)
    group = []
    for s in range(1, n_lat * n_freq):
        dl, df = divmod(s, n_freq)
        group.append({"lat": lax.rem(li + dl, n_lat), "freq": lax.rem(fi + df, n_freq)})
    barrier = pltpu.get_barrier_semaphore()
    last = n_lon - 1
    higher = [li + dl < n_lat for dl in range(1, n_lat)]
    lat_peer = [
        [{"lat": lax.rem(li + dl, n_lat), "freq": f} for f in range(n_freq)] for dl in range(1, n_lat)
    ]
    beside = {
        side: [{"lon": side_at, "freq": f} for f in range(n_freq)]
        for side, side_at in (("east", east), ("west", west))
    }

    def signal(semaphore, peers):
        for peer in peers:
            pl.semaphore_signal(semaphore, inc=1, device_id=peer, device_id_type=MESH)

    def signal_if(condition, semaphore, peers):
        @pl.when(condition)
        def _():
            signal(semaphore, peers)

    signal(barrier, [{"freq": other}])
    for up, (in_first, in_second) in zip(higher, lat_peer):
        signal_if(jnp.logical_or(fi == 0, up), barrier, [in_first])
        signal_if(up, barrier, [in_second])
    signal_if(lo < last, barrier, beside["east"])
    signal_if(lo == 0, barrier, beside["west"])
    at_start, at_end = lax.div(last - lo, last), lax.div(lo, last)
    greeted = 1 + other * (n_lat - 1 + li) + fi * (2 * li) + 2 * (1 - at_start) + 2 * at_end
    answers_lat = n_lat - 1 - li
    answers_lon = 2 * (1 - at_end) + 2 * at_start

    def enter():
        pl.semaphore_wait(barrier, greeted)
        speed_copy().start()
        raw_copy(True).start()
        for up, (in_first, in_second) in zip(higher, lat_peer):
            signal_if(jnp.logical_and(fi == 1, jnp.logical_not(up)), lat_ready, [in_second])
            signal_if(jnp.logical_and(fi == 1, jnp.logical_not(up)), diag_ready, [in_first])
            signal_if(jnp.logical_and(fi == 0, jnp.logical_not(up)), diag_ready, [in_second])
        signal_if(lo > 0, lon_ready, beside["west"])
        signal_if(lo == last, lon_ready, beside["east"])

    packed = pack_up.shape[0]
    far_lat = EDGE * half
    up_ok, down_ok = li < n_lat - 1, li > 0

    def raw_copy(near):
        count = EDGE // 2 * nd * rows
        half_at = (other if near else fi) * count
        src = pl.multiple_of(other * ((nf - EDGE) * nd * rows) + half_at, 8)
        dst = pl.multiple_of(fi * (band * rows) + half_at, 8)
        i = 2 if near else 0
        return pltpu.make_async_remote_copy(
            spectrum.at[pl.ds(src, count)], x.at[pl.ds(dst, count)],
            raw_send.at[i], raw_recv.at[i], device_id={"freq": other}, device_id_type=MESH,
        )

    def speed_copy():
        return pltpu.make_async_remote_copy(
            sources[0], speed_far, raw_send.at[1], raw_recv.at[1],
            device_id={"freq": other}, device_id_type=MESH,
        )

    def lat_copy(up):
        src, dst = (pack_up, got_up) if up else (pack_down, got_down)
        i = int(up)
        return pltpu.make_async_remote_copy(
            src, dst.at[pl.ds(far_lat, packed)], lat_send.at[i], lat_recv.at[i],
            device_id={"lat": li + 1 if up else li - 1}, device_id_type=MESH,
        )

    def lat_far_copy(up):
        src, dst = (pack_up, got_up) if up else (pack_down, got_down)
        i = 2 + int(up)
        return pltpu.make_async_remote_copy(
            src.at[pl.ds(pl.multiple_of(other * far_lat, 8), far_lat)], dst.at[pl.ds(0, far_lat)],
            lat_send.at[i], lat_recv.at[i],
            device_id={"lat": li + 1 if up else li - 1, "freq": other}, device_id_type=MESH,
        )

    def lon_copy(to_east):
        i = int(to_east)
        return pltpu.make_async_remote_copy(
            lon_pack, got_left if to_east else got_right, lon_send.at[i], lon_recv.at[i],
            device_id={"lon": east if to_east else west}, device_id_type=MESH,
        )

    def lon_far_copy(to_east):
        i = 2 + int(to_east)
        return pltpu.make_async_remote_copy(
            lon_far, far_left if to_east else far_right, lon_send.at[i], lon_recv.at[i],
            device_id={"lon": east if to_east else west, "freq": other}, device_id_type=MESH,
        )

    def energy_copy():
        return pltpu.make_async_remote_copy(
            energy, energy_got, sum_send.at[0], sum_recv.at[0],
            device_id={"freq": other}, device_id_type=MESH,
        )

    def tau_copy(s):
        return pltpu.make_async_remote_copy(
            tau_own, taus.at[s], tau_send.at[s], tau_recv.at[s],
            device_id=group[s], device_id_type=MESH,
        )

    def signs(values, j):
        return [bool(values[(8 * j + i) % nd] > 0.0) for i in range(8)]

    eight = lax.broadcasted_iota(jnp.int32, (8, LANES), 0)
    lane = lax.broadcasted_iota(jnp.int32, (8, LANES), 1)

    def rows_of(flags):
        spot = None
        for i, flag in enumerate(flags):
            if flag:
                here = eight == i
                spot = here if spot is None else jnp.logical_or(spot, here)
        return spot

    def choose(flags, yes, no):
        if all(flags):
            return yes()
        if not any(flags):
            return no()
        return jnp.where(rows_of(flags), yes(), no())

    forward = [signs(cosines, j) for j in range(groups)]
    southern = [[(8 * j + i) % nd < half for i in range(8)] for j in range(groups)]

    @pl.when(fi == 1)
    def _():
        enter()

    pack_up[pl.ds(packed - 8, 8), :] = jnp.zeros((8, LANES), F32)
    pack_down[pl.ds(packed - 8, 8), :] = jnp.zeros((8, LANES), F32)
    sums = [jnp.zeros((8, LANES), F32) for _ in range(groups)]
    for i, copy in enumerate(loads):
        if i == len(loads) - 1:

            @pl.when(fi == 0)
            def _():
                enter()

        copy.wait()
        for f in range(2 * step * i, 2 * step * (i + 1)):
            at = half * places[f]
            base = own_rows + nd * f * rows
            pack_up[pl.ds(at, half), :] = x[pl.ds(base + rows - 1, half, stride=rows), :]
            pack_down[pl.ds(at, half), :] = x[pl.ds(base + half * rows, half, stride=rows), :]
        for u in range(step):
            c = i * step + u + first
            base = pl.multiple_of(c * (pair * rows), 8)
            for r in range(rows):
                k = c * rows + r
                for j in range(groups):
                    e = x[pl.ds(base + 8 * rows * j + r, 8, stride=rows), :]
                    z = choose(
                        forward[j],
                        lambda: jnp.where(lane == LANES - 1, e, 0.0),
                        lambda: jnp.where(lane == 0, e, 0.0),
                    )
                    sums[j] = sums[j] + pltpu.roll(z, k, 1)

    for j in range(groups):
        aligned = choose(forward[j], lambda: pltpu.roll(sums[j], 1, 1), lambda: sums[j])
        lon_pack[8 * j : 8 * j + 8, :] = aligned

    begin = (first + (own_chunks - far_chunks) * other) * rows
    whole = jnp.concatenate(
        [lon_pack[...], jnp.zeros((LANES - pair, LANES), F32)], axis=0
    )
    turned = pltpu.roll(whole, lax.rem(LANES - begin, LANES), 1).T
    lon_far[...] = turned[0:8, :]

    def send_columns(answered):
        if answered:
            pl.semaphore_wait(lon_ready, answers_lon)
        for to_east in (True, False):
            lon_copy(to_east).start()
            lon_far_copy(to_east).start()

    @pl.when(lo == last)
    def _():
        send_columns(False)

    @pl.when(jnp.logical_and(fi == 1, up_ok))
    def _():
        pl.semaphore_wait(lat_ready, answers_lat)

    @pl.when(up_ok)
    def _():
        lat_copy(True).start()

    @pl.when(down_ok)
    def _():
        lat_copy(False).start()

    @pl.when(up_ok)
    def _():
        pl.semaphore_wait(diag_ready, answers_lat)
        lat_far_copy(True).start()

    @pl.when(down_ok)
    def _():
        lat_far_copy(False).start()

    raw_copy(False).start()

    for copy in small:
        copy.wait()
    rates[...] = jnp.zeros_like(rates)
    rates[0:1, 0:nf] = speed[...].reshape(1, nf)
    own_rates = rates[...]
    gains[...] = jnp.broadcast_to(
        pltpu.roll(rates[...], EDGE * fi, 1).T[0 : gains.shape[0], 0:1], gains.shape
    )
    bin0 = fi * ((nf - EDGE) * nd)
    lines[...] = jnp.zeros_like(lines)
    target = (quad[...] - bin0).astype(F32)
    shift = jnp.zeros_like(target)
    for i in range(1, chunks):
        shift = shift + jnp.where(target >= float(pair * i), float(pad), 0.0)
    lines[0:2, 0:nbins] = target + shift
    lines[2:3, 0:nbins] = time_step * coef[...].reshape(1, nbins)
    weight = profile[...].reshape(1, nbins)
    lines[3:4, 0:nbins] = weight
    lines[4:6, 0:nbins] = momentum[...] * weight
    lines[...] = pltpu.roll(lines[...], lax.rem(span - bin0, span), 1)
    cols[...] = jnp.full_like(cols, -1.0)
    for k in range(-(-chunks * pair // LANES)):
        block = lines[:, LANES * k : LANES * k + LANES].T
        at = LANES * k
        while at < min(LANES * (k + 1), chunks * pair):
            c = at // pair
            stop = min(pair * (c + 1), LANES * (k + 1))
            cols[at + pad * c : stop + pad * c, :] = block[at - LANES * k : stop - LANES * k]
            at = stop
    for k in range(span // LANES):
        lines[:, LANES * k : LANES * k + LANES] = cols[LANES * k : LANES * k + LANES, :].T
    turned = waves[...].T
    table[pl.ds(0, pair), :] = jnp.broadcast_to(turned[0:pair, 0:1], (pair, LANES))
    table[pl.ds(pair, pair), :] = jnp.broadcast_to(turned[0:pair, 1:2], (pair, LANES))

    @pl.when(jnp.logical_and(lo > 0, lo < last))
    def _():
        send_columns(True)

    @pl.when(jnp.logical_not(down_ok))
    def _():
        got_up[...] = jnp.zeros_like(got_up)

    @pl.when(jnp.logical_not(up_ok))
    def _():
        got_down[...] = jnp.zeros_like(got_down)

    for ref in (mh, ml, th, tl):
        for at in (0, (chunks + 1) * pitch):
            ref[pl.ds(at, pitch), :] = jnp.zeros((pitch, ref.shape[1]), BF16)
    lanes = lax.broadcasted_iota(jnp.int32, (pitch, reach), 1)
    below = lax.broadcasted_iota(jnp.int32, (pitch, reach), 0)
    own_bin = lanes == below + pitch

    def build(c, carry):
        at = pl.multiple_of(pitch * c, 8)
        where = (lanes + (at - pitch)).astype(F32)
        for i in range(2):
            chosen = jnp.where(cols[pl.ds(at, pitch), i : i + 1] == where, 1.0, 0.0)
            pick[pl.ds(pl.multiple_of(2 * at + pitch * i, 16), pitch), :] = chosen.astype(BF16)
        row = (below + at).astype(F32)
        line = pltpu.roll(lines[...], lax.rem(span + pitch - at, span), 1)
        given = jnp.where(own_bin, -2.0, 0.0)
        for i in range(2):
            given = given + jnp.where(line[i : i + 1, :reach] == row, 1.0, 0.0)
        put[pl.ds(pl.multiple_of(at, 16), pitch), :] = given.astype(BF16)
        for i, ref in enumerate((coefs, shapes, weight0, weight1)):
            ref[pl.ds(at, pitch), :] = jnp.broadcast_to(
                cols[pl.ds(at, pitch), 2 + i : 3 + i], (pitch, LANES)
            )
        mf[pl.ds(at + pair, pad), :] = jnp.zeros((pad, mf.shape[1]), F32)
        return carry

    lax.fori_loop(0, chunks, build, 0)
    share = (LANES // n_freq) * all_rows
    cell = lax.broadcasted_iota(jnp.int32, (LANES, share), 1)
    first_cell = (lax.broadcasted_iota(jnp.int32, (LANES, share), 0) - fi * (LANES // n_freq)) * all_rows
    inside = jnp.logical_and(cell >= first_cell, cell < first_cell + all_rows)
    spread_out[...] = jnp.where(inside, 1.0, 0.0).astype(BF16)

    @pl.when(lo == 0)
    def _():
        send_columns(True)

    sea = mask[...].astype(F32)

    inner, rim_rows, columns, (whole_cols, inner_cols, rim_cols) = layout(rows)

    def upwind(e, j):
        if all(forward[j]):
            return pltpu.roll(e, 1, 1)
        if not any(forward[j]):
            return pltpu.roll(e, LANES - 1, 1)
        at = lane + jnp.where(rows_of(forward[j]), LANES - 1, 1)
        return jnp.take_along_axis(e, at & (LANES - 1), axis=1)

    def rates_of(j, gain):
        low, high = 8 * j < nd, 8 * j + 8 > nd
        if low and high:
            g = jnp.where(eight < nd - 8 * j, gain[0], gain[1])
        else:
            g = jnp.broadcast_to(gain[0] if low else gain[1], (8, LANES))
        return g * table[8 * j : 8 * j + 8, :], g * table[pair + 8 * j : pair + 8 * j + 8, :]

    def rim_lane(j):
        return lane == choose(forward[j], lambda: 0, lambda: LANES - 1)

    def prepare(c, gain, sums):
        base = pl.multiple_of(c * (pair * rows), 8)
        at = pl.multiple_of(c * pitch, 16)
        zero = jnp.zeros((8, LANES), F32)
        for j in range(groups):
            ax, ay = rates_of(j, gain)
            stay = 1.0 - ax - ay
            weights = weight0[pl.ds(at + 8 * j, 8), :], weight1[pl.ds(at + 8 * j, 8), :]
            e = [x[pl.ds(base + 8 * rows * j + r, 8, stride=rows), :] for r in range(rows)]
            for r in range(rows):
                nx = jnp.where(rim_lane(j), 0.0, upwind(e[r], j))
                ny = choose(
                    southern[j],
                    lambda: e[r - 1] if r > 0 else zero,
                    lambda: e[r + 1] if r < rows - 1 else zero,
                )
                m = stay * e[r] + ax * nx + ay * ny
                mf[pl.ds(at + 8 * j, 8), columns(r)] = m
                for i, v in enumerate((m, m * weights[0], m * weights[1])):
                    sums[r, i] = sums[r, i] + v

    def complete(c, gain, row_set, keep, outer=None, halo=None):
        at = pl.multiple_of(c * pitch, 16)
        store = pl.multiple_of(c * pitch + pitch, 16)
        held = {}
        for j in range(groups):
            ax, ay = rates_of(j, gain)
            for r in row_set:
                m = mf[pl.ds(at + 8 * j, 8), columns(r)]
                if halo:
                    m = m + ax * jnp.where(rim_lane(j), halo(r, j), 0.0)
                if not keep:
                    mf[pl.ds(at + 8 * j, 8), columns(r)] = m
                    continue
                from_edge = [
                    (r == 0 and south) or (r == rows - 1 and not south) for south in southern[j]
                ]
                if any(from_edge):
                    zero = jnp.zeros((8, LANES), F32)
                    m = m + ay * choose(from_edge, lambda: outer(j), lambda: zero)
                m = m * sea[r : r + 1, :]
                mf[pl.ds(at + 8 * j, 8), columns(r)] = m
                held[j, r] = m
                if j % 2 == 1 or j == groups - 1:
                    start = j if j % 2 == 0 else j - 1
                    both = [held[start, r], held[j, r] if j > start else jnp.zeros_like(m)]
                    hi, lw = split(jnp.concatenate(both, axis=0))
                    mh[pl.ds(store + 8 * start, 16), columns(r)] = hi
                    ml[pl.ds(store + 8 * start, 16), columns(r)] = lw

    def propagate(c, outer, gain, halo, row_set, sums):
        base = pl.multiple_of(c * (pair * rows), 8)
        at = pl.multiple_of(c * pitch, 16)
        store = pl.multiple_of(c * pitch + pitch, 16)
        sums = dict(sums)
        held = {}
        for j in range(groups):
            low, high = 8 * j < nd, 8 * j + 8 > nd
            if low and high:
                g = jnp.where(eight < nd - 8 * j, gain[0], gain[1])
            else:
                g = jnp.broadcast_to(gain[0] if low else gain[1], (8, LANES))
            ax = g * table[8 * j : 8 * j + 8, :]
            ay = g * table[pair + 8 * j : pair + 8 * j + 8, :]
            stay = 1.0 - ax - ay
            e = [x[pl.ds(base + 8 * rows * j + r, 8, stride=rows), :] for r in range(rows)]
            if sums:
                w0, w1 = weight0[pl.ds(at + 8 * j, 8), :], weight1[pl.ds(at + 8 * j, 8), :]
            for r in row_set:
                rim = lane == choose(forward[j], lambda: 0, lambda: LANES - 1)
                nx = jnp.where(rim, halo(r, j), upwind(e[r], j))
                ny = choose(
                    southern[j],
                    lambda: e[r - 1] if r > 0 else outer(j),
                    lambda: e[r + 1] if r < rows - 1 else outer(j),
                )
                m = (stay * e[r] + ax * nx + ay * ny) * sea[r : r + 1, :]
                mf[pl.ds(at + 8 * j, 8), columns(r)] = m
                held[j, r] = m
                if sums:
                    for i, v in enumerate((m, m * w0, m * w1)):
                        sums[r, i] = sums[r, i] + v
                if j % 2 == 1 or j == groups - 1:
                    start = j if j % 2 == 0 else j - 1
                    both = [held[start, r], held[j, r] if j > start else jnp.zeros_like(m)]
                    hi, lw = split(jnp.concatenate(both, axis=0))
                    mh[pl.ds(store + 8 * start, 16), columns(r)] = hi
                    ml[pl.ds(store + 8 * start, 16), columns(r)] = lw
        return sums

    def interact(c, cs):
        width = (cs.stop - cs.start) // LANES
        at = pl.multiple_of(c * pitch, 16)
        lhs = pick[pl.ds(pl.multiple_of(2 * at, 16), 2 * pitch), :window]
        both = jnp.dot(lhs, mh[pl.ds(at, window), cs], preferred_element_type=F32)
        both = both + jnp.dot(lhs, ml[pl.ds(at, window), cs], preferred_element_type=F32)
        third, fourth = both[:pitch], both[pitch:]
        e = mf[pl.ds(at, pitch), cs]
        scale = jnp.concatenate([coefs[pl.ds(at, pitch), :]] * width, axis=1)
        product = third * fourth
        moved = (scale * e) * (e * (third + fourth) - (product + product))
        hi, lw = split(moved)
        to = pl.multiple_of(at + pitch, 16)
        th[pl.ds(to, pitch), cs] = hi
        tl[pl.ds(to, pitch), cs] = lw

    def finish(c, cs):
        finish_chunk(
            c, first, cs, (nd, rows), (put, th, tl, shapes, mf), result,
            lambda r: time_step * wind[r : r + 1, :], lambda r: 1.0,
        )

    def run(what, begin, count, cs, at_once):
        def body(t, carry):
            for u in range(at_once):
                what(begin + t * at_once + u, cs)
            return carry

        lax.fori_loop(0, count // at_once, body, 0)
        for u in range(count - count % at_once, count):
            what(begin + u, cs)

    def receive(ref, first_row, where):
        for i in range(len(where)):
            at = first_row + half * where[i]
            ref[pl.ds(nd * i, half), :] = got_up[pl.ds(at, half), :]
            ref[pl.ds(nd * i + half, half), :] = got_down[pl.ds(at, half), :]

    names = [(r, i) for r in range(rows) for i in range(3)]

    def prepare_own(t, sums):
        sums = dict(zip(names, sums))
        for u in range(step):
            c = first + t * step + u
            prepare(c, [gains[pl.ds(2 * c + i, 1), :] for i in range(2)], sums)
        return tuple(sums[n] for n in names)

    place = lane >> 2 if rows == 4 else lax.div(lane, rows)
    held_rates = pltpu.roll(own_rates, EDGE * fi, 1)
    rate = [
        jnp.take_along_axis(held_rates, jnp.minimum(2 * place + i, LANES - 1), axis=1)[0:1]
        for i in range(2)
    ]
    for j in range(groups):
        here = slice(8 * j, 8 * j + 8)
        ax, _ = rates_of(j, rate)
        heavy = [jnp.zeros((8, LANES), F32) for _ in range(2)]
        for u in range(own_chunks):
            at = pl.multiple_of((first + u) * pitch, 8) + 8 * j
            for i, ref in enumerate((weight0, weight1)):
                heavy[i] = jnp.where(place == first + u, ref[pl.ds(at, 8), :], heavy[i])
        rim_weights[0, here, :] = ax
        rim_weights[1, here, :] = ax * heavy[0]
        rim_weights[2, here, :] = ax * heavy[1]
    zeros = tuple(jnp.zeros((8, LANES), F32) for _ in names)
    sums = dict(zip(names, lax.fori_loop(0, own_chunks // step, prepare_own, zeros)))
    speed_copy().wait_recv()
    rates[0:1, 0:nf] = speed_far[...].reshape(1, nf)
    gains_far[...] = jnp.broadcast_to(
        pltpu.roll(rates[...], fi * (LANES - (nf - EDGE)), 1).T[0:8, 0:1], gains_far.shape
    )

    lon_copy(True).wait_recv()
    lon_copy(False).wait_recv()
    ends = []
    for side, source in ((True, got_left), (False, got_right)):
        for i in range(3):
            total = jnp.zeros((8, LANES), F32)
            for j in range(groups):
                flags = [flag == side for flag in forward[j]]
                if any(flags):
                    here = slice(8 * j, 8 * j + 8)
                    term = rim_weights[i, here, :] * source[here, :]
                    total = total + choose(flags, lambda: term, lambda: jnp.zeros_like(term))
            ends.append(jnp.sum(total, axis=0, keepdims=True))
    ends = jnp.concatenate(ends + [jnp.zeros((2, LANES), F32)], axis=0)
    lanes_left = LANES
    while lanes_left > rows:
        lanes_left //= 2
        ends = ends + pltpu.roll(ends, lanes_left, 1)
    for j in range(groups):
        here = slice(8 * j, 8 * j + 8)
        got_left[here, :] = choose(
            forward[j],
            lambda: got_left[here, :],
            lambda: pltpu.roll(got_right[here, :], LANES - 1, 1),
        )

    def own(row_set, columns_too, rows_too):
        def body(t, carry):
            for u in range(step):
                c = first + t * step + u

                def halo(r, j):
                    return pltpu.roll(got_left[8 * j : 8 * j + 8, :], LANES - (c * rows + r), 1)

                def outer(j):
                    return edge[pl.ds(pl.multiple_of((c - first) * pair, 8) + 8 * j, 8), :]

                gain = [gains[pl.ds(2 * c + i, 1), :] for i in range(2)]
                complete(c, gain, row_set, rows_too, outer, halo if columns_too else None)
            return carry

        lax.fori_loop(0, own_chunks // step, body, 0)

    def edge_sums(t, sums):
        sums = list(sums)
        for u in range(step):
            c = first + t * step + u
            at = pl.multiple_of(c * pitch, 16)
            gain = [gains[pl.ds(2 * c + i, 1), :] for i in range(2)]
            for j in range(groups):
                _, ay = rates_of(j, gain)
                term = ay * edge[pl.ds(pl.multiple_of((c - first) * pair, 8) + 8 * j, 8), :]
                terms = (
                    term,
                    term * weight0[pl.ds(at + 8 * j, 8), :],
                    term * weight1[pl.ds(at + 8 * j, 8), :],
                )
                for side in range(2):
                    flags = [flag == (side == 0) for flag in southern[j]]
                    if any(flags):
                        for i, v in enumerate(terms):
                            sums[3 * side + i] = sums[3 * side + i] + choose(
                                flags, lambda: v, lambda: jnp.zeros_like(v)
                            )
        return tuple(sums)

    near_first = 2 * first - fi
    near_count = chunks - far_chunks - 1
    last_first = 2 * first
    last_count = chunks - 2 * far_chunks
    own(inner, True, True)

    @pl.when(jnp.logical_not(down_ok))
    def _():
        own(rim_rows, True, False)

    @pl.when(down_ok)
    def _():
        lat_copy(True).wait_recv()

    @pl.when(up_ok)
    def _():
        lat_copy(False).wait_recv()

    receive(edge, far_lat, [places[f] for f in range(nf)])

    zeros = tuple(jnp.zeros((8, LANES), F32) for _ in range(6))
    from_rows = lax.fori_loop(0, own_chunks // step, edge_sums, zeros)

    def whole_sum(r, i):
        total = sums[r, i]
        if r == 0:
            total = total + from_rows[i]
        if r == rows - 1:
            total = total + from_rows[3 + i]
        total = jnp.sum(total, axis=0, keepdims=True)
        start = pltpu.roll(ends, (LANES - r) % LANES, 1)[i : i + 1]
        stop = pltpu.roll(ends, LANES - 1 - r, 1)[3 + i : 4 + i]
        total = total + jnp.where(lane[0:1] == 0, start, 0.0)
        total = total + jnp.where(lane[0:1] == LANES - 1, stop, 0.0)
        return total * sea[r : r + 1, :]

    energy[...] = jnp.zeros((8, LANES), F32)
    ids = (lo * LANES + lax.broadcasted_iota(jnp.int32, (all_rows, LANES), 1)) * all_rows
    ids = ids + lax.broadcasted_iota(jnp.int32, (all_rows, LANES), 0)
    totals = [jnp.zeros((all_rows, LANES), F32) for _ in range(2)]
    for r in range(rows):
        energy[r : r + 1, :] = whole_sum(r, 0)
        hit = cells[r : r + 1, :] == ids
        for i in range(2):
            tau = wind[r : r + 1, :] * whole_sum(r, 1 + i)
            totals[i] = totals[i] + jnp.where(hit, tau, 0.0)
    for i in range(2):
        tau_own[pl.ds(i * all_rows, all_rows), :] = totals[i]
    tau_copy(len(group) - 1).start()
    energy_copy().start()
    for s in range(len(group) - 1):
        tau_copy(s).start()


    @pl.when(down_ok)
    def _():
        own(rim_rows, True, False)

    own(rim_rows, False, True)
    run(interact, near_first, near_count, whole_cols, 4)
    run(finish, last_first, last_count, whole_cols, 4)

    @pl.when(down_ok)
    def _():
        lat_far_copy(True).wait_recv()

    @pl.when(up_ok)
    def _():
        lat_far_copy(False).wait_recv()

    receive(edge_far, 0, list(range(EDGE)))
    lon_far_copy(True).wait_recv()
    lon_far_copy(False).wait_recv()
    left, right = far_left[...].T, far_right[...].T
    for j in range(groups):
        here = slice(8 * j, 8 * j + 8)
        ahead = eight[:, 0:8] < 0
        for i, flag in enumerate(forward[j]):
            if flag:
                ahead = jnp.logical_or(ahead, eight[:, 0:8] == i)
        cols_far[here, :] = jnp.where(ahead, left[here], right[here])
    raw_copy(True).wait_recv()
    raw_copy(False).wait_recv()

    for u in range(far_chunks):
        def halo(r, j):
            k = u * rows + r
            return jnp.broadcast_to(cols_far[8 * j : 8 * j + 8, k : k + 1], (8, LANES))

        def outer(j):
            return edge_far[pair * u + 8 * j : pair * u + 8 * j + 8, :]

        gain = [gains_far[2 * u + i : 2 * u + i + 1, :] for i in range(2)]
        propagate(far_first + u, outer, gain, halo, range(rows), {})

    late = (chunks - far_chunks - 1) * other + fi
    run(interact, late, 2, whole_cols, 2)
    energy_copy().wait()
    factors[0:rows, :] = time_step * dissip[...] * ((energy[0:rows, :] + energy_got[0:rows, :]) / nbins)
    factors[rows : 2 * rows, :] = time_step * wind[...]

    raw_copy(True).wait_send()
    raw_copy(False).wait_send()
    speed_copy().wait_send()
    for flag in (True, False):
        lon_copy(flag).wait_send()
        lon_far_copy(flag).wait_send()

    @pl.when(up_ok)
    def _():
        lat_copy(True).wait_send()
        lat_far_copy(True).wait_send()

    @pl.when(down_ok)
    def _():
        lat_copy(False).wait_send()
        lat_far_copy(False).wait_send()

    st = tau_own[...]
    for s in range(len(group)):
        tau_copy(s).wait()
        st = st + taus[s]
    stress[...] = st


def write_kernel(
    sizes, before, mf, th, tl, put, shapes, factors, taus, spread_out, result_out, stress_out,
    result, stress, sems,
):
    n_lat, n_lon, n_freq, nf, nd, rows, nbins = sizes
    pair = 2 * nd
    pitch = round_up(pair, 16)
    own_chunks, far_chunks = nf // 2, EDGE // 2
    columns, (whole_cols, _, _) = layout(rows)[2:]
    fi = lax.axis_index("freq")
    first = far_chunks * fi
    size = pair * rows

    def out(i):
        here = pl.ds(pl.multiple_of(lax.rem(i + first, own_chunks) * size, 8), size)
        return pltpu.make_async_copy(result.at[here], result_out.at[here], sems.at[i])

    def settle(i, carry):
        t = lax.rem(i + first, own_chunks)
        at = pl.multiple_of((t + first) * pitch, 8)
        for r in range(rows):
            spot = pl.ds(t * size + r, pair, stride=rows)
            e = mf[pl.ds(at, pair), columns(r)]
            result[spot, :] = before[spot, :] - e * factors[r : r + 1, :]
        out(i).start()
        return carry

    settled = own_chunks - far_chunks
    lax.fori_loop(0, settled, settle, 0)
    for i in range(settled, own_chunks):
        finish_chunk(
            lax.rem(i + first, own_chunks) + first, first, whole_cols, (nd, rows),
            (put, th, tl, shapes, mf), result,
            lambda r: factors[rows + r : rows + r + 1, :], lambda r: 1.0 - factors[r : r + 1, :],
        )
    for i in range(settled, own_chunks):
        out(i).start()

    all_rows = n_lat * rows
    share = (LANES // n_freq) * all_rows
    st = taus[...]
    wide = sum(
        jnp.dot(term, spread_out[...], preferred_element_type=F32) for term in thirds(st)
    )
    place = lax.broadcasted_iota(jnp.int32, (all_rows, share), 1) & (all_rows - 1)
    own_row = place == lax.broadcasted_iota(jnp.int32, (all_rows, share), 0)
    for i in range(2):
        picked = jnp.where(own_row, wide[i * all_rows : (i + 1) * all_rows], 0.0)
        stress[i : i + 1, :] = jnp.sum(picked, axis=0, keepdims=True)
    last = pltpu.make_async_copy(stress, stress_out, sems.at[own_chunks])
    last.start()

    def wait(i, carry):
        out(i).wait()
        return carry

    lax.fori_loop(0, own_chunks, wait, 0)
    last.wait()


def local(
    axes,
    spectrum,
    group_speed,
    sea_mask,
    wind_growth,
    dissipation,
    wind_profile,
    nonlinear_coef,
    momentum,
    quadruplet,
    ocean_cell,
):
    n_lat, n_lon, n_freq = axes
    nf, nd, rows, width = spectrum.shape
    nbins = wind_profile.shape[0]
    assert n_freq == 2 and nf % 2 == 0 and width == LANES
    band, pair, half = nf * nd, 2 * nd, nd // 2
    pitch = round_up(pair, 16)
    chunks = nf // 2 + EDGE // 2
    all_rows = n_lat * rows
    angles = (np.float32(2.0 * np.pi) * np.arange(nd, dtype=np.float32) / np.float32(nd)).astype(
        np.float32
    )
    cosines, sines = np.cos(angles), np.sin(angles)
    waves = np.zeros((8, LANES), np.float32)
    waves[0, :pair], waves[1, :pair] = np.tile(np.abs(cosines), 2), np.tile(np.abs(sines), 2)

    packed = round_up(nf * half, 8)
    far_lat = EDGE * half
    share = (width // n_freq) * all_rows
    span = round_up(max(nbins, (chunks + 2) * pitch), LANES)
    reach = round_up(3 * pitch, LANES)
    vmem = pl.BlockSpec(memory_space=VMEM)
    hbm = pl.BlockSpec(memory_space=pltpu.HBM)
    sizes = (n_lat, n_lon, n_freq, nf, nd, rows, nbins)
    dma = pltpu.SemaphoreType.DMA
    smalls = (
        group_speed,
        jnp.asarray(waves),
        wind_profile,
        nonlinear_coef,
        momentum,
        quadruplet,
        sea_mask,
        wind_growth,
        dissipation,
        ocean_cell,
    )
    between = [
        jax.ShapeDtypeStruct(shape, dtype)
        for shape, dtype in (
            ((band * rows, width), F32),
            ((chunks * pitch, rows * width), F32),
            (((chunks + 2) * pitch, rows * width), BF16),
            (((chunks + 2) * pitch, rows * width), BF16),
            ((chunks * pitch, reach), BF16),
            ((chunks * pitch, width), F32),
            ((2 * rows, width), F32),
            ((2 * all_rows, width), F32),
            ((width, share), BF16),
        )
    ]
    made = pl.pallas_call(
        functools.partial(wave_kernel, sizes, (cosines, sines)),
        out_shape=between,
        in_specs=[hbm] * 11,
        out_specs=[vmem] * len(between),
        scratch_shapes=[VMEM(a.shape, a.dtype) for a in smalls]
        + [
            VMEM((chunks * pair * rows, width), F32),
            VMEM(((chunks + 2) * pitch, rows * width), BF16),
            VMEM(((chunks + 2) * pitch, rows * width), BF16),
            VMEM((2 * chunks * pitch, reach), BF16),
            VMEM((2 * pair, width), F32),
            VMEM((8, width), F32),
            VMEM((span, 8), F32),
            VMEM((8, span), F32),
            VMEM((chunks * pitch, width), F32),
            VMEM((chunks * pitch, width), F32),
            VMEM((chunks * pitch, width), F32),
            VMEM((3, pair, width), F32),
            VMEM((round_up(nf + EDGE, 8), width), F32),
            VMEM((8, width), F32),
            VMEM(group_speed.shape, F32),
            VMEM((packed, width), F32),
            VMEM((packed, width), F32),
            VMEM((far_lat + packed, width), F32),
            VMEM((far_lat + packed, width), F32),
            VMEM((band, width), F32),
            VMEM((EDGE * nd, width), F32),
            VMEM((pair, width), F32),
            VMEM((pair, width), F32),
            VMEM((pair, width), F32),
            VMEM((8, width), F32),
            VMEM((8, width), F32),
            VMEM((8, width), F32),
            VMEM((pair, 8), F32),
            VMEM((8, width), F32),
            VMEM((8, width), F32),
            VMEM((2 * all_rows, width), F32),
            VMEM((n_lat * n_freq - 1, 2 * all_rows, width), F32),
            dma((nf // 2,)), dma((len(smalls),)),
            *[pltpu.SemaphoreType.REGULAR] * 3,
            dma((3,)), dma((3,)), dma((4,)), dma((4,)), dma((4,)), dma((4,)),
            dma((1,)), dma((1,)), dma((n_lat * n_freq - 1,)), dma((n_lat * n_freq - 1,)),
        ],
        compiler_params=pltpu.CompilerParams(
            collective_id=0, has_side_effects=True, vmem_limit_bytes=32 << 20
        ),
    )(
        *[
            pltpu.with_memory_space_constraint(a, pltpu.HBM)
            for a in (spectrum.reshape(band * rows, width), *smalls)
        ]
    )
    out, ocean = pl.pallas_call(
        functools.partial(write_kernel, sizes),
        out_shape=(
            jax.ShapeDtypeStruct((band * rows, width), F32),
            jax.ShapeDtypeStruct((2, share), F32),
        ),
        in_specs=[vmem] * len(between),
        out_specs=(hbm, hbm),
        scratch_shapes=[
            VMEM((band * rows, width), F32), VMEM((2, share), F32), dma((nf // 2 + 1,)),
        ],
        compiler_params=pltpu.CompilerParams(vmem_limit_bytes=16 << 20),
    )(*made)
    return out.reshape(spectrum.shape), ocean.T


def solution(mesh):
    axes = tuple(mesh.shape[a] for a in ("lat", "lon", "freq"))
    return jax.shard_map(
        functools.partial(local, axes),
        mesh=mesh,
        in_specs=(
            P("freq", None, "lat", "lon"),
            P("freq"),
            P("lat", "lon"),
            P("lat", "lon"),
            P("lat", "lon"),
            P(),
            P(),
            P(),
            P(),
            P("lat", "lon"),
        ),
        out_specs=(P("freq", None, "lat", "lon"), P(("lon", "freq"), None)),
        check_vma=False,
    )
```

```python
import functools

import jax
import jax.numpy as jnp
import numpy as np
from jax import lax
from jax.experimental import pallas as pl
from jax.experimental.pallas import tpu as pltpu
from jax.sharding import PartitionSpec as P

time_step = 0.5
MESH = pl.DeviceIdType.MESH
VMEM = pltpu.VMEM
LANES = 128
EDGE = 4
F32, BF16 = jnp.float32, jnp.bfloat16


def spread(nf):
    order = list(range(EDGE)) + list(range(nf - EDGE, nf)) + list(range(EDGE, nf - EDGE))
    return {f: i for i, f in enumerate(order)}


def round_up(n, m):
    return -(-n // m) * m


def split(v):
    high = v.astype(BF16)
    return high, (v - high.astype(F32)).astype(BF16)


def thirds(v):
    high, low = split(v)
    rest = v - high.astype(F32) - low.astype(F32)
    return high, low, rest.astype(BF16)


def layout(rows):
    inner, rim_rows = list(range(1, rows - 1)), [0, rows - 1]
    slot = {r: i for i, r in enumerate(inner + rim_rows)}

    def columns(r):
        return slice(slot[r] * LANES, slot[r] * LANES + LANES)

    whole = slice(0, rows * LANES)
    split_at = len(inner) * LANES
    return inner, rim_rows, columns, (whole, slice(0, split_at), slice(split_at, rows * LANES))


def finish_chunk(c, first, cs, shape, refs, result, growth, stay):
    nd, rows = shape
    put, th, tl, shapes, mf = refs
    pair = 2 * nd
    pitch = round_up(pair, 16)
    window = 3 * pitch
    columns = layout(rows)[2]
    at = pl.multiple_of(c * pitch, 16)
    lhs = put[pl.ds(at, pitch), :window]
    back = jnp.dot(lhs, th[pl.ds(at, window), cs], preferred_element_type=F32)
    back = back + jnp.dot(lhs, tl[pl.ds(at, window), cs], preferred_element_type=F32)
    profile = shapes[pl.ds(at, pair), :]
    to = (c - first) * (pair * rows)
    for r in range(rows):
        here = columns(r)
        if here.start < cs.start or here.stop > cs.stop:
            continue
        e = mf[pl.ds(at, pair), here]
        gain = back[:pair, here.start - cs.start : here.stop - cs.start]
        result[pl.ds(to + r, pair, stride=rows), :] = e * (stay(r) + profile * growth(r)) + gain


def wave_kernel(sizes, angles, spectrum, *refs):
    sources, refs = refs[:10], refs[10:]
    result, mf, th, tl, put, shapes, factors, stress, spread_out, *refs = refs
    inputs, refs = refs[:10], refs[10:]
    speed, waves, profile, coef, momentum, quad, mask, wind, dissip, cells = inputs
    (
        x, mh, ml, pick, table, rates, cols, lines, coefs, weight0, weight1, rim_weights,
        gains, gains_far, speed_far, pack_up, pack_down, got_up, got_down, edge, edge_far,
        lon_pack, got_left, got_right, lon_far, far_left, far_right, cols_far, energy, energy_got, tau_own, taus,
        load_sem, small_sem, lat_ready, diag_ready, lon_ready, raw_send, raw_recv, lat_send, lat_recv, lon_send, lon_recv,
        sum_send, sum_recv, tau_send, tau_recv,
    ) = refs
    n_lat, n_lon, n_freq, nf, nd, rows, nbins = sizes
    half = nd // 2
    pair = 2 * nd
    band = nf * nd
    all_rows = n_lat * rows
    pitch = round_up(pair, 16)
    pad = pitch - pair
    own_chunks = nf // 2
    far_chunks = EDGE // 2
    chunks = own_chunks + far_chunks
    window = 3 * pitch
    reach = round_up(window, LANES)
    span = lines.shape[1]
    places = spread(nf)
    groups = pair // 8
    cosines, sines = angles
    li, lo, fi = lax.axis_index("lat"), lax.axis_index("lon"), lax.axis_index("freq")
    other = 1 - fi
    first = far_chunks * fi
    far_first = own_chunks * other

    own_rows = pl.multiple_of(first * (pair * rows), 8)
    small = [
        pltpu.make_async_copy(a, b, small_sem.at[i])
        for i, (a, b) in enumerate(zip(sources, inputs))
    ]
    step = 3 if own_chunks % 3 == 0 else 1
    loads = []
    for i in range(own_chunks // step):
        count = step * pair * rows
        loads.append(
            pltpu.make_async_copy(
                spectrum.at[pl.ds(i * count, count)], x.at[pl.ds(own_rows + i * count, count)],
                load_sem.at[i],
            )
        )
    for copy in loads + small:
        copy.start()

    east, west = lax.rem(lo + 1, n_lon), lax.rem(lo + n_lon - 1, n_lon)
    group = []
    for s in range(1, n_lat * n_freq):
        dl, df = divmod(s, n_freq)
        group.append({"lat": lax.rem(li + dl, n_lat), "freq": lax.rem(fi + df, n_freq)})
    barrier = pltpu.get_barrier_semaphore()
    last = n_lon - 1
    higher = [li + dl < n_lat for dl in range(1, n_lat)]
    lat_peer = [
        [{"lat": lax.rem(li + dl, n_lat), "freq": f} for f in range(n_freq)] for dl in range(1, n_lat)
    ]
    beside = {
        side: [{"lon": side_at, "freq": f} for f in range(n_freq)]
        for side, side_at in (("east", east), ("west", west))
    }

    def signal(semaphore, peers):
        for peer in peers:
            pl.semaphore_signal(semaphore, inc=1, device_id=peer, device_id_type=MESH)

    def signal_if(condition, semaphore, peers):
        @pl.when(condition)
        def _():
            signal(semaphore, peers)

    signal(barrier, [{"freq": other}])
    for up, (in_first, in_second) in zip(higher, lat_peer):
        signal_if(jnp.logical_or(fi == 0, up), barrier, [in_first])
        signal_if(up, barrier, [in_second])
    signal_if(lo < last, barrier, beside["east"])
    signal_if(lo == 0, barrier, beside["west"])
    at_start, at_end = lax.div(last - lo, last), lax.div(lo, last)
    greeted = 1 + other * (n_lat - 1 + li) + fi * (2 * li) + 2 * (1 - at_start) + 2 * at_end
    answers_lat = n_lat - 1 - li
    answers_lon = 2 * (1 - at_end) + 2 * at_start

    def enter():
        pl.semaphore_wait(barrier, greeted)
        speed_copy().start()
        raw_copy(True).start()
        for up, (in_first, in_second) in zip(higher, lat_peer):
            signal_if(jnp.logical_and(fi == 1, jnp.logical_not(up)), lat_ready, [in_second])
            signal_if(jnp.logical_and(fi == 1, jnp.logical_not(up)), diag_ready, [in_first])
            signal_if(jnp.logical_and(fi == 0, jnp.logical_not(up)), diag_ready, [in_second])
        signal_if(lo > 0, lon_ready, beside["west"])
        signal_if(lo == last, lon_ready, beside["east"])

    packed = pack_up.shape[0]
    far_lat = EDGE * half
    up_ok, down_ok = li < n_lat - 1, li > 0

    def raw_copy(near):
        count = EDGE // 2 * nd * rows
        half_at = (other if near else fi) * count
        src = pl.multiple_of(other * ((nf - EDGE) * nd * rows) + half_at, 8)
        dst = pl.multiple_of(fi * (band * rows) + half_at, 8)
        i = 2 if near else 0
        return pltpu.make_async_remote_copy(
            spectrum.at[pl.ds(src, count)], x.at[pl.ds(dst, count)],
            raw_send.at[i], raw_recv.at[i], device_id={"freq": other}, device_id_type=MESH,
        )

    def speed_copy():
        return pltpu.make_async_remote_copy(
            sources[0], speed_far, raw_send.at[1], raw_recv.at[1],
            device_id={"freq": other}, device_id_type=MESH,
        )

    def lat_copy(up):
        src, dst = (pack_up, got_up) if up else (pack_down, got_down)
        i = int(up)
        return pltpu.make_async_remote_copy(
            src, dst.at[pl.ds(far_lat, packed)], lat_send.at[i], lat_recv.at[i],
            device_id={"lat": li + 1 if up else li - 1}, device_id_type=MESH,
        )

    def lat_far_copy(up):
        src, dst = (pack_up, got_up) if up else (pack_down, got_down)
        i = 2 + int(up)
        return pltpu.make_async_remote_copy(
            src.at[pl.ds(pl.multiple_of(other * far_lat, 8), far_lat)], dst.at[pl.ds(0, far_lat)],
            lat_send.at[i], lat_recv.at[i],
            device_id={"lat": li + 1 if up else li - 1, "freq": other}, device_id_type=MESH,
        )

    def lon_copy(to_east):
        i = int(to_east)
        return pltpu.make_async_remote_copy(
            lon_pack, got_left if to_east else got_right, lon_send.at[i], lon_recv.at[i],
            device_id={"lon": east if to_east else west}, device_id_type=MESH,
        )

    def lon_far_copy(to_east):
        i = 2 + int(to_east)
        return pltpu.make_async_remote_copy(
            lon_far, far_left if to_east else far_right, lon_send.at[i], lon_recv.at[i],
            device_id={"lon": east if to_east else west, "freq": other}, device_id_type=MESH,
        )

    def energy_copy():
        return pltpu.make_async_remote_copy(
            energy, energy_got, sum_send.at[0], sum_recv.at[0],
            device_id={"freq": other}, device_id_type=MESH,
        )

    def tau_copy(s):
        return pltpu.make_async_remote_copy(
            tau_own, taus.at[s], tau_send.at[s], tau_recv.at[s],
            device_id=group[s], device_id_type=MESH,
        )

    def signs(values, j):
        return [bool(values[(8 * j + i) % nd] > 0.0) for i in range(8)]

    eight = lax.broadcasted_iota(jnp.int32, (8, LANES), 0)
    lane = lax.broadcasted_iota(jnp.int32, (8, LANES), 1)

    def rows_of(flags):
        spot = None
        for i, flag in enumerate(flags):
            if flag:
                here = eight == i
                spot = here if spot is None else jnp.logical_or(spot, here)
        return spot

    def choose(flags, yes, no):
        if all(flags):
            return yes()
        if not any(flags):
            return no()
        return jnp.where(rows_of(flags), yes(), no())

    forward = [signs(cosines, j) for j in range(groups)]
    southern = [[(8 * j + i) % nd < half for i in range(8)] for j in range(groups)]

    @pl.when(fi == 1)
    def _():
        enter()

    pack_up[pl.ds(packed - 8, 8), :] = jnp.zeros((8, LANES), F32)
    pack_down[pl.ds(packed - 8, 8), :] = jnp.zeros((8, LANES), F32)
    sums = [jnp.zeros((8, LANES), F32) for _ in range(groups)]
    for i, copy in enumerate(loads):
        if i == len(loads) - 1:

            @pl.when(fi == 0)
            def _():
                enter()

        copy.wait()
        for f in range(2 * step * i, 2 * step * (i + 1)):
            at = half * places[f]
            base = own_rows + nd * f * rows
            pack_up[pl.ds(at, half), :] = x[pl.ds(base + rows - 1, half, stride=rows), :]
            pack_down[pl.ds(at, half), :] = x[pl.ds(base + half * rows, half, stride=rows), :]
        for u in range(step):
            c = i * step + u + first
            base = pl.multiple_of(c * (pair * rows), 8)
            for r in range(rows):
                k = c * rows + r
                for j in range(groups):
                    e = x[pl.ds(base + 8 * rows * j + r, 8, stride=rows), :]
                    z = choose(
                        forward[j],
                        lambda: jnp.where(lane == LANES - 1, e, 0.0),
                        lambda: jnp.where(lane == 0, e, 0.0),
                    )
                    sums[j] = sums[j] + pltpu.roll(z, k, 1)

    for j in range(groups):
        aligned = choose(forward[j], lambda: pltpu.roll(sums[j], 1, 1), lambda: sums[j])
        lon_pack[8 * j : 8 * j + 8, :] = aligned

    begin = (first + (own_chunks - far_chunks) * other) * rows
    whole = jnp.concatenate(
        [lon_pack[...], jnp.zeros((LANES - pair, LANES), F32)], axis=0
    )
    turned = pltpu.roll(whole, lax.rem(LANES - begin, LANES), 1).T
    lon_far[...] = turned[0:8, :]

    def send_columns(answered):
        if answered:
            pl.semaphore_wait(lon_ready, answers_lon)
        for to_east in (True, False):
            lon_copy(to_east).start()
            lon_far_copy(to_east).start()

    @pl.when(lo == last)
    def _():
        send_columns(False)

    @pl.when(jnp.logical_and(fi == 1, up_ok))
    def _():
        pl.semaphore_wait(lat_ready, answers_lat)

    @pl.when(up_ok)
    def _():
        lat_copy(True).start()

    @pl.when(down_ok)
    def _():
        lat_copy(False).start()

    @pl.when(up_ok)
    def _():
        pl.semaphore_wait(diag_ready, answers_lat)
        lat_far_copy(True).start()

    @pl.when(down_ok)
    def _():
        lat_far_copy(False).start()

    raw_copy(False).start()

    for copy in small:
        copy.wait()
    rates[...] = jnp.zeros_like(rates)
    rates[0:1, 0:nf] = speed[...].reshape(1, nf)
    own_rates = rates[...]
    gains[...] = jnp.broadcast_to(
        pltpu.roll(rates[...], EDGE * fi, 1).T[0 : gains.shape[0], 0:1], gains.shape
    )
    bin0 = fi * ((nf - EDGE) * nd)
    lines[...] = jnp.zeros_like(lines)
    target = (quad[...] - bin0).astype(F32)
    shift = jnp.zeros_like(target)
    for i in range(1, chunks):
        shift = shift + jnp.where(target >= float(pair * i), float(pad), 0.0)
    lines[0:2, 0:nbins] = target + shift
    lines[2:3, 0:nbins] = time_step * coef[...].reshape(1, nbins)
    weight = profile[...].reshape(1, nbins)
    lines[3:4, 0:nbins] = weight
    lines[4:6, 0:nbins] = momentum[...] * weight
    lines[...] = pltpu.roll(lines[...], lax.rem(span - bin0, span), 1)
    cols[...] = jnp.full_like(cols, -1.0)
    for k in range(-(-chunks * pair // LANES)):
        block = lines[:, LANES * k : LANES * k + LANES].T
        at = LANES * k
        while at < min(LANES * (k + 1), chunks * pair):
            c = at // pair
            stop = min(pair * (c + 1), LANES * (k + 1))
            cols[at + pad * c : stop + pad * c, :] = block[at - LANES * k : stop - LANES * k]
            at = stop
    for k in range(span // LANES):
        lines[:, LANES * k : LANES * k + LANES] = cols[LANES * k : LANES * k + LANES, :].T
    turned = waves[...].T
    table[pl.ds(0, pair), :] = jnp.broadcast_to(turned[0:pair, 0:1], (pair, LANES))
    table[pl.ds(pair, pair), :] = jnp.broadcast_to(turned[0:pair, 1:2], (pair, LANES))

    @pl.when(jnp.logical_and(lo > 0, lo < last))
    def _():
        send_columns(True)

    @pl.when(jnp.logical_not(down_ok))
    def _():
        got_up[...] = jnp.zeros_like(got_up)

    @pl.when(jnp.logical_not(up_ok))
    def _():
        got_down[...] = jnp.zeros_like(got_down)

    for ref in (mh, ml, th, tl):
        for at in (0, (chunks + 1) * pitch):
            ref[pl.ds(at, pitch), :] = jnp.zeros((pitch, ref.shape[1]), BF16)
    lanes = lax.broadcasted_iota(jnp.int32, (pitch, reach), 1)
    below = lax.broadcasted_iota(jnp.int32, (pitch, reach), 0)
    own_bin = lanes == below + pitch

    def build(c, carry):
        at = pl.multiple_of(pitch * c, 8)
        where = (lanes + (at - pitch)).astype(F32)
        for i in range(2):
            chosen = jnp.where(cols[pl.ds(at, pitch), i : i + 1] == where, 1.0, 0.0)
            pick[pl.ds(pl.multiple_of(2 * at + pitch * i, 16), pitch), :] = chosen.astype(BF16)
        row = (below + at).astype(F32)
        line = pltpu.roll(lines[...], lax.rem(span + pitch - at, span), 1)
        given = jnp.where(own_bin, -2.0, 0.0)
        for i in range(2):
            given = given + jnp.where(line[i : i + 1, :reach] == row, 1.0, 0.0)
        put[pl.ds(pl.multiple_of(at, 16), pitch), :] = given.astype(BF16)
        for i, ref in enumerate((coefs, shapes, weight0, weight1)):
            ref[pl.ds(at, pitch), :] = jnp.broadcast_to(
                cols[pl.ds(at, pitch), 2 + i : 3 + i], (pitch, LANES)
            )
        mf[pl.ds(at + pair, pad), :] = jnp.zeros((pad, mf.shape[1]), F32)
        return carry

    lax.fori_loop(0, chunks, build, 0)
    share = (LANES // n_freq) * all_rows
    cell = lax.broadcasted_iota(jnp.int32, (LANES, share), 1)
    first_cell = (lax.broadcasted_iota(jnp.int32, (LANES, share), 0) - fi * (LANES // n_freq)) * all_rows
    inside = jnp.logical_and(cell >= first_cell, cell < first_cell + all_rows)
    spread_out[...] = jnp.where(inside, 1.0, 0.0).astype(BF16)

    @pl.when(lo == 0)
    def _():
        send_columns(True)

    sea = mask[...].astype(F32)

    inner, rim_rows, columns, (whole_cols, inner_cols, rim_cols) = layout(rows)

    def upwind(e, j):
        if all(forward[j]):
            return pltpu.roll(e, 1, 1)
        if not any(forward[j]):
            return pltpu.roll(e, LANES - 1, 1)
        at = lane + jnp.where(rows_of(forward[j]), LANES - 1, 1)
        return jnp.take_along_axis(e, at & (LANES - 1), axis=1)

    def rates_of(j, gain):
        low, high = 8 * j < nd, 8 * j + 8 > nd
        if low and high:
            g = jnp.where(eight < nd - 8 * j, gain[0], gain[1])
        else:
            g = jnp.broadcast_to(gain[0] if low else gain[1], (8, LANES))
        return g * table[8 * j : 8 * j + 8, :], g * table[pair + 8 * j : pair + 8 * j + 8, :]

    def rim_lane(j):
        return lane == choose(forward[j], lambda: 0, lambda: LANES - 1)

    def prepare(c, gain, sums):
        base = pl.multiple_of(c * (pair * rows), 8)
        at = pl.multiple_of(c * pitch, 16)
        zero = jnp.zeros((8, LANES), F32)
        for j in range(groups):
            ax, ay = rates_of(j, gain)
            stay = 1.0 - ax - ay
            weights = weight0[pl.ds(at + 8 * j, 8), :], weight1[pl.ds(at + 8 * j, 8), :]
            e = [x[pl.ds(base + 8 * rows * j + r, 8, stride=rows), :] for r in range(rows)]
            for r in range(rows):
                nx = jnp.where(rim_lane(j), 0.0, upwind(e[r], j))
                ny = choose(
                    southern[j],
                    lambda: e[r - 1] if r > 0 else zero,
                    lambda: e[r + 1] if r < rows - 1 else zero,
                )
                m = stay * e[r] + ax * nx + ay * ny
                mf[pl.ds(at + 8 * j, 8), columns(r)] = m
                for i, v in enumerate((m, m * weights[0], m * weights[1])):
                    sums[r, i] = sums[r, i] + v

    def complete(c, gain, row_set, keep, outer=None, halo=None):
        at = pl.multiple_of(c * pitch, 16)
        store = pl.multiple_of(c * pitch + pitch, 16)
        held = {}
        for j in range(groups):
            ax, ay = rates_of(j, gain)
            for r in row_set:
                m = mf[pl.ds(at + 8 * j, 8), columns(r)]
                if halo:
                    m = m + ax * jnp.where(rim_lane(j), halo(r, j), 0.0)
                if not keep:
                    mf[pl.ds(at + 8 * j, 8), columns(r)] = m
                    continue
                from_edge = [
                    (r == 0 and south) or (r == rows - 1 and not south) for south in southern[j]
                ]
                if any(from_edge):
                    zero = jnp.zeros((8, LANES), F32)
                    m = m + ay * choose(from_edge, lambda: outer(j), lambda: zero)
                m = m * sea[r : r + 1, :]
                mf[pl.ds(at + 8 * j, 8), columns(r)] = m
                held[j, r] = m
                if j % 2 == 1 or j == groups - 1:
                    start = j if j % 2 == 0 else j - 1
                    both = [held[start, r], held[j, r] if j > start else jnp.zeros_like(m)]
                    hi, lw = split(jnp.concatenate(both, axis=0))
                    mh[pl.ds(store + 8 * start, 16), columns(r)] = hi
                    ml[pl.ds(store + 8 * start, 16), columns(r)] = lw

    def propagate(c, outer, gain, halo, row_set, sums):
        base = pl.multiple_of(c * (pair * rows), 8)
        at = pl.multiple_of(c * pitch, 16)
        store = pl.multiple_of(c * pitch + pitch, 16)
        sums = dict(sums)
        held = {}
        for j in range(groups):
            low, high = 8 * j < nd, 8 * j + 8 > nd
            if low and high:
                g = jnp.where(eight < nd - 8 * j, gain[0], gain[1])
            else:
                g = jnp.broadcast_to(gain[0] if low else gain[1], (8, LANES))
            ax = g * table[8 * j : 8 * j + 8, :]
            ay = g * table[pair + 8 * j : pair + 8 * j + 8, :]
            stay = 1.0 - ax - ay
            e = [x[pl.ds(base + 8 * rows * j + r, 8, stride=rows), :] for r in range(rows)]
            if sums:
                w0, w1 = weight0[pl.ds(at + 8 * j, 8), :], weight1[pl.ds(at + 8 * j, 8), :]
            for r in row_set:
                rim = lane == choose(forward[j], lambda: 0, lambda: LANES - 1)
                nx = jnp.where(rim, halo(r, j), upwind(e[r], j))
                ny = choose(
                    southern[j],
                    lambda: e[r - 1] if r > 0 else outer(j),
                    lambda: e[r + 1] if r < rows - 1 else outer(j),
                )
                m = (stay * e[r] + ax * nx + ay * ny) * sea[r : r + 1, :]
                mf[pl.ds(at + 8 * j, 8), columns(r)] = m
                held[j, r] = m
                if sums:
                    for i, v in enumerate((m, m * w0, m * w1)):
                        sums[r, i] = sums[r, i] + v
                if j % 2 == 1 or j == groups - 1:
                    start = j if j % 2 == 0 else j - 1
                    both = [held[start, r], held[j, r] if j > start else jnp.zeros_like(m)]
                    hi, lw = split(jnp.concatenate(both, axis=0))
                    mh[pl.ds(store + 8 * start, 16), columns(r)] = hi
                    ml[pl.ds(store + 8 * start, 16), columns(r)] = lw
        return sums

    def interact(c, cs):
        width = (cs.stop - cs.start) // LANES
        at = pl.multiple_of(c * pitch, 16)
        lhs = pick[pl.ds(pl.multiple_of(2 * at, 16), 2 * pitch), :window]
        both = jnp.dot(lhs, mh[pl.ds(at, window), cs], preferred_element_type=F32)
        both = both + jnp.dot(lhs, ml[pl.ds(at, window), cs], preferred_element_type=F32)
        third, fourth = both[:pitch], both[pitch:]
        e = mf[pl.ds(at, pitch), cs]
        scale = jnp.concatenate([coefs[pl.ds(at, pitch), :]] * width, axis=1)
        product = third * fourth
        moved = (scale * e) * (e * (third + fourth) - (product + product))
        hi, lw = split(moved)
        to = pl.multiple_of(at + pitch, 16)
        th[pl.ds(to, pitch), cs] = hi
        tl[pl.ds(to, pitch), cs] = lw

    def finish(c, cs):
        finish_chunk(
            c, first, cs, (nd, rows), (put, th, tl, shapes, mf), result,
            lambda r: time_step * wind[r : r + 1, :], lambda r: 1.0,
        )

    def run(what, begin, count, cs, at_once):
        def body(t, carry):
            for u in range(at_once):
                what(begin + t * at_once + u, cs)
            return carry

        lax.fori_loop(0, count // at_once, body, 0)
        for u in range(count - count % at_once, count):
            what(begin + u, cs)

    def receive(ref, first_row, where):
        for i in range(len(where)):
            at = first_row + half * where[i]
            ref[pl.ds(nd * i, half), :] = got_up[pl.ds(at, half), :]
            ref[pl.ds(nd * i + half, half), :] = got_down[pl.ds(at, half), :]

    names = [(r, i) for r in range(rows) for i in range(3)]

    def prepare_own(t, sums):
        sums = dict(zip(names, sums))
        for u in range(step):
            c = first + t * step + u
            prepare(c, [gains[pl.ds(2 * c + i, 1), :] for i in range(2)], sums)
        return tuple(sums[n] for n in names)

    place = lane >> 2 if rows == 4 else lax.div(lane, rows)
    held_rates = pltpu.roll(own_rates, EDGE * fi, 1)
    rate = [
        jnp.take_along_axis(held_rates, jnp.minimum(2 * place + i, LANES - 1), axis=1)[0:1]
        for i in range(2)
    ]
    for j in range(groups):
        here = slice(8 * j, 8 * j + 8)
        ax, _ = rates_of(j, rate)
        heavy = [jnp.zeros((8, LANES), F32) for _ in range(2)]
        for u in range(own_chunks):
            at = pl.multiple_of((first + u) * pitch, 8) + 8 * j
            for i, ref in enumerate((weight0, weight1)):
                heavy[i] = jnp.where(place == first + u, ref[pl.ds(at, 8), :], heavy[i])
        rim_weights[0, here, :] = ax
        rim_weights[1, here, :] = ax * heavy[0]
        rim_weights[2, here, :] = ax * heavy[1]
    zeros = tuple(jnp.zeros((8, LANES), F32) for _ in names)
    sums = dict(zip(names, lax.fori_loop(0, own_chunks // step, prepare_own, zeros)))
    speed_copy().wait_recv()
    rates[0:1, 0:nf] = speed_far[...].reshape(1, nf)
    gains_far[...] = jnp.broadcast_to(
        pltpu.roll(rates[...], fi * (LANES - (nf - EDGE)), 1).T[0:8, 0:1], gains_far.shape
    )

    lon_copy(True).wait_recv()
    lon_copy(False).wait_recv()
    ends = []
    for side, source in ((True, got_left), (False, got_right)):
        for i in range(3):
            total = jnp.zeros((8, LANES), F32)
            for j in range(groups):
                flags = [flag == side for flag in forward[j]]
                if any(flags):
                    here = slice(8 * j, 8 * j + 8)
                    term = rim_weights[i, here, :] * source[here, :]
                    total = total + choose(flags, lambda: term, lambda: jnp.zeros_like(term))
            ends.append(jnp.sum(total, axis=0, keepdims=True))
    ends = jnp.concatenate(ends + [jnp.zeros((2, LANES), F32)], axis=0)
    lanes_left = LANES
    while lanes_left > rows:
        lanes_left //= 2
        ends = ends + pltpu.roll(ends, lanes_left, 1)
    for j in range(groups):
        here = slice(8 * j, 8 * j + 8)
        got_left[here, :] = choose(
            forward[j],
            lambda: got_left[here, :],
            lambda: pltpu.roll(got_right[here, :], LANES - 1, 1),
        )

    def own(row_set, columns_too, rows_too):
        def body(t, carry):
            for u in range(step):
                c = first + t * step + u

                def halo(r, j):
                    return pltpu.roll(got_left[8 * j : 8 * j + 8, :], LANES - (c * rows + r), 1)

                def outer(j):
                    return edge[pl.ds(pl.multiple_of((c - first) * pair, 8) + 8 * j, 8), :]

                gain = [gains[pl.ds(2 * c + i, 1), :] for i in range(2)]
                complete(c, gain, row_set, rows_too, outer, halo if columns_too else None)
            return carry

        lax.fori_loop(0, own_chunks // step, body, 0)

    def edge_sums(t, sums):
        sums = list(sums)
        for u in range(step):
            c = first + t * step + u
            at = pl.multiple_of(c * pitch, 16)
            gain = [gains[pl.ds(2 * c + i, 1), :] for i in range(2)]
            for j in range(groups):
                _, ay = rates_of(j, gain)
                term = ay * edge[pl.ds(pl.multiple_of((c - first) * pair, 8) + 8 * j, 8), :]
                terms = (
                    term,
                    term * weight0[pl.ds(at + 8 * j, 8), :],
                    term * weight1[pl.ds(at + 8 * j, 8), :],
                )
                for side in range(2):
                    flags = [flag == (side == 0) for flag in southern[j]]
                    if any(flags):
                        for i, v in enumerate(terms):
                            sums[3 * side + i] = sums[3 * side + i] + choose(
                                flags, lambda: v, lambda: jnp.zeros_like(v)
                            )
        return tuple(sums)

    near_first = 2 * first - fi
    near_count = chunks - far_chunks - 1
    last_first = 2 * first
    last_count = chunks - 2 * far_chunks
    own(inner, True, True)

    @pl.when(jnp.logical_not(down_ok))
    def _():
        own(rim_rows, True, False)

    @pl.when(down_ok)
    def _():
        lat_copy(True).wait_recv()

    @pl.when(up_ok)
    def _():
        lat_copy(False).wait_recv()

    receive(edge, far_lat, [places[f] for f in range(nf)])

    zeros = tuple(jnp.zeros((8, LANES), F32) for _ in range(6))
    from_rows = lax.fori_loop(0, own_chunks // step, edge_sums, zeros)

    def whole_sum(r, i):
        total = sums[r, i]
        if r == 0:
            total = total + from_rows[i]
        if r == rows - 1:
            total = total + from_rows[3 + i]
        total = jnp.sum(total, axis=0, keepdims=True)
        start = pltpu.roll(ends, (LANES - r) % LANES, 1)[i : i + 1]
        stop = pltpu.roll(ends, LANES - 1 - r, 1)[3 + i : 4 + i]
        total = total + jnp.where(lane[0:1] == 0, start, 0.0)
        total = total + jnp.where(lane[0:1] == LANES - 1, stop, 0.0)
        return total * sea[r : r + 1, :]

    energy[...] = jnp.zeros((8, LANES), F32)
    ids = (lo * LANES + lax.broadcasted_iota(jnp.int32, (all_rows, LANES), 1)) * all_rows
    ids = ids + lax.broadcasted_iota(jnp.int32, (all_rows, LANES), 0)
    totals = [jnp.zeros((all_rows, LANES), F32) for _ in range(2)]
    for r in range(rows):
        energy[r : r + 1, :] = whole_sum(r, 0)
        hit = cells[r : r + 1, :] == ids
        for i in range(2):
            tau = wind[r : r + 1, :] * whole_sum(r, 1 + i)
            totals[i] = totals[i] + jnp.where(hit, tau, 0.0)
    for i in range(2):
        tau_own[pl.ds(i * all_rows, all_rows), :] = totals[i]
    tau_copy(len(group) - 1).start()
    energy_copy().start()
    for s in range(len(group) - 1):
        tau_copy(s).start()


    @pl.when(down_ok)
    def _():
        own(rim_rows, True, False)

    own(rim_rows, False, True)
    run(interact, near_first, near_count, whole_cols, 8)
    run(finish, last_first, last_count, whole_cols, 7)

    @pl.when(down_ok)
    def _():
        lat_far_copy(True).wait_recv()

    @pl.when(up_ok)
    def _():
        lat_far_copy(False).wait_recv()

    receive(edge_far, 0, list(range(EDGE)))
    lon_far_copy(True).wait_recv()
    lon_far_copy(False).wait_recv()
    left, right = far_left[...].T, far_right[...].T
    for j in range(groups):
        here = slice(8 * j, 8 * j + 8)
        ahead = eight[:, 0:8] < 0
        for i, flag in enumerate(forward[j]):
            if flag:
                ahead = jnp.logical_or(ahead, eight[:, 0:8] == i)
        cols_far[here, :] = jnp.where(ahead, left[here], right[here])
    raw_copy(True).wait_recv()
    raw_copy(False).wait_recv()

    for u in range(far_chunks):
        def halo(r, j):
            k = u * rows + r
            return jnp.broadcast_to(cols_far[8 * j : 8 * j + 8, k : k + 1], (8, LANES))

        def outer(j):
            return edge_far[pair * u + 8 * j : pair * u + 8 * j + 8, :]

        gain = [gains_far[2 * u + i : 2 * u + i + 1, :] for i in range(2)]
        propagate(far_first + u, outer, gain, halo, range(rows), {})

    late = (chunks - far_chunks - 1) * other + fi
    run(interact, late, 2, whole_cols, 2)
    energy_copy().wait()
    factors[0:rows, :] = time_step * dissip[...] * ((energy[0:rows, :] + energy_got[0:rows, :]) / nbins)
    factors[rows : 2 * rows, :] = time_step * wind[...]

    raw_copy(True).wait_send()
    raw_copy(False).wait_send()
    speed_copy().wait_send()
    for flag in (True, False):
        lon_copy(flag).wait_send()
        lon_far_copy(flag).wait_send()

    @pl.when(up_ok)
    def _():
        lat_copy(True).wait_send()
        lat_far_copy(True).wait_send()

    @pl.when(down_ok)
    def _():
        lat_copy(False).wait_send()
        lat_far_copy(False).wait_send()

    st = tau_own[...]
    for s in range(len(group)):
        tau_copy(s).wait()
        st = st + taus[s]
    stress[...] = st


def write_kernel(
    sizes, before, mf, th, tl, put, shapes, factors, taus, spread_out, result_out, stress_out,
    result, stress, sems,
):
    n_lat, n_lon, n_freq, nf, nd, rows, nbins = sizes
    pair = 2 * nd
    pitch = round_up(pair, 16)
    own_chunks, far_chunks = nf // 2, EDGE // 2
    columns, (whole_cols, _, _) = layout(rows)[2:]
    fi = lax.axis_index("freq")
    first = far_chunks * fi
    size = pair * rows

    def out(i):
        here = pl.ds(pl.multiple_of(lax.rem(i + first, own_chunks) * size, 8), size)
        return pltpu.make_async_copy(result.at[here], result_out.at[here], sems.at[i])

    def settle(i, carry):
        t = lax.rem(i + first, own_chunks)
        at = pl.multiple_of((t + first) * pitch, 8)
        for r in range(rows):
            spot = pl.ds(t * size + r, pair, stride=rows)
            e = mf[pl.ds(at, pair), columns(r)]
            result[spot, :] = before[spot, :] - e * factors[r : r + 1, :]
        out(i).start()
        return carry

    settled = own_chunks - far_chunks
    lax.fori_loop(0, settled, settle, 0)
    for i in range(settled, own_chunks):
        finish_chunk(
            lax.rem(i + first, own_chunks) + first, first, whole_cols, (nd, rows),
            (put, th, tl, shapes, mf), result,
            lambda r: factors[rows + r : rows + r + 1, :], lambda r: 1.0 - factors[r : r + 1, :],
        )
    for i in range(settled, own_chunks):
        out(i).start()

    all_rows = n_lat * rows
    share = (LANES // n_freq) * all_rows
    st = taus[...]
    wide = sum(
        jnp.dot(term, spread_out[...], preferred_element_type=F32) for term in thirds(st)
    )
    place = lax.broadcasted_iota(jnp.int32, (all_rows, share), 1) & (all_rows - 1)
    own_row = place == lax.broadcasted_iota(jnp.int32, (all_rows, share), 0)
    for i in range(2):
        picked = jnp.where(own_row, wide[i * all_rows : (i + 1) * all_rows], 0.0)
        stress[i : i + 1, :] = jnp.sum(picked, axis=0, keepdims=True)
    last = pltpu.make_async_copy(stress, stress_out, sems.at[own_chunks])
    last.start()

    def wait(i, carry):
        out(i).wait()
        return carry

    lax.fori_loop(0, own_chunks, wait, 0)
    last.wait()


def local(
    axes,
    spectrum,
    group_speed,
    sea_mask,
    wind_growth,
    dissipation,
    wind_profile,
    nonlinear_coef,
    momentum,
    quadruplet,
    ocean_cell,
):
    n_lat, n_lon, n_freq = axes
    nf, nd, rows, width = spectrum.shape
    nbins = wind_profile.shape[0]
    assert n_freq == 2 and nf % 2 == 0 and width == LANES
    band, pair, half = nf * nd, 2 * nd, nd // 2
    pitch = round_up(pair, 16)
    chunks = nf // 2 + EDGE // 2
    all_rows = n_lat * rows
    angles = (np.float32(2.0 * np.pi) * np.arange(nd, dtype=np.float32) / np.float32(nd)).astype(
        np.float32
    )
    cosines, sines = np.cos(angles), np.sin(angles)
    waves = np.zeros((8, LANES), np.float32)
    waves[0, :pair], waves[1, :pair] = np.tile(np.abs(cosines), 2), np.tile(np.abs(sines), 2)

    packed = round_up(nf * half, 8)
    far_lat = EDGE * half
    share = (width // n_freq) * all_rows
    span = round_up(max(nbins, (chunks + 2) * pitch), LANES)
    reach = round_up(3 * pitch, LANES)
    vmem = pl.BlockSpec(memory_space=VMEM)
    hbm = pl.BlockSpec(memory_space=pltpu.HBM)
    sizes = (n_lat, n_lon, n_freq, nf, nd, rows, nbins)
    dma = pltpu.SemaphoreType.DMA
    smalls = (
        group_speed,
        jnp.asarray(waves),
        wind_profile,
        nonlinear_coef,
        momentum,
        quadruplet,
        sea_mask,
        wind_growth,
        dissipation,
        ocean_cell,
    )
    between = [
        jax.ShapeDtypeStruct(shape, dtype)
        for shape, dtype in (
            ((band * rows, width), F32),
            ((chunks * pitch, rows * width), F32),
            (((chunks + 2) * pitch, rows * width), BF16),
            (((chunks + 2) * pitch, rows * width), BF16),
            ((chunks * pitch, reach), BF16),
            ((chunks * pitch, width), F32),
            ((2 * rows, width), F32),
            ((2 * all_rows, width), F32),
            ((width, share), BF16),
        )
    ]
    made = pl.pallas_call(
        functools.partial(wave_kernel, sizes, (cosines, sines)),
        out_shape=between,
        in_specs=[hbm] * 11,
        out_specs=[vmem] * len(between),
        scratch_shapes=[VMEM(a.shape, a.dtype) for a in smalls]
        + [
            VMEM((chunks * pair * rows, width), F32),
            VMEM(((chunks + 2) * pitch, rows * width), BF16),
            VMEM(((chunks + 2) * pitch, rows * width), BF16),
            VMEM((2 * chunks * pitch, reach), BF16),
            VMEM((2 * pair, width), F32),
            VMEM((8, width), F32),
            VMEM((span, 8), F32),
            VMEM((8, span), F32),
            VMEM((chunks * pitch, width), F32),
            VMEM((chunks * pitch, width), F32),
            VMEM((chunks * pitch, width), F32),
            VMEM((3, pair, width), F32),
            VMEM((round_up(nf + EDGE, 8), width), F32),
            VMEM((8, width), F32),
            VMEM(group_speed.shape, F32),
            VMEM((packed, width), F32),
            VMEM((packed, width), F32),
            VMEM((far_lat + packed, width), F32),
            VMEM((far_lat + packed, width), F32),
            VMEM((band, width), F32),
            VMEM((EDGE * nd, width), F32),
            VMEM((pair, width), F32),
            VMEM((pair, width), F32),
            VMEM((pair, width), F32),
            VMEM((8, width), F32),
            VMEM((8, width), F32),
            VMEM((8, width), F32),
            VMEM((pair, 8), F32),
            VMEM((8, width), F32),
            VMEM((8, width), F32),
            VMEM((2 * all_rows, width), F32),
            VMEM((n_lat * n_freq - 1, 2 * all_rows, width), F32),
            dma((nf // 2,)), dma((len(smalls),)),
            *[pltpu.SemaphoreType.REGULAR] * 3,
            dma((3,)), dma((3,)), dma((4,)), dma((4,)), dma((4,)), dma((4,)),
            dma((1,)), dma((1,)), dma((n_lat * n_freq - 1,)), dma((n_lat * n_freq - 1,)),
        ],
        compiler_params=pltpu.CompilerParams(
            collective_id=0, has_side_effects=True, vmem_limit_bytes=32 << 20
        ),
    )(
        *[
            pltpu.with_memory_space_constraint(a, pltpu.HBM)
            for a in (spectrum.reshape(band * rows, width), *smalls)
        ]
    )
    out, ocean = pl.pallas_call(
        functools.partial(write_kernel, sizes),
        out_shape=(
            jax.ShapeDtypeStruct((band * rows, width), F32),
            jax.ShapeDtypeStruct((2, share), F32),
        ),
        in_specs=[vmem] * len(between),
        out_specs=(hbm, hbm),
        scratch_shapes=[
            VMEM((band * rows, width), F32), VMEM((2, share), F32), dma((nf // 2 + 1,)),
        ],
        compiler_params=pltpu.CompilerParams(vmem_limit_bytes=16 << 20),
    )(*made)
    return out.reshape(spectrum.shape), ocean.T


def solution(mesh):
    axes = tuple(mesh.shape[a] for a in ("lat", "lon", "freq"))
    return jax.shard_map(
        functools.partial(local, axes),
        mesh=mesh,
        in_specs=(
            P("freq", None, "lat", "lon"),
            P("freq"),
            P("lat", "lon"),
            P("lat", "lon"),
            P("lat", "lon"),
            P(),
            P(),
            P(),
            P(),
            P("lat", "lon"),
        ),
        out_specs=(P("freq", None, "lat", "lon"), P(("lon", "freq"), None)),
        check_vma=False,
    )
```

```python
import functools

import jax
import jax.numpy as jnp
import numpy as np
from jax import lax
from jax.experimental import pallas as pl
from jax.experimental.pallas import tpu as pltpu
from jax.sharding import PartitionSpec as P

time_step = 0.5
MESH = pl.DeviceIdType.MESH
VMEM = pltpu.VMEM
LANES = 128
EDGE = 4
F32, BF16 = jnp.float32, jnp.bfloat16


def spread(nf):
    order = list(range(EDGE)) + list(range(nf - EDGE, nf)) + list(range(EDGE, nf - EDGE))
    return {f: i for i, f in enumerate(order)}


def round_up(n, m):
    return -(-n // m) * m


def split(v):
    high = v.astype(BF16)
    return high, (v - high.astype(F32)).astype(BF16)


def thirds(v):
    high, low = split(v)
    rest = v - high.astype(F32) - low.astype(F32)
    return high, low, rest.astype(BF16)


def layout(rows):
    inner, rim_rows = list(range(1, rows - 1)), [0, rows - 1]
    slot = {r: i for i, r in enumerate(inner + rim_rows)}

    def columns(r):
        return slice(slot[r] * LANES, slot[r] * LANES + LANES)

    whole = slice(0, rows * LANES)
    split_at = len(inner) * LANES
    return inner, rim_rows, columns, (whole, slice(0, split_at), slice(split_at, rows * LANES))


def finish_chunk(c, first, cs, shape, refs, result, growth, stay):
    nd, rows = shape
    put, th, tl, shapes, mf = refs
    pair = 2 * nd
    pitch = round_up(pair, 16)
    window = 3 * pitch
    columns = layout(rows)[2]
    at = pl.multiple_of(c * pitch, 16)
    lhs = put[pl.ds(at, pitch), :window]
    back = jnp.dot(lhs, th[pl.ds(at, window), cs], preferred_element_type=F32)
    back = back + jnp.dot(lhs, tl[pl.ds(at, window), cs], preferred_element_type=F32)
    profile = shapes[pl.ds(at, pair), :]
    to = (c - first) * (pair * rows)
    for r in range(rows):
        here = columns(r)
        if here.start < cs.start or here.stop > cs.stop:
            continue
        e = mf[pl.ds(at, pair), here]
        gain = back[:pair, here.start - cs.start : here.stop - cs.start]
        result[pl.ds(to + r, pair, stride=rows), :] = e * (stay(r) + profile * growth(r)) + gain


def wave_kernel(sizes, angles, spectrum, *refs):
    sources, refs = refs[:10], refs[10:]
    result, mf, th, tl, put, shapes, factors, stress, spread_out, *refs = refs
    inputs, refs = refs[:10], refs[10:]
    speed, waves, profile, coef, momentum, quad, mask, wind, dissip, cells = inputs
    (
        x, mh, ml, pick, table, rates, cols, lines, coefs, weight0, weight1, rim_weights,
        gains, gains_far, speed_far, pack_up, pack_down, got_up, got_down, edge, edge_far,
        lon_pack, got_left, got_right, lon_far, far_left, far_right, cols_far, energy, energy_got, tau_own, taus,
        load_sem, small_sem, lat_ready, diag_ready, lon_ready, raw_send, raw_recv, lat_send, lat_recv, lon_send, lon_recv,
        sum_send, sum_recv, tau_send, tau_recv,
    ) = refs
    n_lat, n_lon, n_freq, nf, nd, rows, nbins = sizes
    half = nd // 2
    pair = 2 * nd
    band = nf * nd
    all_rows = n_lat * rows
    pitch = round_up(pair, 16)
    pad = pitch - pair
    own_chunks = nf // 2
    far_chunks = EDGE // 2
    chunks = own_chunks + far_chunks
    window = 3 * pitch
    reach = round_up(window, LANES)
    span = lines.shape[1]
    places = spread(nf)
    groups = pair // 8
    cosines, sines = angles
    li, lo, fi = lax.axis_index("lat"), lax.axis_index("lon"), lax.axis_index("freq")
    other = 1 - fi
    first = far_chunks * fi
    far_first = own_chunks * other

    own_rows = pl.multiple_of(first * (pair * rows), 8)
    small = [
        pltpu.make_async_copy(a, b, small_sem.at[i])
        for i, (a, b) in enumerate(zip(sources, inputs))
    ]
    step = 3 if own_chunks % 3 == 0 else 1
    loads = []
    for i in range(own_chunks // step):
        count = step * pair * rows
        loads.append(
            pltpu.make_async_copy(
                spectrum.at[pl.ds(i * count, count)], x.at[pl.ds(own_rows + i * count, count)],
                load_sem.at[i],
            )
        )
    for copy in loads + small:
        copy.start()

    east, west = lax.rem(lo + 1, n_lon), lax.rem(lo + n_lon - 1, n_lon)
    group = []
    for s in range(1, n_lat * n_freq):
        dl, df = divmod(s, n_freq)
        group.append({"lat": lax.rem(li + dl, n_lat), "freq": lax.rem(fi + df, n_freq)})
    barrier = pltpu.get_barrier_semaphore()
    last = n_lon - 1
    higher = [li + dl < n_lat for dl in range(1, n_lat)]
    lat_peer = [
        [{"lat": lax.rem(li + dl, n_lat), "freq": f} for f in range(n_freq)] for dl in range(1, n_lat)
    ]
    beside = {
        side: [{"lon": side_at, "freq": f} for f in range(n_freq)]
        for side, side_at in (("east", east), ("west", west))
    }

    def signal(semaphore, peers):
        for peer in peers:
            pl.semaphore_signal(semaphore, inc=1, device_id=peer, device_id_type=MESH)

    def signal_if(condition, semaphore, peers):
        @pl.when(condition)
        def _():
            signal(semaphore, peers)

    signal(barrier, [{"freq": other}])
    for up, (in_first, in_second) in zip(higher, lat_peer):
        signal_if(jnp.logical_or(fi == 0, up), barrier, [in_first])
        signal_if(up, barrier, [in_second])
    signal_if(lo < last, barrier, beside["east"])
    signal_if(lo == 0, barrier, beside["west"])
    at_start, at_end = lax.div(last - lo, last), lax.div(lo, last)
    greeted = 1 + other * (n_lat - 1 + li) + fi * (2 * li) + 2 * (1 - at_start) + 2 * at_end
    answers_lat = n_lat - 1 - li
    answers_lon = 2 * (1 - at_end) + 2 * at_start

    def enter():
        pl.semaphore_wait(barrier, greeted)
        speed_copy().start()
        raw_copy(True).start()
        for up, (in_first, in_second) in zip(higher, lat_peer):
            signal_if(jnp.logical_and(fi == 1, jnp.logical_not(up)), lat_ready, [in_second])
            signal_if(jnp.logical_and(fi == 1, jnp.logical_not(up)), diag_ready, [in_first])
            signal_if(jnp.logical_and(fi == 0, jnp.logical_not(up)), diag_ready, [in_second])
        signal_if(lo > 0, lon_ready, beside["west"])
        signal_if(lo == last, lon_ready, beside["east"])

    packed = pack_up.shape[0]
    far_lat = EDGE * half
    up_ok, down_ok = li < n_lat - 1, li > 0

    def raw_copy(near):
        count = EDGE // 2 * nd * rows
        half_at = (other if near else fi) * count
        src = pl.multiple_of(other * ((nf - EDGE) * nd * rows) + half_at, 8)
        dst = pl.multiple_of(fi * (band * rows) + half_at, 8)
        i = 2 if near else 0
        return pltpu.make_async_remote_copy(
            spectrum.at[pl.ds(src, count)], x.at[pl.ds(dst, count)],
            raw_send.at[i], raw_recv.at[i], device_id={"freq": other}, device_id_type=MESH,
        )

    def speed_copy():
        return pltpu.make_async_remote_copy(
            sources[0], speed_far, raw_send.at[1], raw_recv.at[1],
            device_id={"freq": other}, device_id_type=MESH,
        )

    def lat_copy(up):
        src, dst = (pack_up, got_up) if up else (pack_down, got_down)
        i = int(up)
        return pltpu.make_async_remote_copy(
            src, dst.at[pl.ds(far_lat, packed)], lat_send.at[i], lat_recv.at[i],
            device_id={"lat": li + 1 if up else li - 1}, device_id_type=MESH,
        )

    def lat_far_copy(up):
        src, dst = (pack_up, got_up) if up else (pack_down, got_down)
        i = 2 + int(up)
        return pltpu.make_async_remote_copy(
            src.at[pl.ds(pl.multiple_of(other * far_lat, 8), far_lat)], dst.at[pl.ds(0, far_lat)],
            lat_send.at[i], lat_recv.at[i],
            device_id={"lat": li + 1 if up else li - 1, "freq": other}, device_id_type=MESH,
        )

    def lon_copy(to_east):
        i = int(to_east)
        return pltpu.make_async_remote_copy(
            lon_pack, got_left if to_east else got_right, lon_send.at[i], lon_recv.at[i],
            device_id={"lon": east if to_east else west}, device_id_type=MESH,
        )

    def lon_far_copy(to_east):
        i = 2 + int(to_east)
        return pltpu.make_async_remote_copy(
            lon_far, far_left if to_east else far_right, lon_send.at[i], lon_recv.at[i],
            device_id={"lon": east if to_east else west, "freq": other}, device_id_type=MESH,
        )

    def energy_copy():
        return pltpu.make_async_remote_copy(
            energy, energy_got, sum_send.at[0], sum_recv.at[0],
            device_id={"freq": other}, device_id_type=MESH,
        )

    def tau_copy(s):
        return pltpu.make_async_remote_copy(
            tau_own, taus.at[s], tau_send.at[s], tau_recv.at[s],
            device_id=group[s], device_id_type=MESH,
        )

    def signs(values, j):
        return [bool(values[(8 * j + i) % nd] > 0.0) for i in range(8)]

    eight = lax.broadcasted_iota(jnp.int32, (8, LANES), 0)
    lane = lax.broadcasted_iota(jnp.int32, (8, LANES), 1)

    def rows_of(flags):
        spot = None
        for i, flag in enumerate(flags):
            if flag:
                here = eight == i
                spot = here if spot is None else jnp.logical_or(spot, here)
        return spot

    def choose(flags, yes, no):
        if all(flags):
            return yes()
        if not any(flags):
            return no()
        return jnp.where(rows_of(flags), yes(), no())

    forward = [signs(cosines, j) for j in range(groups)]
    southern = [[(8 * j + i) % nd < half for i in range(8)] for j in range(groups)]

    @pl.when(fi == 1)
    def _():
        enter()

    pack_up[pl.ds(packed - 8, 8), :] = jnp.zeros((8, LANES), F32)
    pack_down[pl.ds(packed - 8, 8), :] = jnp.zeros((8, LANES), F32)
    sums = [jnp.zeros((8, LANES), F32) for _ in range(groups)]
    for i, copy in enumerate(loads):
        if i == len(loads) - 1:

            @pl.when(fi == 0)
            def _():
                enter()

        copy.wait()
        for f in range(2 * step * i, 2 * step * (i + 1)):
            at = half * places[f]
            base = own_rows + nd * f * rows
            pack_up[pl.ds(at, half), :] = x[pl.ds(base + rows - 1, half, stride=rows), :]
            pack_down[pl.ds(at, half), :] = x[pl.ds(base + half * rows, half, stride=rows), :]
        for u in range(step):
            c = i * step + u + first
            base = pl.multiple_of(c * (pair * rows), 8)
            for r in range(rows):
                k = c * rows + r
                for j in range(groups):
                    e = x[pl.ds(base + 8 * rows * j + r, 8, stride=rows), :]
                    z = choose(
                        forward[j],
                        lambda: jnp.where(lane == LANES - 1, e, 0.0),
                        lambda: jnp.where(lane == 0, e, 0.0),
                    )
                    sums[j] = sums[j] + pltpu.roll(z, k, 1)

    for j in range(groups):
        aligned = choose(forward[j], lambda: pltpu.roll(sums[j], 1, 1), lambda: sums[j])
        lon_pack[8 * j : 8 * j + 8, :] = aligned

    begin = (first + (own_chunks - far_chunks) * other) * rows
    whole = jnp.concatenate(
        [lon_pack[...], jnp.zeros((LANES - pair, LANES), F32)], axis=0
    )
    turned = pltpu.roll(whole, lax.rem(LANES - begin, LANES), 1).T
    lon_far[...] = turned[0:8, :]

    def send_columns(answered):
        if answered:
            pl.semaphore_wait(lon_ready, answers_lon)
        for to_east in (True, False):
            lon_copy(to_east).start()
            lon_far_copy(to_east).start()

    @pl.when(lo == last)
    def _():
        send_columns(False)

    @pl.when(jnp.logical_and(fi == 1, up_ok))
    def _():
        pl.semaphore_wait(lat_ready, answers_lat)

    @pl.when(up_ok)
    def _():
        lat_copy(True).start()

    @pl.when(down_ok)
    def _():
        lat_copy(False).start()

    @pl.when(up_ok)
    def _():
        pl.semaphore_wait(diag_ready, answers_lat)
        lat_far_copy(True).start()

    @pl.when(down_ok)
    def _():
        lat_far_copy(False).start()

    raw_copy(False).start()

    for copy in small:
        copy.wait()
    rates[...] = jnp.zeros_like(rates)
    rates[0:1, 0:nf] = speed[...].reshape(1, nf)
    own_rates = rates[...]
    gains[...] = jnp.broadcast_to(
        pltpu.roll(rates[...], EDGE * fi, 1).T[0 : gains.shape[0], 0:1], gains.shape
    )
    bin0 = fi * ((nf - EDGE) * nd)
    lines[...] = jnp.zeros_like(lines)
    target = (quad[...] - bin0).astype(F32)
    shift = jnp.zeros_like(target)
    for i in range(1, chunks):
        shift = shift + jnp.where(target >= float(pair * i), float(pad), 0.0)
    lines[0:2, 0:nbins] = target + shift
    lines[2:3, 0:nbins] = time_step * coef[...].reshape(1, nbins)
    weight = profile[...].reshape(1, nbins)
    lines[3:4, 0:nbins] = weight
    lines[4:6, 0:nbins] = momentum[...] * weight
    lines[...] = pltpu.roll(lines[...], lax.rem(span - bin0, span), 1)
    cols[...] = jnp.full_like(cols, -1.0)
    for k in range(-(-chunks * pair // LANES)):
        block = lines[:, LANES * k : LANES * k + LANES].T
        at = LANES * k
        while at < min(LANES * (k + 1), chunks * pair):
            c = at // pair
            stop = min(pair * (c + 1), LANES * (k + 1))
            cols[at + pad * c : stop + pad * c, :] = block[at - LANES * k : stop - LANES * k]
            at = stop
    for k in range(span // LANES):
        lines[:, LANES * k : LANES * k + LANES] = cols[LANES * k : LANES * k + LANES, :].T
    turned = waves[...].T
    table[pl.ds(0, pair), :] = jnp.broadcast_to(turned[0:pair, 0:1], (pair, LANES))
    table[pl.ds(pair, pair), :] = jnp.broadcast_to(turned[0:pair, 1:2], (pair, LANES))

    @pl.when(jnp.logical_and(lo > 0, lo < last))
    def _():
        send_columns(True)

    @pl.when(jnp.logical_not(down_ok))
    def _():
        got_up[...] = jnp.zeros_like(got_up)

    @pl.when(jnp.logical_not(up_ok))
    def _():
        got_down[...] = jnp.zeros_like(got_down)

    for ref in (mh, ml, th, tl):
        for at in (0, (chunks + 1) * pitch):
            ref[pl.ds(at, pitch), :] = jnp.zeros((pitch, ref.shape[1]), BF16)
    lanes = lax.broadcasted_iota(jnp.int32, (pitch, reach), 1)
    below = lax.broadcasted_iota(jnp.int32, (pitch, reach), 0)
    own_bin = lanes == below + pitch

    def build(c, carry):
        at = pl.multiple_of(pitch * c, 8)
        where = (lanes + (at - pitch)).astype(F32)
        for i in range(2):
            chosen = jnp.where(cols[pl.ds(at, pitch), i : i + 1] == where, 1.0, 0.0)
            pick[pl.ds(pl.multiple_of(2 * at + pitch * i, 16), pitch), :] = chosen.astype(BF16)
        row = (below + at).astype(F32)
        line = pltpu.roll(lines[...], lax.rem(span + pitch - at, span), 1)
        given = jnp.where(own_bin, -2.0, 0.0)
        for i in range(2):
            given = given + jnp.where(line[i : i + 1, :reach] == row, 1.0, 0.0)
        put[pl.ds(pl.multiple_of(at, 16), pitch), :] = given.astype(BF16)
        for i, ref in enumerate((coefs, shapes, weight0, weight1)):
            ref[pl.ds(at, pitch), :] = jnp.broadcast_to(
                cols[pl.ds(at, pitch), 2 + i : 3 + i], (pitch, LANES)
            )
        mf[pl.ds(at + pair, pad), :] = jnp.zeros((pad, mf.shape[1]), F32)
        return carry

    lax.fori_loop(0, chunks, build, 0)
    share = (LANES // n_freq) * all_rows
    cell = lax.broadcasted_iota(jnp.int32, (LANES, share), 1)
    first_cell = (lax.broadcasted_iota(jnp.int32, (LANES, share), 0) - fi * (LANES // n_freq)) * all_rows
    inside = jnp.logical_and(cell >= first_cell, cell < first_cell + all_rows)
    spread_out[...] = jnp.where(inside, 1.0, 0.0).astype(BF16)

    @pl.when(lo == 0)
    def _():
        send_columns(True)

    sea = mask[...].astype(F32)

    inner, rim_rows, columns, (whole_cols, inner_cols, rim_cols) = layout(rows)

    def upwind(e, j):
        if all(forward[j]):
            return pltpu.roll(e, 1, 1)
        if not any(forward[j]):
            return pltpu.roll(e, LANES - 1, 1)
        at = lane + jnp.where(rows_of(forward[j]), LANES - 1, 1)
        return jnp.take_along_axis(e, at & (LANES - 1), axis=1)

    def rates_of(j, gain):
        low, high = 8 * j < nd, 8 * j + 8 > nd
        if low and high:
            g = jnp.where(eight < nd - 8 * j, gain[0], gain[1])
        else:
            g = jnp.broadcast_to(gain[0] if low else gain[1], (8, LANES))
        return g * table[8 * j : 8 * j + 8, :], g * table[pair + 8 * j : pair + 8 * j + 8, :]

    def rim_lane(j):
        return lane == choose(forward[j], lambda: 0, lambda: LANES - 1)

    def prepare(c, gain, sums):
        base = pl.multiple_of(c * (pair * rows), 8)
        at = pl.multiple_of(c * pitch, 16)
        zero = jnp.zeros((8, LANES), F32)
        for j in range(groups):
            ax, ay = rates_of(j, gain)
            stay = 1.0 - ax - ay
            weights = weight0[pl.ds(at + 8 * j, 8), :], weight1[pl.ds(at + 8 * j, 8), :]
            e = [x[pl.ds(base + 8 * rows * j + r, 8, stride=rows), :] for r in range(rows)]
            for r in range(rows):
                nx = jnp.where(rim_lane(j), 0.0, upwind(e[r], j))
                ny = choose(
                    southern[j],
                    lambda: e[r - 1] if r > 0 else zero,
                    lambda: e[r + 1] if r < rows - 1 else zero,
                )
                m = stay * e[r] + ax * nx + ay * ny
                mf[pl.ds(at + 8 * j, 8), columns(r)] = m
                for i, v in enumerate((m, m * weights[0], m * weights[1])):
                    sums[r, i] = sums[r, i] + v

    def complete(c, gain, row_set, keep, outer=None, halo=None):
        at = pl.multiple_of(c * pitch, 16)
        store = pl.multiple_of(c * pitch + pitch, 16)
        held = {}
        for j in range(groups):
            ax, ay = rates_of(j, gain)
            for r in row_set:
                m = mf[pl.ds(at + 8 * j, 8), columns(r)]
                if halo:
                    m = m + ax * jnp.where(rim_lane(j), halo(r, j), 0.0)
                if not keep:
                    mf[pl.ds(at + 8 * j, 8), columns(r)] = m
                    continue
                from_edge = [
                    (r == 0 and south) or (r == rows - 1 and not south) for south in southern[j]
                ]
                if any(from_edge):
                    zero = jnp.zeros((8, LANES), F32)
                    m = m + ay * choose(from_edge, lambda: outer(j), lambda: zero)
                m = m * sea[r : r + 1, :]
                mf[pl.ds(at + 8 * j, 8), columns(r)] = m
                held[j, r] = m
                if j % 2 == 1 or j == groups - 1:
                    start = j if j % 2 == 0 else j - 1
                    both = [held[start, r], held[j, r] if j > start else jnp.zeros_like(m)]
                    hi, lw = split(jnp.concatenate(both, axis=0))
                    mh[pl.ds(store + 8 * start, 16), columns(r)] = hi
                    ml[pl.ds(store + 8 * start, 16), columns(r)] = lw

    def propagate(c, outer, gain, halo, row_set, sums):
        base = pl.multiple_of(c * (pair * rows), 8)
        at = pl.multiple_of(c * pitch, 16)
        store = pl.multiple_of(c * pitch + pitch, 16)
        sums = dict(sums)
        held = {}
        for j in range(groups):
            low, high = 8 * j < nd, 8 * j + 8 > nd
            if low and high:
                g = jnp.where(eight < nd - 8 * j, gain[0], gain[1])
            else:
                g = jnp.broadcast_to(gain[0] if low else gain[1], (8, LANES))
            ax = g * table[8 * j : 8 * j + 8, :]
            ay = g * table[pair + 8 * j : pair + 8 * j + 8, :]
            stay = 1.0 - ax - ay
            e = [x[pl.ds(base + 8 * rows * j + r, 8, stride=rows), :] for r in range(rows)]
            if sums:
                w0, w1 = weight0[pl.ds(at + 8 * j, 8), :], weight1[pl.ds(at + 8 * j, 8), :]
            for r in row_set:
                rim = lane == choose(forward[j], lambda: 0, lambda: LANES - 1)
                nx = jnp.where(rim, halo(r, j), upwind(e[r], j))
                ny = choose(
                    southern[j],
                    lambda: e[r - 1] if r > 0 else outer(j),
                    lambda: e[r + 1] if r < rows - 1 else outer(j),
                )
                m = (stay * e[r] + ax * nx + ay * ny) * sea[r : r + 1, :]
                mf[pl.ds(at + 8 * j, 8), columns(r)] = m
                held[j, r] = m
                if sums:
                    for i, v in enumerate((m, m * w0, m * w1)):
                        sums[r, i] = sums[r, i] + v
                if j % 2 == 1 or j == groups - 1:
                    start = j if j % 2 == 0 else j - 1
                    both = [held[start, r], held[j, r] if j > start else jnp.zeros_like(m)]
                    hi, lw = split(jnp.concatenate(both, axis=0))
                    mh[pl.ds(store + 8 * start, 16), columns(r)] = hi
                    ml[pl.ds(store + 8 * start, 16), columns(r)] = lw
        return sums

    def interact(c, cs):
        width = (cs.stop - cs.start) // LANES
        at = pl.multiple_of(c * pitch, 16)
        lhs = pick[pl.ds(pl.multiple_of(2 * at, 16), 2 * pitch), :window]
        both = jnp.dot(lhs, mh[pl.ds(at, window), cs], preferred_element_type=F32)
        both = both + jnp.dot(lhs, ml[pl.ds(at, window), cs], preferred_element_type=F32)
        third, fourth = both[:pitch], both[pitch:]
        e = mf[pl.ds(at, pitch), cs]
        scale = jnp.concatenate([coefs[pl.ds(at, pitch), :]] * width, axis=1)
        product = third * fourth
        moved = (scale * e) * (e * (third + fourth) - (product + product))
        hi, lw = split(moved)
        to = pl.multiple_of(at + pitch, 16)
        th[pl.ds(to, pitch), cs] = hi
        tl[pl.ds(to, pitch), cs] = lw

    def finish(c, cs):
        finish_chunk(
            c, first, cs, (nd, rows), (put, th, tl, shapes, mf), result,
            lambda r: time_step * wind[r : r + 1, :], lambda r: 1.0,
        )

    def run(what, begin, count, cs, at_once):
        def body(t, carry):
            for u in range(at_once):
                what(begin + t * at_once + u, cs)
            return carry

        lax.fori_loop(0, count // at_once, body, 0)
        for u in range(count - count % at_once, count):
            what(begin + u, cs)

    def receive(ref, first_row, where):
        for i in range(len(where)):
            at = first_row + half * where[i]
            ref[pl.ds(nd * i, half), :] = got_up[pl.ds(at, half), :]
            ref[pl.ds(nd * i + half, half), :] = got_down[pl.ds(at, half), :]

    names = [(r, i) for r in range(rows) for i in range(3)]

    def prepare_own(t, sums):
        sums = dict(zip(names, sums))
        for u in range(step):
            c = first + t * step + u
            prepare(c, [gains[pl.ds(2 * c + i, 1), :] for i in range(2)], sums)
        return tuple(sums[n] for n in names)

    place = lane >> 2 if rows == 4 else lax.div(lane, rows)
    held_rates = pltpu.roll(own_rates, EDGE * fi, 1)
    rate = [
        jnp.take_along_axis(held_rates, jnp.minimum(2 * place + i, LANES - 1), axis=1)[0:1]
        for i in range(2)
    ]
    for j in range(groups):
        here = slice(8 * j, 8 * j + 8)
        ax, _ = rates_of(j, rate)
        heavy = [jnp.zeros((8, LANES), F32) for _ in range(2)]
        for u in range(own_chunks):
            at = pl.multiple_of((first + u) * pitch, 8) + 8 * j
            for i, ref in enumerate((weight0, weight1)):
                heavy[i] = jnp.where(place == first + u, ref[pl.ds(at, 8), :], heavy[i])
        rim_weights[0, here, :] = ax
        rim_weights[1, here, :] = ax * heavy[0]
        rim_weights[2, here, :] = ax * heavy[1]
    zeros = tuple(jnp.zeros((8, LANES), F32) for _ in names)
    sums = dict(zip(names, lax.fori_loop(0, own_chunks // step, prepare_own, zeros)))
    speed_copy().wait_recv()
    rates[0:1, 0:nf] = speed_far[...].reshape(1, nf)
    gains_far[...] = jnp.broadcast_to(
        pltpu.roll(rates[...], fi * (LANES - (nf - EDGE)), 1).T[0:8, 0:1], gains_far.shape
    )

    lon_copy(True).wait_recv()
    lon_copy(False).wait_recv()
    ends = []
    for side, source in ((True, got_left), (False, got_right)):
        for i in range(3):
            total = jnp.zeros((8, LANES), F32)
            for j in range(groups):
                flags = [flag == side for flag in forward[j]]
                if any(flags):
                    here = slice(8 * j, 8 * j + 8)
                    term = rim_weights[i, here, :] * source[here, :]
                    total = total + choose(flags, lambda: term, lambda: jnp.zeros_like(term))
            ends.append(jnp.sum(total, axis=0, keepdims=True))
    ends = jnp.concatenate(ends + [jnp.zeros((2, LANES), F32)], axis=0)
    lanes_left = LANES
    while lanes_left > rows:
        lanes_left //= 2
        ends = ends + pltpu.roll(ends, lanes_left, 1)
    for j in range(groups):
        here = slice(8 * j, 8 * j + 8)
        got_left[here, :] = choose(
            forward[j],
            lambda: got_left[here, :],
            lambda: pltpu.roll(got_right[here, :], LANES - 1, 1),
        )

    def own(row_set, columns_too, rows_too):
        at_once = step if columns_too else own_chunks

        def body(t, carry):
            for u in range(at_once):
                c = first + t * at_once + u

                def halo(r, j):
                    return pltpu.roll(got_left[8 * j : 8 * j + 8, :], LANES - (c * rows + r), 1)

                def outer(j):
                    return edge[pl.ds(pl.multiple_of((c - first) * pair, 8) + 8 * j, 8), :]

                gain = [gains[pl.ds(2 * c + i, 1), :] for i in range(2)]
                complete(c, gain, row_set, rows_too, outer, halo if columns_too else None)
            return carry

        lax.fori_loop(0, own_chunks // at_once, body, 0)

    def edge_sums(t, sums):
        sums = list(sums)
        for u in range(step):
            c = first + t * step + u
            at = pl.multiple_of(c * pitch, 16)
            gain = [gains[pl.ds(2 * c + i, 1), :] for i in range(2)]
            for j in range(groups):
                _, ay = rates_of(j, gain)
                term = ay * edge[pl.ds(pl.multiple_of((c - first) * pair, 8) + 8 * j, 8), :]
                terms = (
                    term,
                    term * weight0[pl.ds(at + 8 * j, 8), :],
                    term * weight1[pl.ds(at + 8 * j, 8), :],
                )
                for side in range(2):
                    flags = [flag == (side == 0) for flag in southern[j]]
                    if any(flags):
                        for i, v in enumerate(terms):
                            sums[3 * side + i] = sums[3 * side + i] + choose(
                                flags, lambda: v, lambda: jnp.zeros_like(v)
                            )
        return tuple(sums)

    near_first = 2 * first - fi
    near_count = chunks - far_chunks - 1
    last_first = 2 * first
    last_count = chunks - 2 * far_chunks
    own(inner, True, True)

    @pl.when(jnp.logical_not(down_ok))
    def _():
        own(rim_rows, True, False)

    @pl.when(down_ok)
    def _():
        lat_copy(True).wait_recv()

    @pl.when(up_ok)
    def _():
        lat_copy(False).wait_recv()

    receive(edge, far_lat, [places[f] for f in range(nf)])

    zeros = tuple(jnp.zeros((8, LANES), F32) for _ in range(6))
    from_rows = lax.fori_loop(0, own_chunks // step, edge_sums, zeros)

    def whole_sum(r, i):
        total = sums[r, i]
        if r == 0:
            total = total + from_rows[i]
        if r == rows - 1:
            total = total + from_rows[3 + i]
        total = jnp.sum(total, axis=0, keepdims=True)
        start = pltpu.roll(ends, (LANES - r) % LANES, 1)[i : i + 1]
        stop = pltpu.roll(ends, LANES - 1 - r, 1)[3 + i : 4 + i]
        total = total + jnp.where(lane[0:1] == 0, start, 0.0)
        total = total + jnp.where(lane[0:1] == LANES - 1, stop, 0.0)
        return total * sea[r : r + 1, :]

    energy[...] = jnp.zeros((8, LANES), F32)
    ids = (lo * LANES + lax.broadcasted_iota(jnp.int32, (all_rows, LANES), 1)) * all_rows
    ids = ids + lax.broadcasted_iota(jnp.int32, (all_rows, LANES), 0)
    totals = [jnp.zeros((all_rows, LANES), F32) for _ in range(2)]
    for r in range(rows):
        energy[r : r + 1, :] = whole_sum(r, 0)
        hit = cells[r : r + 1, :] == ids
        for i in range(2):
            tau = wind[r : r + 1, :] * whole_sum(r, 1 + i)
            totals[i] = totals[i] + jnp.where(hit, tau, 0.0)
    for i in range(2):
        tau_own[pl.ds(i * all_rows, all_rows), :] = totals[i]
    tau_copy(len(group) - 1).start()
    energy_copy().start()
    for s in range(len(group) - 1):
        tau_copy(s).start()


    @pl.when(down_ok)
    def _():
        own(rim_rows, True, False)

    own(rim_rows, False, True)
    run(interact, near_first, near_count, whole_cols, 8)
    run(finish, last_first, last_count, whole_cols, 7)

    @pl.when(down_ok)
    def _():
        lat_far_copy(True).wait_recv()

    @pl.when(up_ok)
    def _():
        lat_far_copy(False).wait_recv()

    receive(edge_far, 0, list(range(EDGE)))
    lon_far_copy(True).wait_recv()
    lon_far_copy(False).wait_recv()
    left, right = far_left[...].T, far_right[...].T
    for j in range(groups):
        here = slice(8 * j, 8 * j + 8)
        ahead = eight[:, 0:8] < 0
        for i, flag in enumerate(forward[j]):
            if flag:
                ahead = jnp.logical_or(ahead, eight[:, 0:8] == i)
        cols_far[here, :] = jnp.where(ahead, left[here], right[here])
    raw_copy(True).wait_recv()
    raw_copy(False).wait_recv()

    for u in range(far_chunks):
        def halo(r, j):
            k = u * rows + r
            return jnp.broadcast_to(cols_far[8 * j : 8 * j + 8, k : k + 1], (8, LANES))

        def outer(j):
            return edge_far[pair * u + 8 * j : pair * u + 8 * j + 8, :]

        gain = [gains_far[2 * u + i : 2 * u + i + 1, :] for i in range(2)]
        propagate(far_first + u, outer, gain, halo, range(rows), {})

    late = (chunks - far_chunks - 1) * other + fi
    run(interact, late, 2, whole_cols, 2)
    energy_copy().wait()
    factors[0:rows, :] = time_step * dissip[...] * ((energy[0:rows, :] + energy_got[0:rows, :]) / nbins)
    factors[rows : 2 * rows, :] = time_step * wind[...]

    raw_copy(True).wait_send()
    raw_copy(False).wait_send()
    speed_copy().wait_send()
    for flag in (True, False):
        lon_copy(flag).wait_send()
        lon_far_copy(flag).wait_send()

    @pl.when(up_ok)
    def _():
        lat_copy(True).wait_send()
        lat_far_copy(True).wait_send()

    @pl.when(down_ok)
    def _():
        lat_copy(False).wait_send()
        lat_far_copy(False).wait_send()

    st = tau_own[...]
    for s in range(len(group)):
        tau_copy(s).wait()
        st = st + taus[s]
    stress[...] = st


def write_kernel(
    sizes, before, mf, th, tl, put, shapes, factors, taus, spread_out, result_out, stress_out,
    result, stress, sems,
):
    n_lat, n_lon, n_freq, nf, nd, rows, nbins = sizes
    pair = 2 * nd
    pitch = round_up(pair, 16)
    own_chunks, far_chunks = nf // 2, EDGE // 2
    columns, (whole_cols, _, _) = layout(rows)[2:]
    fi = lax.axis_index("freq")
    first = far_chunks * fi
    size = pair * rows

    def out(i):
        here = pl.ds(pl.multiple_of(lax.rem(i + first, own_chunks) * size, 8), size)
        return pltpu.make_async_copy(result.at[here], result_out.at[here], sems.at[i])

    def settle(i, carry):
        t = lax.rem(i + first, own_chunks)
        at = pl.multiple_of((t + first) * pitch, 8)
        for r in range(rows):
            spot = pl.ds(t * size + r, pair, stride=rows)
            e = mf[pl.ds(at, pair), columns(r)]
            result[spot, :] = before[spot, :] - e * factors[r : r + 1, :]
        out(i).start()
        return carry

    settled = own_chunks - far_chunks
    lax.fori_loop(0, settled, settle, 0)
    for i in range(settled, own_chunks):
        finish_chunk(
            lax.rem(i + first, own_chunks) + first, first, whole_cols, (nd, rows),
            (put, th, tl, shapes, mf), result,
            lambda r: factors[rows + r : rows + r + 1, :], lambda r: 1.0 - factors[r : r + 1, :],
        )
    for i in range(settled, own_chunks):
        out(i).start()

    all_rows = n_lat * rows
    share = (LANES // n_freq) * all_rows
    st = taus[...]
    wide = sum(
        jnp.dot(term, spread_out[...], preferred_element_type=F32) for term in thirds(st)
    )
    place = lax.broadcasted_iota(jnp.int32, (all_rows, share), 1) & (all_rows - 1)
    own_row = place == lax.broadcasted_iota(jnp.int32, (all_rows, share), 0)
    for i in range(2):
        picked = jnp.where(own_row, wide[i * all_rows : (i + 1) * all_rows], 0.0)
        stress[i : i + 1, :] = jnp.sum(picked, axis=0, keepdims=True)
    last = pltpu.make_async_copy(stress, stress_out, sems.at[own_chunks])
    last.start()

    def wait(i, carry):
        out(i).wait()
        return carry

    lax.fori_loop(0, own_chunks, wait, 0)
    last.wait()


def local(
    axes,
    spectrum,
    group_speed,
    sea_mask,
    wind_growth,
    dissipation,
    wind_profile,
    nonlinear_coef,
    momentum,
    quadruplet,
    ocean_cell,
):
    n_lat, n_lon, n_freq = axes
    nf, nd, rows, width = spectrum.shape
    nbins = wind_profile.shape[0]
    assert n_freq == 2 and nf % 2 == 0 and width == LANES
    band, pair, half = nf * nd, 2 * nd, nd // 2
    pitch = round_up(pair, 16)
    chunks = nf // 2 + EDGE // 2
    all_rows = n_lat * rows
    angles = (np.float32(2.0 * np.pi) * np.arange(nd, dtype=np.float32) / np.float32(nd)).astype(
        np.float32
    )
    cosines, sines = np.cos(angles), np.sin(angles)
    waves = np.zeros((8, LANES), np.float32)
    waves[0, :pair], waves[1, :pair] = np.tile(np.abs(cosines), 2), np.tile(np.abs(sines), 2)

    packed = round_up(nf * half, 8)
    far_lat = EDGE * half
    share = (width // n_freq) * all_rows
    span = round_up(max(nbins, (chunks + 2) * pitch), LANES)
    reach = round_up(3 * pitch, LANES)
    vmem = pl.BlockSpec(memory_space=VMEM)
    hbm = pl.BlockSpec(memory_space=pltpu.HBM)
    sizes = (n_lat, n_lon, n_freq, nf, nd, rows, nbins)
    dma = pltpu.SemaphoreType.DMA
    smalls = (
        group_speed,
        jnp.asarray(waves),
        wind_profile,
        nonlinear_coef,
        momentum,
        quadruplet,
        sea_mask,
        wind_growth,
        dissipation,
        ocean_cell,
    )
    between = [
        jax.ShapeDtypeStruct(shape, dtype)
        for shape, dtype in (
            ((band * rows, width), F32),
            ((chunks * pitch, rows * width), F32),
            (((chunks + 2) * pitch, rows * width), BF16),
            (((chunks + 2) * pitch, rows * width), BF16),
            ((chunks * pitch, reach), BF16),
            ((chunks * pitch, width), F32),
            ((2 * rows, width), F32),
            ((2 * all_rows, width), F32),
            ((width, share), BF16),
        )
    ]
    made = pl.pallas_call(
        functools.partial(wave_kernel, sizes, (cosines, sines)),
        out_shape=between,
        in_specs=[hbm] * 11,
        out_specs=[vmem] * len(between),
        scratch_shapes=[VMEM(a.shape, a.dtype) for a in smalls]
        + [
            VMEM((chunks * pair * rows, width), F32),
            VMEM(((chunks + 2) * pitch, rows * width), BF16),
            VMEM(((chunks + 2) * pitch, rows * width), BF16),
            VMEM((2 * chunks * pitch, reach), BF16),
            VMEM((2 * pair, width), F32),
            VMEM((8, width), F32),
            VMEM((span, 8), F32),
            VMEM((8, span), F32),
            VMEM((chunks * pitch, width), F32),
            VMEM((chunks * pitch, width), F32),
            VMEM((chunks * pitch, width), F32),
            VMEM((3, pair, width), F32),
            VMEM((round_up(nf + EDGE, 8), width), F32),
            VMEM((8, width), F32),
            VMEM(group_speed.shape, F32),
            VMEM((packed, width), F32),
            VMEM((packed, width), F32),
            VMEM((far_lat + packed, width), F32),
            VMEM((far_lat + packed, width), F32),
            VMEM((band, width), F32),
            VMEM((EDGE * nd, width), F32),
            VMEM((pair, width), F32),
            VMEM((pair, width), F32),
            VMEM((pair, width), F32),
            VMEM((8, width), F32),
            VMEM((8, width), F32),
            VMEM((8, width), F32),
            VMEM((pair, 8), F32),
            VMEM((8, width), F32),
            VMEM((8, width), F32),
            VMEM((2 * all_rows, width), F32),
            VMEM((n_lat * n_freq - 1, 2 * all_rows, width), F32),
            dma((nf // 2,)), dma((len(smalls),)),
            *[pltpu.SemaphoreType.REGULAR] * 3,
            dma((3,)), dma((3,)), dma((4,)), dma((4,)), dma((4,)), dma((4,)),
            dma((1,)), dma((1,)), dma((n_lat * n_freq - 1,)), dma((n_lat * n_freq - 1,)),
        ],
        compiler_params=pltpu.CompilerParams(
            collective_id=0, has_side_effects=True, vmem_limit_bytes=32 << 20
        ),
    )(
        *[
            pltpu.with_memory_space_constraint(a, pltpu.HBM)
            for a in (spectrum.reshape(band * rows, width), *smalls)
        ]
    )
    out, ocean = pl.pallas_call(
        functools.partial(write_kernel, sizes),
        out_shape=(
            jax.ShapeDtypeStruct((band * rows, width), F32),
            jax.ShapeDtypeStruct((2, share), F32),
        ),
        in_specs=[vmem] * len(between),
        out_specs=(hbm, hbm),
        scratch_shapes=[
            VMEM((band * rows, width), F32), VMEM((2, share), F32), dma((nf // 2 + 1,)),
        ],
        compiler_params=pltpu.CompilerParams(vmem_limit_bytes=16 << 20),
    )(*made)
    return out.reshape(spectrum.shape), ocean.T


def solution(mesh):
    axes = tuple(mesh.shape[a] for a in ("lat", "lon", "freq"))
    return jax.shard_map(
        functools.partial(local, axes),
        mesh=mesh,
        in_specs=(
            P("freq", None, "lat", "lon"),
            P("freq"),
            P("lat", "lon"),
            P("lat", "lon"),
            P("lat", "lon"),
            P(),
            P(),
            P(),
            P(),
            P("lat", "lon"),
        ),
        out_specs=(P("freq", None, "lat", "lon"), P(("lon", "freq"), None)),
        check_vma=False,
    )
```
